8 devices in a mesh: data: 2 (over z, y), model: 4 (over x, core).
Axes of the slice: x: 2, y: 2, z: 1, core: 2. Of those that a mesh axis runs over, the one named last changes fastest.
Arguments:
- tokens: bfloat16 [16384, 2048], P('data')
- w_query: bfloat16 [2048, 2048], P('data', 'model')
- w_kv: bfloat16 [2048, 256], P('data')
- w_out: bfloat16 [2048, 2048], P('model', 'data')
- ln_gain: float32 [2048], replicated
- positions: int32 [256], replicated
- grad_out: bfloat16 [16384, 2048], P('data')
Outputs:
- output 1: bfloat16 [16384, 2048], P('data')
- output 2: bfloat16 [16384, 2048], P('data')
- output 3: bfloat16 [2048, 2048], P('data', 'model')
- output 4: bfloat16 [2048, 256], P('data')
- output 5: bfloat16 [2048, 2048], P('model', 'data')
All inputs are finite; a program needn't handle non-finite values.
Results may differ from the reference program's by a relative error of at most 0.0145341.
Values are sent between devices in bfloat16 or wider.
A program may use at most 1 GiB of HBM per device.

```python
import jax
import jax.numpy as jnp
from jax import lax

D = 2048
HEADS = 16
HEAD = 128
SEQ_LEN = 256
SEQ_COUNT = 64
NORM_EPS = 1e-6
TOTAL_TOK = SEQ_COUNT * SEQ_LEN


def setup_inputs(seed: int = 0) -> dict:
    keys = jax.random.split(jax.random.key(seed), 7)
    out_scale = (SEQ_LEN / (16.0 * HEADS * HEAD)) ** 0.5
    tokens = jax.random.normal(keys[0], (TOTAL_TOK, D), jnp.float32)
    w_query = jax.random.normal(keys[1], (D, HEADS * HEAD), jnp.float32) * D ** -0.5
    w_kv = jax.random.normal(keys[2], (D, 2 * HEAD), jnp.float32) * D ** -0.5
    w_out = jax.random.normal(keys[3], (HEADS * HEAD, D), jnp.float32) * out_scale
    ln_gain = jax.random.uniform(keys[4], (D,), jnp.float32, 0.5, 1.5)
    positions = jax.random.permutation(keys[5], SEQ_LEN).astype(jnp.int32)
    grad_out = jax.random.normal(keys[6], (TOTAL_TOK, D), jnp.float32)
    return {
        "tokens": tokens.astype(jnp.bfloat16),
        "w_query": w_query.astype(jnp.bfloat16),
        "w_kv": w_kv.astype(jnp.bfloat16),
        "w_out": w_out.astype(jnp.bfloat16),
        "ln_gain": ln_gain,
        "positions": positions,
        "grad_out": grad_out.astype(jnp.bfloat16),
    }


def reference(tokens, w_query, w_kv, w_out, ln_gain, positions, grad_out):
    visible = positions[None, :] <= positions[:, None]
    score_scale = HEAD ** -0.5

    def attend_one(pair):
        q_seq, kv_seq = pair
        scores = jnp.einsum("qhe,ke->hqk", q_seq.astype(jnp.float32), kv_seq[:, :HEAD].astype(jnp.float32)) * score_scale
        probs = jax.nn.softmax(jnp.where(visible[None], scores, -1e30), axis=-1).astype(jnp.bfloat16)
        mixed = jnp.einsum("hqk,ke->qhe", probs.astype(jnp.float32), kv_seq[:, HEAD:].astype(jnp.float32))
        return mixed.astype(jnp.bfloat16)

    def forward(tok_rows, q_weight, kv_weight, o_weight):
        rows_f = tok_rows.astype(jnp.float32)
        centred = rows_f - jnp.mean(rows_f, axis=-1, keepdims=True)
        inv_std = lax.rsqrt(jnp.mean(centred * centred, axis=-1, keepdims=True) + NORM_EPS)
        hidden = (centred * inv_std * ln_gain).astype(jnp.bfloat16)
        queries = jnp.dot(hidden, q_weight, preferred_element_type=jnp.float32).astype(jnp.bfloat16)
        key_vals = jnp.dot(hidden, kv_weight, preferred_element_type=jnp.float32).astype(jnp.bfloat16)
        mixed = lax.map(jax.checkpoint(attend_one), (queries.reshape(SEQ_COUNT, SEQ_LEN, HEADS, HEAD), key_vals.reshape(SEQ_COUNT, SEQ_LEN, 2 * HEAD)))
        mixed = mixed.reshape(TOTAL_TOK, HEADS * HEAD)
        return jnp.dot(mixed, o_weight, preferred_element_type=jnp.float32).astype(jnp.bfloat16)

    result, pullback = jax.vjp(forward, tokens, w_query, w_kv, w_out)
    grad_tokens, grad_query, grad_kv, grad_o = pullback(grad_out)
    return (result, grad_tokens, grad_query, grad_kv, grad_o)
```

```python
import functools

import jax
import jax.numpy as jnp
from jax import lax
from jax.experimental import pallas as pl
from jax.experimental.pallas import tpu as pltpu
from jax.sharding import PartitionSpec as P

NORM_EPS = 1e-6
LOG2E = 1.4426950408889634
BF16, F32 = jnp.bfloat16, jnp.float32
NN = (((1,), (0,)), ((), ()))
NT = (((1,), (1,)), ((), ()))
TN = (((0,), (0,)), ((), ()))
MESH = pl.DeviceIdType.MESH
ANY = pl.BlockSpec(memory_space=pl.ANY)
VMEM = pl.BlockSpec(memory_space=pltpu.VMEM)
LIMIT = 62 * 2**20


def dot(a, b, dims):
    return lax.dot_general(a, b, dims, preferred_element_type=F32)


def place():
    d, m = lax.axis_index("data"), lax.axis_index("model")
    x, c = m // 2, m % 2
    return d, m, x, c, (1 - d, m), (d, 2 * (1 - x) + c), (d, 2 * x + (1 - c))


def entry_barrier(peers):
    barrier = pltpu.get_barrier_semaphore()
    for peer in peers:
        pl.semaphore_signal(barrier, inc=1, device_id=peer, device_id_type=MESH)
    pl.semaphore_wait(barrier, len(peers))


def remote(src, dst, send, recv, peer):
    return pltpu.make_async_remote_copy(src_ref=src, dst_ref=dst, send_sem=send, recv_sem=recv, device_id=peer, device_id_type=MESH)


class Gather:
    def __init__(self, piece, full, region, send, recv, local):
        self.piece, self.full, self.region = piece, full, region
        self.send, self.recv, self.local = send, recv, local

    def copies(self):
        d, m, x, c, yn, xn, pn = place()
        ym, xm = (1 - d, m), (d, 2 * (1 - x) + c)
        full, reg, s, r = self.full, self.region, self.send, self.recv
        at = lambda dm, part=None: full.at[reg(dm[0], dm[1], part)]
        diag = (1 - d, 2 * (1 - x) + c)
        own = at((d, m))
        first = [remote(self.piece, own, s.at[0], r.at[0], yn), remote(self.piece, own, s.at[1], r.at[1], xn), remote(self.piece, own, s.at[2], r.at[2], pn)]
        second = [
            remote(at(ym, 0), at(ym, 0), s.at[3], r.at[3], xn),
            remote(at(xm, 1), at(xm, 1), s.at[4], r.at[4], yn),
            remote(at(ym), at(ym), s.at[5], r.at[5], pn),
            remote(at(xm), at(xm), s.at[6], r.at[6], pn),
        ]
        third = [remote(at(diag, 0), at(diag, 0), s.at[7], r.at[7], pn), remote(at(diag, 1), at(diag, 1), s.at[8], r.at[8], pn)]
        mine = pltpu.make_async_copy(self.piece, own, self.local)
        return first, second, third, mine

    def start(self):
        first, second, third, mine = self.copies()
        for copy in first:
            copy.start()
        mine.start()

    def middle(self):
        first, second, third, mine = self.copies()
        first[0].wait_recv()
        second[0].start()
        second[2].start()
        first[1].wait_recv()
        second[1].start()
        second[3].start()

    def finish(self):
        first, second, third, mine = self.copies()
        second[0].wait_recv()
        third[0].start()
        second[1].wait_recv()
        third[1].start()
        mine.wait()
        first[2].wait_recv()
        second[2].wait_recv()
        second[3].wait_recv()
        third[0].wait_recv()
        third[1].wait_recv()
        for copy in first + second + third:
            copy.wait_send()


def normalize(rows):
    rows = rows.astype(F32)
    centred = rows - jnp.mean(rows, axis=-1, keepdims=True)
    inv_std = lax.rsqrt(jnp.mean(centred * centred, axis=-1, keepdims=True) + NORM_EPS)
    return centred * inv_std, inv_std


def q_region(rows, cols, d, m, part):
    if part is None:
        return pl.ds(d * rows, rows), pl.ds(pl.multiple_of(m * cols, cols), cols)
    return pl.ds(d * rows + part * (rows // 2), rows // 2), pl.ds(pl.multiple_of(m * cols, cols), cols)


def o_region(rows, cols, d, m, part):
    if part is None:
        return pl.ds(m * rows, rows), pl.ds(pl.multiple_of(d * cols, cols), cols)
    return pl.ds(m * rows + part * (rows // 2), rows // 2), pl.ds(pl.multiple_of(d * cols, cols), cols)


def gather_norm_kernel(half, tok, wq, wkv, gain, wq_full, wkv_full, hidden, q_send, q_recv, kv_send, kv_recv, local):
    d, m, x, c, yn, xn, pn = place()
    rows, cols = wq.shape
    entry_barrier((yn, xn, pn))
    krows = wkv.shape[0] // 2
    k_here = lambda dd, cc: wkv_full.at[pl.ds(dd * 2 * krows + cc * krows, krows), :]
    k_out = remote(wkv.at[pl.ds(c * krows, krows), :], k_here(d, c), kv_send.at[0], kv_recv.at[0], yn)
    k_fwd = remote(k_here(1 - d, c), k_here(1 - d, c), kv_send.at[1], kv_recv.at[1], pn)
    k_own = pltpu.make_async_copy(wkv, wkv_full.at[pl.ds(d * 2 * krows, 2 * krows), :], local.at[1])
    k_out.start()
    gather = Gather(wq, wq_full, functools.partial(q_region, rows, cols), q_send, q_recv, local.at[0])
    gather.start()
    k_own.start()

    def block(tok_blk, hid_blk):
        hid_blk[...] = (normalize(tok_blk[...])[0] * gain[...]).astype(BF16)

    depth, tile = tok.shape[1], 512
    spec = pl.BlockSpec((tile, depth), lambda i: (i, 0))
    pltpu.emit_pipeline(block, grid=(half // tile,), in_specs=[spec], out_specs=[spec])(tok.at[pl.ds(c * half, half), :], hidden)
    k_out.wait_recv()
    k_fwd.start()
    gather.middle()
    gather.finish()
    k_fwd.wait_recv()
    k_own.wait()
    k_out.wait_send()
    k_fwd.wait_send()


def project_kernel(hidden, wq_full, wkv_full, wo, queries, key_vals, wo_full, o_send, o_recv, local):
    d, m, x, c, yn, xn, pn = place()
    rows, cols = wo.shape
    entry_barrier((yn, xn, pn))
    gather = Gather(wo, wo_full, functools.partial(o_region, rows, cols), o_send, o_recv, local)
    gather.start()
    depth, width = wq_full.shape
    tile = 1024

    def block(a, b, out):
        out[...] = dot(a[...], b[...], NN).astype(BF16)

    def run(cols_lo, cols_n, w, out):
        pltpu.emit_pipeline(
            block,
            grid=(hidden.shape[0] // tile,),
            in_specs=[pl.BlockSpec((tile, depth), lambda i: (i, 0)), pl.BlockSpec((depth, cols_n), lambda i: (0, cols_lo // cols_n))],
            out_specs=[pl.BlockSpec((tile, cols_n), lambda i: (i, cols_lo // cols_n))],
        )(hidden, w, out)

    run(0, wkv_full.shape[1], wkv_full, key_vals)
    run(0, width // 2, wq_full, queries)
    gather.middle()
    run(width // 2, width // 2, wq_full, queries)
    gather.finish()


def mm_kernel(dims, off, a, b, out):
    out[...] = dot(a[...], b[...], dims).astype(BF16)


def matmul(a, b, dims, rows, row_block, tile=1024):
    depth = a.shape[1]
    width = b.shape[1] if dims == NN else b.shape[0]
    b_spec = pl.BlockSpec((depth, tile), lambda j, i, off: (0, j)) if dims == NN else pl.BlockSpec((tile, depth), lambda j, i, off: (j, 0))
    return pl.pallas_call(
        functools.partial(mm_kernel, dims),
        grid_spec=pltpu.PrefetchScalarGridSpec(
            num_scalar_prefetch=1,
            grid=(width // tile, rows // tile),
            in_specs=[pl.BlockSpec((tile, depth), lambda j, i, off: (off[0] + i, 0)), b_spec],
            out_specs=pl.BlockSpec((tile, tile), lambda j, i, off: (i, j)),
        ),
        out_shape=jax.ShapeDtypeStruct((rows, width), BF16),
        cost_estimate=pl.CostEstimate(flops=2 * rows * depth * width, bytes_accessed=2 * (rows * depth + depth * width + rows * width), transcendentals=0),
        compiler_params=pltpu.CompilerParams(vmem_limit_bytes=LIMIT),
    )(row_block, a, b)


def attend_kernel(heads, q_ref, do_ref, kv_ref, pos_c_ref, pos_r_ref, o_ref, dq_ref, dkv_ref, seen, pt, dst):
    seq, head_dim = kv_ref.shape[0], kv_ref.shape[1] // 2

    @pl.when(pl.program_id(0) == 0)
    def _():
        seen[...] = jnp.where(pos_c_ref[...] <= pos_r_ref[...], 1.0, -1.0)

    k, v = kv_ref[:, :head_dim], kv_ref[:, head_dim:]
    kt, vt = k.T, v.T
    scale = head_dim ** -0.5
    cols = lambda h: slice(h * head_dim, (h + 1) * head_dim)
    lanes = lambda h: slice(h * seq, (h + 1) * seq)
    scores, grads, total = {}, {}, [None, None]

    def scored(h):
        scores[h] = dot(k, q_ref[:, cols(h)], NT)
        grads[h] = dot(v, do_ref[:, cols(h)], NT)

    def softmax(h):
        s = jnp.where(seen[...] > 0, scores.pop(h) * (scale * LOG2E), -1e30)
        e = jnp.exp2(s - jnp.max(s, axis=0, keepdims=True))
        p = e * (1.0 / jnp.sum(e, axis=0, keepdims=True))
        pt[:, lanes(h)] = p.astype(BF16)
        dp = grads.pop(h)
        dst[:, lanes(h)] = (p * (dp - jnp.sum(p * dp, axis=0, keepdims=True))).astype(BF16)

    def mixed(h):
        o_ref[:, cols(h)] = dot(vt, pt[:, lanes(h)], NN).T.astype(BF16)
        dq_ref[:, cols(h)] = (dot(kt, dst[:, lanes(h)], NN).T * scale).astype(BF16)
        dv = dot(pt[:, lanes(h)], do_ref[:, cols(h)], NN)
        dk = dot(dst[:, lanes(h)], q_ref[:, cols(h)], NN)
        total[0] = dk if total[0] is None else total[0] + dk
        total[1] = dv if total[1] is None else total[1] + dv

    for t in range(heads + 2):
        if t < heads:
            scored(t)
        if 0 <= t - 2:
            mixed(t - 2)
        if 0 <= t - 1 < heads:
            softmax(t - 1)
    dkv_ref[:, :head_dim] = (total[0] * scale).astype(BF16)
    dkv_ref[:, head_dim:] = total[1].astype(BF16)


def attend(queries, grad_mixed, key_vals, positions):
    rows, width = queries.shape
    seq, pair = positions.shape[0], key_vals.shape[1]
    heads = width // (pair // 2)
    wide = pl.BlockSpec((seq, width), lambda i: (i, 0))
    narrow = pl.BlockSpec((seq, pair), lambda i: (i, 0))
    return pl.pallas_call(
        functools.partial(attend_kernel, heads),
        grid=(rows // seq,),
        in_specs=[wide, wide, narrow, pl.BlockSpec((seq, 1), lambda i: (0, 0)), pl.BlockSpec((1, seq), lambda i: (0, 0))],
        out_specs=[wide, wide, narrow],
        out_shape=[jax.ShapeDtypeStruct((rows, width), BF16)] * 2 + [jax.ShapeDtypeStruct((rows, pair), BF16)],
        scratch_shapes=[pltpu.VMEM((seq, seq), F32), pltpu.VMEM((seq, heads * seq), BF16), pltpu.VMEM((seq, heads * seq), BF16)],
        cost_estimate=pl.CostEstimate(flops=12 * rows * seq * width, bytes_accessed=8 * rows * width, transcendentals=rows * seq * heads),
        compiler_params=pltpu.CompilerParams(vmem_limit_bytes=LIMIT),
    )(queries, grad_mixed, key_vals, positions.reshape(seq, 1), positions.reshape(1, seq))


def wgrad_o_kernel(off, a, b, out):
    part = dot(a[...], b[...], TN)

    @pl.when(pl.program_id(2) == 0)
    def _():
        out[...] = part

    @pl.when(pl.program_id(2) > 0)
    def _():
        out[...] += part


def wgrad_o(mixed, grads, offs, height, tile=1024, deep=2048):
    rows, width = mixed.shape[0], grads.shape[1]
    return pl.pallas_call(
        wgrad_o_kernel,
        grid_spec=pltpu.PrefetchScalarGridSpec(
            num_scalar_prefetch=1,
            grid=(height // tile, width // tile, rows // deep),
            in_specs=[pl.BlockSpec((deep, tile), lambda i, j, k, off: (k, off[1] + i)), pl.BlockSpec((deep, tile), lambda i, j, k, off: (off[0] + k, j))],
            out_specs=pl.BlockSpec((tile, tile), lambda i, j, k, off: (i, j)),
        ),
        out_shape=jax.ShapeDtypeStruct((height, width), F32),
        cost_estimate=pl.CostEstimate(flops=2 * rows * height * width, bytes_accessed=4 * rows * width, transcendentals=0),
        compiler_params=pltpu.CompilerParams(vmem_limit_bytes=LIMIT),
    )(offs, mixed, grads)


def wgrad_q_kernel(off, a, b, c, out_b, out_c):
    part_b = dot(a[...], b[...], TN)
    part_c = dot(a[...], c[...], TN)

    @pl.when(pl.program_id(1) == 0)
    def _():
        out_b[...] = part_b
        out_c[...] = part_c

    @pl.when(pl.program_id(1) > 0)
    def _():
        out_b[...] += part_b
        out_c[...] += part_c


def wgrad_q(hidden, grad_query, grad_kv, offs, tile=1024, deep=1024):
    rows, depth = hidden.shape
    pair = grad_kv.shape[1]
    half = grad_query.shape[1] // 2
    return pl.pallas_call(
        wgrad_q_kernel,
        grid_spec=pltpu.PrefetchScalarGridSpec(
            num_scalar_prefetch=1,
            grid=(depth // tile, rows // deep),
            in_specs=[
                pl.BlockSpec((deep, tile), lambda i, k, off: (k, i)),
                pl.BlockSpec((deep, half), lambda i, k, off: (k, off[0])),
                pl.BlockSpec((deep, pair), lambda i, k, off: (k, 0)),
            ],
            out_specs=[pl.BlockSpec((tile, half), lambda i, k, off: (i, 0)), pl.BlockSpec((tile, pair), lambda i, k, off: (i, 0))],
        ),
        out_shape=[jax.ShapeDtypeStruct((depth, half), F32), jax.ShapeDtypeStruct((depth, pair), F32)],
        cost_estimate=pl.CostEstimate(flops=2 * rows * depth * (half + pair), bytes_accessed=4 * rows * depth, transcendentals=0),
        compiler_params=pltpu.CompilerParams(vmem_limit_bytes=LIMIT),
    )(offs, hidden, grad_query, grad_kv)


def grad_tok_kernel(blocks, off, gq, gkv, wq, wkv, gain, tok, out, held):
    i = pl.program_id(0)

    def product():
        return dot(gq[...], wq[...], NT) + dot(gkv[...], wkv[...], NT)

    def epilogue():
        normed, inv_std = normalize(tok[...])
        g = held[...] * gain[...]
        out[...] = (inv_std * (g - jnp.mean(g, axis=-1, keepdims=True) - normed * jnp.mean(g * normed, axis=-1, keepdims=True))).astype(BF16)

    @pl.when(i == 0)
    def _():
        held[...] = product()

    @pl.when((i > 0) & (i < blocks))
    def _():
        fresh = product()
        epilogue()
        held[...] = fresh

    @pl.when(i == blocks)
    def _():
        epilogue()


def grad_tok(grad_query, grad_kv, wq, wkv, gain, tok, row_block, tile=512):
    rows, width = grad_query.shape
    depth, pair = wkv.shape
    blocks = rows // tile
    now = lambda i, off: (jnp.minimum(i, blocks - 1), 0)
    late = lambda i, off: (off[0] + jnp.maximum(i - 1, 0), 0)
    whole = lambda i, off: (0, 0)
    once = pl.Buffered(1)
    return pl.pallas_call(
        functools.partial(grad_tok_kernel, blocks),
        grid_spec=pltpu.PrefetchScalarGridSpec(
            num_scalar_prefetch=1,
            grid=(blocks + 1,),
            in_specs=[
                pl.BlockSpec((tile, width), now),
                pl.BlockSpec((tile, pair), now),
                pl.BlockSpec((depth, width), whole, pipeline_mode=once),
                pl.BlockSpec((depth, pair), whole, pipeline_mode=once),
                pl.BlockSpec((1, depth), whole, pipeline_mode=once),
                pl.BlockSpec((tile, depth), late),
            ],
            out_specs=pl.BlockSpec((tile, depth), lambda i, off: (jnp.maximum(i - 1, 0), 0)),
            scratch_shapes=[pltpu.VMEM((tile, depth), F32)],
        ),
        out_shape=jax.ShapeDtypeStruct((rows, depth), BF16),
        cost_estimate=pl.CostEstimate(flops=2 * rows * depth * (width + pair), bytes_accessed=8 * rows * depth, transcendentals=0),
        compiler_params=pltpu.CompilerParams(vmem_limit_bytes=LIMIT),
    )(row_block, grad_query, grad_kv, wq, wkv, gain, tok)


def join_kernel(blocks, off, own, got, out):
    i = pl.program_id(0)
    is_own = (i // blocks) == off[0]

    @pl.when(is_own)
    def _():
        out[...] = own[...]

    @pl.when(jnp.logical_not(is_own))
    def _():
        out[...] = got[...]


def join(own, got, core, tile=1024):
    rows, width = own.shape
    blocks = rows // tile
    own_map = lambda i, off: (jnp.clip(i - off[0] * blocks, 0, blocks - 1), 0)
    got_map = lambda i, off: (jnp.clip(i - (1 - off[0]) * blocks, 0, blocks - 1), 0)
    return pl.pallas_call(
        functools.partial(join_kernel, blocks),
        grid_spec=pltpu.PrefetchScalarGridSpec(
            num_scalar_prefetch=1,
            grid=(2 * blocks,),
            in_specs=[pl.BlockSpec((tile, width), own_map), pl.BlockSpec((tile, width), got_map)],
            out_specs=pl.BlockSpec((tile, width), lambda i, off: (i, 0)),
        ),
        out_shape=jax.ShapeDtypeStruct((2 * rows, width), own.dtype),
        cost_estimate=pl.CostEstimate(flops=rows * width, bytes_accessed=8 * rows * width, transcendentals=0),
        compiler_params=pltpu.CompilerParams(vmem_limit_bytes=LIMIT),
    )(core, own, got)


def solution(mesh):
    model_size = mesh.shape["model"]
    cores = [(i, i ^ 1) for i in range(model_size)]
    datas = [(0, 1), (1, 0)]
    sems = lambda n: pltpu.SemaphoreType.DMA((n,))

    def device_step(tok, wq_blk, wkv_blk, wo_blk, ln_gain, positions, grad):
        count, depth = tok.shape
        half = count // 2
        width = wq_blk.shape[1] * model_size
        pair = wkv_blk.shape[1]
        m = lax.axis_index("model")
        d = lax.axis_index("data")
        x, c = m // 2, m % 2
        gain = ln_gain.reshape(1, depth)
        comm = lambda cid: pltpu.CompilerParams(collective_id=cid, has_side_effects=True, vmem_limit_bytes=LIMIT)

        wq, wkv, hidden = pl.pallas_call(
            functools.partial(gather_norm_kernel, half),
            in_specs=[ANY, VMEM, VMEM, VMEM],
            out_specs=[ANY, ANY, ANY],
            out_shape=[jax.ShapeDtypeStruct((depth, width), BF16), jax.ShapeDtypeStruct((depth, pair), BF16), jax.ShapeDtypeStruct((half, depth), BF16)],
            scratch_shapes=[sems(9), sems(9), sems(2), sems(2), sems(2)],
            compiler_params=comm(0),
        )(tok, wq_blk, wkv_blk, gain)
        queries, key_vals, wo = pl.pallas_call(
            project_kernel,
            in_specs=[ANY, ANY, ANY, VMEM],
            out_specs=[ANY, ANY, ANY],
            out_shape=[jax.ShapeDtypeStruct((half, width), BF16), jax.ShapeDtypeStruct((half, pair), BF16), jax.ShapeDtypeStruct((width, depth), BF16)],
            scratch_shapes=[sems(9), sems(9), pltpu.SemaphoreType.DMA],
            compiler_params=comm(1),
        )(hidden, wq, wkv, wo_blk)

        core = c.reshape(1).astype(jnp.int32)
        grad_mixed = matmul(grad, wo, NT, half, core * (half // 1024))
        mixed, grad_query, grad_kv = attend(queries, grad_mixed, key_vals, positions)

        own_rows = width // 2
        part_o = wgrad_o(mixed, grad, jnp.stack([c * (half // 2048), x * (own_rows // 1024)]).astype(jnp.int32), own_rows)
        part_q, part_kv = wgrad_q(hidden, grad_query, grad_kv, x.reshape(1).astype(jnp.int32))

        def reduce_pieces(part, axis_core, axis_data):
            def split(a, index, axis):
                size = a.shape[axis] // 2
                keep = lax.dynamic_slice_in_dim(a, index * size, size, axis)
                give = lax.dynamic_slice_in_dim(a, (1 - index) * size, size, axis)
                return keep, give

            keep, give = split(part, c, axis_core)
            both = keep + lax.ppermute(give, "model", cores)
            keep, give = split(both, d, axis_data)
            return keep + lax.ppermute(give, "data", datas)

        grad_w_out = reduce_pieces(part_o, 0, 1).astype(BF16)
        grad_w_query = reduce_pieces(part_q, 1, 0).astype(BF16)
        kv_cols = reduce_pieces(part_kv, 1, 0).astype(BF16)
        kv_other = lax.ppermute(kv_cols, "model", cores)
        grad_w_kv = jnp.where(c == 0, jnp.concatenate([kv_cols, kv_other], axis=1), jnp.concatenate([kv_other, kv_cols], axis=1))

        dtok = grad_tok(grad_query, grad_kv, wq, wkv, gain, tok, core * (half // 512))
        dtok_other = lax.ppermute(dtok, "model", cores)
        out = matmul(mixed, wo, NN, half, core * 0)
        out_other = lax.ppermute(out, "model", cores)
        grad_tokens = join(dtok, dtok_other, core)
        attn_out = join(out, out_other, core)
        return attn_out, grad_tokens, grad_w_query, grad_w_kv, grad_w_out

    return jax.shard_map(
        device_step,
        mesh=mesh,
        in_specs=(P("data", None), P("data", "model"), P("data", None), P("model", "data"), P(), P(), P("data", None)),
        out_specs=(P("data", None), P("data", None), P("data", "model"), P("data", None), P("model", "data")),
        check_vma=False,
    )
```

```python
import functools

import jax
import jax.numpy as jnp
from jax import lax
from jax.experimental import pallas as pl
from jax.experimental.pallas import tpu as pltpu
from jax.sharding import PartitionSpec as P

NORM_EPS = 1e-6
LOG2E = 1.4426950408889634
BF16, F32 = jnp.bfloat16, jnp.float32
NN = (((1,), (0,)), ((), ()))
NT = (((1,), (1,)), ((), ()))
TN = (((0,), (0,)), ((), ()))
MESH = pl.DeviceIdType.MESH
ANY = pl.BlockSpec(memory_space=pl.ANY)
VMEM = pl.BlockSpec(memory_space=pltpu.VMEM)
LIMIT = 62 * 2**20


def dot(a, b, dims):
    return lax.dot_general(a, b, dims, preferred_element_type=F32)


def place():
    d, m = lax.axis_index("data"), lax.axis_index("model")
    x, c = m // 2, m % 2
    return d, m, x, c, (1 - d, m), (d, 2 * (1 - x) + c), (d, 2 * x + (1 - c))


def entry_barrier(peers):
    barrier = pltpu.get_barrier_semaphore()
    for peer in peers:
        pl.semaphore_signal(barrier, inc=1, device_id=peer, device_id_type=MESH)
    pl.semaphore_wait(barrier, len(peers))


def remote(src, dst, send, recv, peer):
    return pltpu.make_async_remote_copy(src_ref=src, dst_ref=dst, send_sem=send, recv_sem=recv, device_id=peer, device_id_type=MESH)


class Gather:
    def __init__(self, piece, full, region, send, recv, local):
        self.piece, self.full, self.region = piece, full, region
        self.send, self.recv, self.local = send, recv, local

    def copies(self):
        d, m, x, c, yn, xn, pn = place()
        ym, xm = (1 - d, m), (d, 2 * (1 - x) + c)
        full, reg, s, r = self.full, self.region, self.send, self.recv
        at = lambda dm, part=None: full.at[reg(dm[0], dm[1], part)]
        diag = (1 - d, 2 * (1 - x) + c)
        own = at((d, m))
        first = [remote(self.piece, own, s.at[0], r.at[0], yn), remote(self.piece, own, s.at[1], r.at[1], xn), remote(self.piece, own, s.at[2], r.at[2], pn)]
        second = [
            remote(at(ym, 0), at(ym, 0), s.at[3], r.at[3], xn),
            remote(at(xm, 1), at(xm, 1), s.at[4], r.at[4], yn),
            remote(at(ym), at(ym), s.at[5], r.at[5], pn),
            remote(at(xm), at(xm), s.at[6], r.at[6], pn),
        ]
        third = [remote(at(diag, 0), at(diag, 0), s.at[7], r.at[7], pn), remote(at(diag, 1), at(diag, 1), s.at[8], r.at[8], pn)]
        mine = pltpu.make_async_copy(self.piece, own, self.local)
        return first, second, third, mine

    def start(self):
        first, second, third, mine = self.copies()
        for copy in first:
            copy.start()
        mine.start()

    def middle(self):
        first, second, third, mine = self.copies()
        first[1].wait_recv()
        second[1].start()
        second[3].start()
        first[0].wait_recv()
        second[0].start()
        second[2].start()

    def own_half(self):
        first, second, third, mine = self.copies()
        mine.wait()
        first[2].wait_recv()
        second[2].wait_recv()

    def finish(self):
        first, second, third, mine = self.copies()
        second[0].wait_recv()
        third[0].start()
        second[1].wait_recv()
        third[1].start()
        second[3].wait_recv()
        third[0].wait_recv()
        third[1].wait_recv()
        for copy in first + second + third:
            copy.wait_send()


def q_region(rows, cols, d, m, part):
    if part is None:
        return pl.ds(d * rows, rows), pl.ds(pl.multiple_of(m * cols, cols), cols)
    return pl.ds(d * rows + part * (rows // 2), rows // 2), pl.ds(pl.multiple_of(m * cols, cols), cols)


def o_region(rows, cols, d, m, part):
    if part is None:
        return pl.ds(m * rows, rows), pl.ds(pl.multiple_of(d * cols, cols), cols)
    return pl.ds(m * rows + part * (rows // 2), rows // 2), pl.ds(pl.multiple_of(d * cols, cols), cols)


def front_kernel(half, tok, wq, wkv, wo, gain, wcat, wo_full, hidden, means, inv_stds, proj, q_send, q_recv, o_send, o_recv, kv_send, kv_recv, local):
    d, m, x, c, yn, xn, pn = place()
    rows, cols = wq.shape
    depth, width = wo_full.shape[1], wo_full.shape[0]
    krows, pair = wkv.shape[0] // 2, wkv.shape[1]
    entry_barrier((yn, xn, pn))
    k_here = lambda dd, cc: wcat.at[pl.ds(dd * 2 * krows + cc * krows, krows), pl.ds(width, pair)]
    k_out = remote(wkv.at[pl.ds(c * krows, krows), :], k_here(d, c), kv_send.at[0], kv_recv.at[0], yn)
    k_fwd = remote(k_here(1 - d, c), k_here(1 - d, c), kv_send.at[1], kv_recv.at[1], pn)
    k_own = pltpu.make_async_copy(wkv, wcat.at[pl.ds(d * 2 * krows, 2 * krows), pl.ds(width, pair)], local.at[2])
    k_out.start()
    gather_q = Gather(wq, wcat, functools.partial(q_region, rows, cols), q_send, q_recv, local.at[0])
    gather_o = Gather(wo, wo_full, functools.partial(o_region, wo.shape[0], wo.shape[1]), o_send, o_recv, local.at[1])
    gather_q.start()
    k_own.start()

    def norm_block(tok_blk, hid_blk, mean_blk, inv_blk):
        rows_f = tok_blk[...].astype(F32)
        mean = jnp.mean(rows_f, axis=-1, keepdims=True)
        centred = rows_f - mean
        inv_std = lax.rsqrt(jnp.mean(centred * centred, axis=-1, keepdims=True) + NORM_EPS)
        hid_blk[...] = (centred * inv_std * gain[...]).astype(BF16)
        mean_blk[...] = jnp.broadcast_to(mean, mean_blk.shape)
        inv_blk[...] = jnp.broadcast_to(inv_std, inv_blk.shape)

    tile = 512
    pltpu.emit_pipeline(
        norm_block,
        grid=(half // tile,),
        in_specs=[pl.BlockSpec((tile, depth), lambda i: (i, 0))],
        out_specs=[pl.BlockSpec((tile, depth), lambda i: (i, 0))] + [pl.BlockSpec((tile, 128), lambda i: (i, 0))] * 2,
    )(tok.at[pl.ds(c * half, half), :], hidden, means, inv_stds)

    big = 1024

    def block(a, b, out):
        out[...] = dot(a[...], b[...], NN).astype(BF16)

    def run(col, cols_n, row_block, row_blocks):
        span = pl.ds(pl.multiple_of(col, cols_n), cols_n)
        pltpu.emit_pipeline(
            block,
            grid=(row_blocks,),
            in_specs=[pl.BlockSpec((big, depth), lambda i: (row_block + i, 0)), pl.BlockSpec((depth, cols_n), lambda i: (0, 0))],
            out_specs=[pl.BlockSpec((big, cols_n), lambda i: (row_block + i, 0))],
        )(hidden, wcat.at[:, span], proj.at[:, span])

    blocks = half // big
    k_out.wait_recv()
    k_fwd.start()
    k_own.wait()
    k_fwd.wait_recv()
    run(width, pair, 0, blocks)
    gather_q.middle()
    gather_o.start()
    gather_q.own_half()
    run(x * (width // 2), width // 2, 0, blocks)
    gather_q.finish()
    run((1 - x) * (width // 2), width // 2, 0, blocks // 2)
    gather_o.middle()
    run((1 - x) * (width // 2), width // 2, blocks // 2, blocks - blocks // 2)
    gather_o.own_half()
    gather_o.finish()
    k_out.wait_send()
    k_fwd.wait_send()


def mm_kernel(dims, off, a, b, out):
    out[...] = dot(a[...], b[...], dims).astype(BF16)


def matmul(a, b, dims, rows, row_block, tile=1024):
    depth = a.shape[1]
    width = b.shape[1] if dims == NN else b.shape[0]
    b_spec = pl.BlockSpec((depth, tile), lambda j, i, off: (0, j)) if dims == NN else pl.BlockSpec((tile, depth), lambda j, i, off: (j, 0))
    return pl.pallas_call(
        functools.partial(mm_kernel, dims),
        grid_spec=pltpu.PrefetchScalarGridSpec(
            num_scalar_prefetch=1,
            grid=(width // tile, rows // tile),
            in_specs=[pl.BlockSpec((tile, depth), lambda j, i, off: (off[0] + i, 0)), b_spec],
            out_specs=pl.BlockSpec((tile, tile), lambda j, i, off: (i, j)),
        ),
        out_shape=jax.ShapeDtypeStruct((rows, width), BF16),
        cost_estimate=pl.CostEstimate(flops=2 * rows * depth * width, bytes_accessed=2 * (rows * depth + depth * width + rows * width), transcendentals=0),
        compiler_params=pltpu.CompilerParams(vmem_limit_bytes=LIMIT),
    )(row_block, a, b)


def attend_kernel(heads, head_dim, qkv_ref, do_ref, pos_c_ref, pos_r_ref, o_ref, dqkv_ref, seen, pt, dst):
    seq, width = do_ref.shape
    q_ref, dq_ref = qkv_ref, dqkv_ref

    @pl.when(pl.program_id(0) == 0)
    def _():
        seen[...] = jnp.where(pos_c_ref[...] <= pos_r_ref[...], 1.0, -1.0)

    k, v = qkv_ref[:, width : width + head_dim], qkv_ref[:, width + head_dim :]
    kt, vt = k.T, v.T
    scale = head_dim ** -0.5
    cols = lambda h: slice(h * head_dim, (h + 1) * head_dim)
    lanes = lambda h: slice(h * seq, (h + 1) * seq)
    scores, grads, total = {}, {}, [None, None]

    def scored(h):
        scores[h] = dot(k, q_ref[:, cols(h)], NT)
        grads[h] = dot(v, do_ref[:, cols(h)], NT)

    def softmax(h):
        s = jnp.where(seen[...] > 0, scores.pop(h) * (scale * LOG2E), -1e30)
        e = jnp.exp2(s - jnp.max(s, axis=0, keepdims=True))
        p = e * (1.0 / jnp.sum(e, axis=0, keepdims=True))
        pt[:, lanes(h)] = p.astype(BF16)
        dp = grads.pop(h)
        dst[:, lanes(h)] = (p * (dp - jnp.sum(p * dp, axis=0, keepdims=True))).astype(BF16)

    def mixed(h):
        o_ref[:, cols(h)] = dot(vt, pt[:, lanes(h)], NN).T.astype(BF16)
        dq_ref[:, cols(h)] = (dot(kt, dst[:, lanes(h)], NN).T * scale).astype(BF16)
        dv = dot(pt[:, lanes(h)], do_ref[:, cols(h)], NN)
        dk = dot(dst[:, lanes(h)], q_ref[:, cols(h)], NN)
        total[0] = dk if total[0] is None else total[0] + dk
        total[1] = dv if total[1] is None else total[1] + dv

    for t in range(heads + 2):
        if t < heads:
            scored(t)
        if 0 <= t - 2:
            mixed(t - 2)
        if 0 <= t - 1 < heads:
            softmax(t - 1)
    dqkv_ref[:, width : width + head_dim] = (total[0] * scale).astype(BF16)
    dqkv_ref[:, width + head_dim :] = total[1].astype(BF16)


def attend(proj, grad_mixed, positions):
    rows, width = grad_mixed.shape
    seq, total = positions.shape[0], proj.shape[1]
    head_dim = (total - width) // 2
    heads = width // head_dim
    wide = pl.BlockSpec((seq, width), lambda i: (i, 0))
    wider = pl.BlockSpec((seq, total), lambda i: (i, 0))
    return pl.pallas_call(
        functools.partial(attend_kernel, heads, head_dim),
        grid=(rows // seq,),
        in_specs=[wider, wide, pl.BlockSpec((seq, 1), lambda i: (0, 0)), pl.BlockSpec((1, seq), lambda i: (0, 0))],
        out_specs=[wide, wider],
        out_shape=[jax.ShapeDtypeStruct((rows, width), BF16), jax.ShapeDtypeStruct((rows, total), BF16)],
        scratch_shapes=[pltpu.VMEM((seq, seq), F32), pltpu.VMEM((seq, heads * seq), BF16), pltpu.VMEM((seq, heads * seq), BF16)],
        cost_estimate=pl.CostEstimate(flops=12 * rows * seq * width, bytes_accessed=8 * rows * width, transcendentals=rows * seq * heads),
        compiler_params=pltpu.CompilerParams(vmem_limit_bytes=LIMIT),
    )(proj, grad_mixed, positions.reshape(seq, 1), positions.reshape(1, seq))


def give_kernel(off, a, b, out):
    part = dot(a[...], b[...], TN)

    @pl.when(pl.program_id(2) == 0)
    def _():
        out[...] = part

    @pl.when(pl.program_id(2) > 0)
    def _():
        out[...] += part


def keep_kernel(axis, off, a, b, got, send, keep):
    part = dot(a[...], b[...], TN)
    k = pl.program_id(2)

    def add(out):
        @pl.when(k == 0)
        def _():
            out[...] = got[...] + part

        @pl.when(k > 0)
        def _():
            out[...] += part

    pl.when(pl.program_id(axis) == 0)(lambda: add(send))
    pl.when(pl.program_id(axis) == 1)(lambda: add(keep))


def wgrad(a, b, offs, shape, tiles, got=None, axis=None):
    bm, bn, deep = tiles
    height, width = shape
    grid = (height // bm, width // bn, a.shape[0] // deep)
    half = lambda t, ax, off: jnp.where(t == 0, 1 - off[3], off[3]) if axis == ax else t
    in_specs = [
        pl.BlockSpec((deep, bm), lambda i, j, k, off: (k, off[0] + half(i, 0, off))),
        pl.BlockSpec((deep, bn), lambda i, j, k, off: (off[1] + k, off[2] + half(j, 1, off))),
    ]
    cost = pl.CostEstimate(flops=2 * a.shape[0] * height * width, bytes_accessed=2 * a.shape[0] * (height + width), transcendentals=0)
    params = pltpu.CompilerParams(vmem_limit_bytes=LIMIT)
    if got is None:
        return pl.pallas_call(
            give_kernel,
            grid_spec=pltpu.PrefetchScalarGridSpec(
                num_scalar_prefetch=1, grid=grid, in_specs=in_specs, out_specs=pl.BlockSpec((bm, bn), lambda i, j, k, off: (i, j))
            ),
            out_shape=jax.ShapeDtypeStruct(shape, F32),
            cost_estimate=cost,
            compiler_params=params,
        )(offs, a, b)
    piece = pl.BlockSpec((bm, bn), lambda i, j, k, off: (0, 0))
    return pl.pallas_call(
        functools.partial(keep_kernel, axis),
        grid_spec=pltpu.PrefetchScalarGridSpec(
            num_scalar_prefetch=1,
            grid=grid,
            in_specs=in_specs + [pl.BlockSpec((bm, bn), lambda i, j, k, off: (half(i, 0, off), half(j, 1, off)))],
            out_specs=[piece, piece],
        ),
        out_shape=[jax.ShapeDtypeStruct((bm, bn), F32)] * 2,
        cost_estimate=cost,
        compiler_params=params,
    )(offs, a, b, got)


def out_kernel(off, a, b, full, send):
    block = dot(a[...], b[...], NN).astype(BF16)
    full[...] = block
    send[...] = block


def project_out(mixed, wo, core, tile=1024):
    rows, depth = mixed.shape
    width = wo.shape[1]
    blocks = rows // tile
    return pl.pallas_call(
        out_kernel,
        grid_spec=pltpu.PrefetchScalarGridSpec(
            num_scalar_prefetch=1,
            grid=(width // tile, blocks),
            in_specs=[pl.BlockSpec((tile, depth), lambda j, i, off: (i, 0)), pl.BlockSpec((depth, tile), lambda j, i, off: (0, j))],
            out_specs=[pl.BlockSpec((tile, tile), lambda j, i, off: (off[0] * blocks + i, j)), pl.BlockSpec((tile, tile), lambda j, i, off: (i, j))],
        ),
        out_shape=[jax.ShapeDtypeStruct((2 * rows, width), BF16), jax.ShapeDtypeStruct((rows, width), BF16)],
        cost_estimate=pl.CostEstimate(flops=2 * rows * depth * width, bytes_accessed=2 * rows * (depth + 2 * width), transcendentals=0),
        compiler_params=pltpu.CompilerParams(vmem_limit_bytes=LIMIT),
    )(core, mixed, wo)


def grad_tok_kernel(passing, off, gqkv, wcat, gain, tok, means, inv_stds, *refs):
    if passing:
        got, _, _, full, send, y_full = refs
        y_full[...] = got[...]
    else:
        full, send = refs
    mean, inv_std = means[:, :1], inv_stds[:, :1]
    g = dot(gqkv[...], wcat[...], NT) * gain[...]
    normed = (tok[...].astype(F32) - mean) * inv_std
    block = (inv_std * (g - jnp.mean(g, axis=-1, keepdims=True) - normed * jnp.mean(g * normed, axis=-1, keepdims=True))).astype(BF16)
    full[...] = block
    send[...] = block


def grad_tok(gqkv, wcat, gain, tok, means, inv_stds, core, part, earlier=None, tile=512):
    rows, total = gqkv.shape
    depth = wcat.shape[0]
    blocks = rows // tile
    steps = blocks // 2
    first = part * steps
    whole = lambda i, off: (0, 0)
    once = pl.Buffered(1)
    in_specs = [
        pl.BlockSpec((tile, total), lambda i, off: (first + i, 0)),
        pl.BlockSpec((depth, total), whole, pipeline_mode=once),
        pl.BlockSpec((1, depth), whole, pipeline_mode=once),
        pl.BlockSpec((tile, depth), lambda i, off: (off[0] * blocks + first + i, 0)),
        pl.BlockSpec((tile, 128), lambda i, off: (first + i, 0)),
        pl.BlockSpec((tile, 128), lambda i, off: (first + i, 0)),
    ]
    own = pl.BlockSpec((tile, depth), lambda i, off: (off[0] * blocks + first + i, 0))
    out_specs = [own, pl.BlockSpec((tile, depth), lambda i, off: (i, 0))]
    out_shape = [jax.ShapeDtypeStruct((2 * rows, depth), BF16), jax.ShapeDtypeStruct((rows // 2, depth), BF16)]
    args, aliases = [core, gqkv, wcat, gain, tok, means, inv_stds], {}
    if earlier is not None:
        dx, y, got = earlier
        args += [got, dx, y]
        wide = 2 * tile
        in_specs += [pl.BlockSpec((wide, depth), lambda i, off: (i, 0)), ANY, ANY]
        out_specs.append(pl.BlockSpec((wide, depth), lambda i, off: ((1 - off[0]) * steps + i, 0)))
        out_shape.append(jax.ShapeDtypeStruct(y.shape, BF16))
        aliases = {8: 0, 9: 2}
    return pl.pallas_call(
        functools.partial(grad_tok_kernel, earlier is not None),
        grid_spec=pltpu.PrefetchScalarGridSpec(num_scalar_prefetch=1, grid=(steps,), in_specs=in_specs, out_specs=out_specs),
        out_shape=out_shape,
        input_output_aliases=aliases,
        cost_estimate=pl.CostEstimate(flops=rows * depth * total, bytes_accessed=5 * rows * depth, transcendentals=0),
        compiler_params=pltpu.CompilerParams(vmem_limit_bytes=LIMIT),
    )(*args)


def fill_kernel(off, got, _, out):
    out[...] = got[...]


def fill(full, got, core, part, tile=1024):
    rows, width = got.shape
    blocks = rows // tile
    return pl.pallas_call(
        fill_kernel,
        grid_spec=pltpu.PrefetchScalarGridSpec(
            num_scalar_prefetch=1,
            grid=(blocks,),
            in_specs=[pl.BlockSpec((tile, width), lambda i, off: (i, 0)), ANY],
            out_specs=pl.BlockSpec((tile, width), lambda i, off: ((1 - off[0]) * 2 * blocks + part * blocks + i, 0)),
        ),
        out_shape=jax.ShapeDtypeStruct(full.shape, full.dtype),
        input_output_aliases={2: 0},
        cost_estimate=pl.CostEstimate(flops=rows * width, bytes_accessed=4 * rows * width, transcendentals=0),
        compiler_params=pltpu.CompilerParams(vmem_limit_bytes=LIMIT),
    )(core, got, full)


def after(value, *others):
    return lax.optimization_barrier((value,) + others)[0]


def solution(mesh):
    model_size = mesh.shape["model"]
    cores = [(i, i ^ 1) for i in range(model_size)]
    datas = [(0, 1), (1, 0)]
    sems = lambda n: pltpu.SemaphoreType.DMA((n,))

    def device_step(tok, wq_blk, wkv_blk, wo_blk, ln_gain, positions, grad):
        count, depth = tok.shape
        half = count // 2
        width = wq_blk.shape[1] * model_size
        pair = wkv_blk.shape[1]
        piece = width // model_size
        m = lax.axis_index("model")
        d = lax.axis_index("data")
        x, c = m // 2, m % 2
        gain = ln_gain.reshape(1, depth)
        core = c.reshape(1).astype(jnp.int32)
        index = lambda *v: jnp.stack([jnp.asarray(t, jnp.int32) for t in v])
        swap = lambda a: lax.ppermute(a, "model", cores)

        wcat, wo, hidden, means, inv_stds, proj = pl.pallas_call(
            functools.partial(front_kernel, half),
            in_specs=[ANY, VMEM, VMEM, VMEM, VMEM],
            out_specs=[ANY] * 6,
            out_shape=[
                jax.ShapeDtypeStruct((depth, width + pair), BF16),
                jax.ShapeDtypeStruct((width, depth), BF16),
                jax.ShapeDtypeStruct((half, depth), BF16),
                jax.ShapeDtypeStruct((half, 128), F32),
                jax.ShapeDtypeStruct((half, 128), F32),
                jax.ShapeDtypeStruct((half, width + pair), BF16),
            ],
            scratch_shapes=[sems(9), sems(9), sems(9), sems(9), sems(2), sems(2), sems(3)],
            compiler_params=pltpu.CompilerParams(collective_id=0, has_side_effects=True, vmem_limit_bytes=LIMIT),
        )(tok, wq_blk, wkv_blk, wo_blk, gain)

        grad_mixed = matmul(grad, wo, NT, half, core * (half // 1024))
        mixed, gqkv = attend(proj, grad_mixed, positions)

        deep = 2048
        mine, other = 2 * x + c, 2 * x + 1 - c
        row_o = c * (half // deep)
        give_o = wgrad(mixed, grad, index(other, row_o, 0, 0), (piece, depth), (piece, depth // 2, deep))
        got_o = swap(give_o)
        give_q = wgrad(after(hidden, give_o), gqkv, index(0, 0, other, 0), (depth, piece), (depth // 2, piece, deep))
        got_q = swap(give_q)
        part_kv = wgrad(after(hidden, give_q), gqkv, index(0, 0, width // pair, 0), (depth, pair), (depth // 2, pair, deep))
        send_o, keep_o = wgrad(after(mixed, part_kv), grad, index(mine, row_o, 0, d), (piece, depth), (piece, depth // 2, deep), got_o, 1)
        data_o = lax.ppermute(send_o, "data", datas)
        send_q, keep_q = wgrad(after(hidden, send_o), gqkv, index(0, 0, mine, d), (depth, piece), (depth // 2, piece, deep), got_q, 0)
        data_q = lax.ppermute(send_q, "data", datas)

        def halves(a, i, axis):
            size = a.shape[axis] // 2
            return lax.dynamic_slice_in_dim(a, i * size, size, axis), lax.dynamic_slice_in_dim(a, (1 - i) * size, size, axis)

        kv_keep, kv_give = halves(part_kv, c, 1)
        kv_sum = kv_keep + swap(kv_give)
        kv_keep, kv_give = halves(kv_sum, d, 0)
        kv_data = lax.ppermute(kv_give, "data", datas)

        y, y_send = project_out(after(mixed, send_q, kv_sum), wo, core)
        y_got = swap(y_send)
        kv_cols = (kv_keep + kv_data).astype(BF16)
        kv_other = swap(kv_cols)
        grad_w_out = (keep_o + data_o).astype(BF16)
        dx, dx_send = grad_tok(after(gqkv, y_send, grad_w_out, kv_cols), wcat, gain, tok, means, inv_stds, core, 0)
        dx_got_0 = swap(dx_send)
        grad_w_query = (keep_q + data_q).astype(BF16)
        grad_w_kv = jnp.where(c == 0, jnp.concatenate([kv_cols, kv_other], axis=1), jnp.concatenate([kv_other, kv_cols], axis=1))
        dx, dx_send, y = grad_tok(after(gqkv, dx_send, grad_w_query, grad_w_kv), wcat, gain, tok, means, inv_stds, core, 1, (dx, y, y_got))
        dx_got_1 = swap(dx_send)
        dx = fill(dx, dx_got_0, core, 0)
        dx = fill(dx, dx_got_1, core, 1)
        return y, dx, grad_w_query, grad_w_kv, grad_w_out

    return jax.shard_map(
        device_step,
        mesh=mesh,
        in_specs=(P("data", None), P("data", "model"), P("data", None), P("model", "data"), P(), P(), P("data", None)),
        out_specs=(P("data", None), P("data", None), P("data", "model"), P("data", None), P("model", "data")),
        check_vma=False,
    )
```

```python
import functools

import jax
import jax.numpy as jnp
from jax import lax
from jax.experimental import pallas as pl
from jax.experimental.pallas import tpu as pltpu
from jax.sharding import PartitionSpec as P


NORM_EPS = 1e-6
LOG2E = 1.4426950408889634
BF16, F32 = jnp.bfloat16, jnp.float32
NN = (((1,), (0,)), ((), ()))
NT = (((1,), (1,)), ((), ()))
TN = (((0,), (0,)), ((), ()))
MESH = pl.DeviceIdType.MESH
ANY = pl.BlockSpec(memory_space=pl.ANY)
VMEM = pl.BlockSpec(memory_space=pltpu.VMEM)
LIMIT = 62 * 2**20


def dot(a, b, dims):
    return lax.dot_general(a, b, dims, preferred_element_type=F32)


def place():
    d, m = lax.axis_index("data"), lax.axis_index("model")
    x, c = m // 2, m % 2
    return d, m, x, c, (1 - d, m), (d, 2 * (1 - x) + c), (d, 2 * x + (1 - c))


def entry_barrier(peers):
    barrier = pltpu.get_barrier_semaphore()
    for peer in peers:
        pl.semaphore_signal(barrier, inc=1, device_id=peer, device_id_type=MESH)
    pl.semaphore_wait(barrier, len(peers))


def remote(src, dst, send, recv, peer):
    return pltpu.make_async_remote_copy(src_ref=src, dst_ref=dst, send_sem=send, recv_sem=recv, device_id=peer, device_id_type=MESH)


class Gather:
    def __init__(self, piece, full, region, send, recv, local):
        self.piece, self.full, self.region = piece, full, region
        self.send, self.recv, self.local = send, recv, local

    def copies(self):
        d, m, x, c, yn, xn, pn = place()
        ym, xm = (1 - d, m), (d, 2 * (1 - x) + c)
        full, reg, s, r = self.full, self.region, self.send, self.recv
        at = lambda dm, part=None: full.at[reg(dm[0], dm[1], part)]
        diag = (1 - d, 2 * (1 - x) + c)
        own = at((d, m))
        first = [remote(self.piece, own, s.at[0], r.at[0], yn), remote(self.piece, own, s.at[1], r.at[1], xn), remote(self.piece, own, s.at[2], r.at[2], pn)]
        second = [
            remote(at(ym, 0), at(ym, 0), s.at[3], r.at[3], xn),
            remote(at(xm, 1), at(xm, 1), s.at[4], r.at[4], yn),
            remote(at(ym), at(ym), s.at[5], r.at[5], pn),
            remote(at(xm), at(xm), s.at[6], r.at[6], pn),
        ]
        third = [remote(at(diag, 0), at(diag, 0), s.at[7], r.at[7], pn), remote(at(diag, 1), at(diag, 1), s.at[8], r.at[8], pn)]
        mine = pltpu.make_async_copy(self.piece, own, self.local)
        return first, second, third, mine

    def start(self):
        first, _, _, mine = self.copies()
        for copy in first:
            copy.start()
        mine.start()

    def middle(self):
        first, second, _, _ = self.copies()
        first[1].wait_recv()
        second[1].start()
        second[3].start()
        first[0].wait_recv()
        second[0].start()
        second[2].start()

    def own_half(self):
        first, second, _, mine = self.copies()
        mine.wait()
        first[2].wait_recv()
        second[2].wait_recv()

    def finish(self):
        first, second, third, _ = self.copies()
        second[0].wait_recv()
        third[0].start()
        second[1].wait_recv()
        third[1].start()
        second[3].wait_recv()
        third[0].wait_recv()
        third[1].wait_recv()
        for copy in first + second + third:
            copy.wait_send()


def q_region(rows, cols, d, m, part):
    if part is None:
        return pl.ds(d * rows, rows), pl.ds(pl.multiple_of(m * cols, cols), cols)
    return pl.ds(d * rows + part * (rows // 2), rows // 2), pl.ds(pl.multiple_of(m * cols, cols), cols)


def o_region(rows, cols, d, m, part):
    if part is None:
        return pl.ds(m * rows, rows), pl.ds(pl.multiple_of(d * cols, cols), cols)
    return pl.ds(m * rows + part * (rows // 2), rows // 2), pl.ds(pl.multiple_of(d * cols, cols), cols)


def front_kernel(half, tok, wq, wkv, wo, gain, wcat, wo_full, hidden, means, inv_stds, proj, q_send, q_recv, o_send, o_recv, kv_send, kv_recv, local):
    d, _, x, c, yn, xn, pn = place()
    rows, cols = wq.shape
    depth, width = wo_full.shape[1], wo_full.shape[0]
    krows, pair = wkv.shape[0] // 2, wkv.shape[1]
    entry_barrier((yn, xn, pn))
    k_here = lambda dd, cc: wcat.at[pl.ds(dd * 2 * krows + cc * krows, krows), pl.ds(width, pair)]
    k_out = remote(wkv.at[pl.ds(c * krows, krows), :], k_here(d, c), kv_send.at[0], kv_recv.at[0], yn)
    k_fwd = remote(k_here(1 - d, c), k_here(1 - d, c), kv_send.at[1], kv_recv.at[1], pn)
    k_own = pltpu.make_async_copy(wkv, wcat.at[pl.ds(d * 2 * krows, 2 * krows), pl.ds(width, pair)], local.at[2])
    k_out.start()
    gather_q = Gather(wq, wcat, functools.partial(q_region, rows, cols), q_send, q_recv, local.at[0])
    gather_o = Gather(wo, wo_full, functools.partial(o_region, wo.shape[0], wo.shape[1]), o_send, o_recv, local.at[1])
    gather_q.start()
    k_own.start()

    def norm_block(tok_blk, hid_blk, mean_blk, inv_blk):
        rows_f = tok_blk[...].astype(F32)
        mean = jnp.mean(rows_f, axis=-1, keepdims=True)
        centred = rows_f - mean
        inv_std = lax.rsqrt(jnp.mean(centred * centred, axis=-1, keepdims=True) + NORM_EPS)
        hid_blk[...] = (centred * inv_std * gain[...]).astype(BF16)
        mean_blk[...] = jnp.broadcast_to(mean, mean_blk.shape)
        inv_blk[...] = jnp.broadcast_to(inv_std, inv_blk.shape)

    tile = 512
    pltpu.emit_pipeline(
        norm_block,
        grid=(half // tile,),
        in_specs=[pl.BlockSpec((tile, depth), lambda i: (i, 0))],
        out_specs=[pl.BlockSpec((tile, depth), lambda i: (i, 0))] + [pl.BlockSpec((tile, 128), lambda i: (i, 0))] * 2,
    )(tok.at[pl.ds(c * half, half), :], hidden, means, inv_stds)

    big = 1024

    def block(a, b, out):
        out[...] = dot(a[...], b[...], NN).astype(BF16)

    def run(col, cols_n, row_block, row_blocks):
        span = pl.ds(pl.multiple_of(col, cols_n), cols_n)
        pltpu.emit_pipeline(
            block,
            grid=(row_blocks,),
            in_specs=[pl.BlockSpec((big, depth), lambda i: (row_block + i, 0)), pl.BlockSpec((depth, cols_n), lambda i: (0, 0))],
            out_specs=[pl.BlockSpec((big, cols_n), lambda i: (row_block + i, 0))],
        )(hidden, wcat.at[:, span], proj.at[:, span])

    blocks = half // big
    k_out.wait_recv()
    k_fwd.start()
    k_own.wait()
    k_fwd.wait_recv()
    run(width, pair, 0, blocks)
    gather_q.middle()
    gather_o.start()
    gather_q.own_half()
    run(x * (width // 2), width // 2, 0, blocks)
    gather_q.finish()
    run((1 - x) * (width // 2), width // 2, 0, blocks // 2)
    gather_o.middle()
    run((1 - x) * (width // 2), width // 2, blocks // 2, blocks - blocks // 2)
    gather_o.own_half()
    gather_o.finish()
    k_out.wait_send()
    k_fwd.wait_send()


def mm_kernel(dims, off, a, b, out):
    out[...] = dot(a[...], b[...], dims).astype(BF16)


def matmul(a, b, dims, rows, row_block, tile=1024):
    depth = a.shape[1]
    width = b.shape[1] if dims == NN else b.shape[0]
    b_spec = pl.BlockSpec((depth, tile), lambda j, i, off: (0, j)) if dims == NN else pl.BlockSpec((tile, depth), lambda j, i, off: (j, 0))
    return pl.pallas_call(
        functools.partial(mm_kernel, dims),
        grid_spec=pltpu.PrefetchScalarGridSpec(
            num_scalar_prefetch=1,
            grid=(width // tile, rows // tile),
            in_specs=[pl.BlockSpec((tile, depth), lambda j, i, off: (off[0] + i, 0)), b_spec],
            out_specs=pl.BlockSpec((tile, tile), lambda j, i, off: (i, j)),
        ),
        out_shape=jax.ShapeDtypeStruct((rows, width), BF16),
        cost_estimate=pl.CostEstimate(flops=2 * rows * depth * width, bytes_accessed=2 * (rows * depth + depth * width + rows * width), transcendentals=0),
        compiler_params=pltpu.CompilerParams(vmem_limit_bytes=LIMIT),
    )(row_block, a, b)


def attend_kernel(heads, head_dim, qkv_ref, do_ref, pos_c_ref, pos_r_ref, o_ref, dqkv_ref, seen, pt, dst):
    seq, width = do_ref.shape
    q_ref, dq_ref = qkv_ref, dqkv_ref

    @pl.when(pl.program_id(0) == 0)
    def _():
        seen[...] = jnp.where(pos_c_ref[...] <= pos_r_ref[...], 1.0, -1.0)

    k, v = qkv_ref[:, width : width + head_dim], qkv_ref[:, width + head_dim :]
    kt, vt = k.T, v.T
    scale = head_dim ** -0.5
    cols = lambda h: slice(h * head_dim, (h + 1) * head_dim)
    lanes = lambda h: slice(h * seq, (h + 1) * seq)
    scores, grads, total = {}, {}, [None, None]

    def scored(h):
        scores[h] = dot(k, q_ref[:, cols(h)], NT)
        grads[h] = dot(v, do_ref[:, cols(h)], NT)

    def softmax(h):
        s = jnp.where(seen[...] > 0, scores.pop(h) * (scale * LOG2E), -1e30)
        e = jnp.exp2(s - jnp.max(s, axis=0, keepdims=True))
        p = e * (1.0 / jnp.sum(e, axis=0, keepdims=True))
        pt[:, lanes(h)] = p.astype(BF16)
        dp = grads.pop(h)
        dst[:, lanes(h)] = (p * (dp - jnp.sum(p * dp, axis=0, keepdims=True))).astype(BF16)

    def mixed(h):
        o_ref[:, cols(h)] = dot(vt, pt[:, lanes(h)], NN).T.astype(BF16)
        dq_ref[:, cols(h)] = (dot(kt, dst[:, lanes(h)], NN).T * scale).astype(BF16)
        dv = dot(pt[:, lanes(h)], do_ref[:, cols(h)], NN)
        dk = dot(dst[:, lanes(h)], q_ref[:, cols(h)], NN)
        total[0] = dk if total[0] is None else total[0] + dk
        total[1] = dv if total[1] is None else total[1] + dv

    for t in range(heads + 2):
        if t < heads:
            scored(t)
        if 0 <= t - 2:
            mixed(t - 2)
        if 0 <= t - 1 < heads:
            softmax(t - 1)
    dqkv_ref[:, width : width + head_dim] = (total[0] * scale).astype(BF16)
    dqkv_ref[:, width + head_dim :] = total[1].astype(BF16)


def attend(proj, grad_mixed, positions):
    rows, width = grad_mixed.shape
    seq, total = positions.shape[0], proj.shape[1]
    head_dim = (total - width) // 2
    heads = width // head_dim
    wide = pl.BlockSpec((seq, width), lambda i: (i, 0))
    wider = pl.BlockSpec((seq, total), lambda i: (i, 0))
    return pl.pallas_call(
        functools.partial(attend_kernel, heads, head_dim),
        grid=(rows // seq,),
        in_specs=[wider, wide, pl.BlockSpec((seq, 1), lambda i: (0, 0)), pl.BlockSpec((1, seq), lambda i: (0, 0))],
        out_specs=[wide, wider],
        out_shape=[jax.ShapeDtypeStruct((rows, width), BF16), jax.ShapeDtypeStruct((rows, total), BF16)],
        scratch_shapes=[pltpu.VMEM((seq, seq), F32), pltpu.VMEM((seq, heads * seq), BF16), pltpu.VMEM((seq, heads * seq), BF16)],
        cost_estimate=pl.CostEstimate(flops=12 * rows * seq * width, bytes_accessed=8 * rows * width, transcendentals=rows * seq * heads),
        compiler_params=pltpu.CompilerParams(vmem_limit_bytes=LIMIT),
    )(proj, grad_mixed, positions.reshape(seq, 1), positions.reshape(1, seq))


def give_kernel(off, a, b, out):
    part = dot(a[...], b[...], TN)

    @pl.when(pl.program_id(2) == 0)
    def _():
        out[...] = part

    @pl.when(pl.program_id(2) > 0)
    def _():
        out[...] += part


def keep_kernel(axis, off, a, b, got, send, keep):
    part = dot(a[...], b[...], TN)
    k = pl.program_id(2)

    def add(out):
        @pl.when(k == 0)
        def _():
            out[...] = got[...] + part

        @pl.when(k > 0)
        def _():
            out[...] += part

    pl.when(pl.program_id(axis) == 0)(lambda: add(send))
    pl.when(pl.program_id(axis) == 1)(lambda: add(keep))


def wgrad(a, b, offs, shape, tiles, got=None, axis=None):
    bm, bn, deep = tiles
    height, width = shape
    grid = (height // bm, width // bn, a.shape[0] // deep)
    half = lambda t, ax, off: jnp.where(t == 0, 1 - off[3], off[3]) if axis == ax else t
    in_specs = [
        pl.BlockSpec((deep, bm), lambda i, j, k, off: (k, off[0] + half(i, 0, off))),
        pl.BlockSpec((deep, bn), lambda i, j, k, off: (off[1] + k, off[2] + half(j, 1, off))),
    ]
    cost = pl.CostEstimate(flops=2 * a.shape[0] * height * width, bytes_accessed=2 * a.shape[0] * (height + width), transcendentals=0)
    params = pltpu.CompilerParams(vmem_limit_bytes=LIMIT)
    if got is None:
        return pl.pallas_call(
            give_kernel,
            grid_spec=pltpu.PrefetchScalarGridSpec(
                num_scalar_prefetch=1, grid=grid, in_specs=in_specs, out_specs=pl.BlockSpec((bm, bn), lambda i, j, k, off: (i, j))
            ),
            out_shape=jax.ShapeDtypeStruct(shape, F32),
            cost_estimate=cost,
            compiler_params=params,
        )(offs, a, b)
    piece = pl.BlockSpec((bm, bn), lambda i, j, k, off: (0, 0))
    return pl.pallas_call(
        functools.partial(keep_kernel, axis),
        grid_spec=pltpu.PrefetchScalarGridSpec(
            num_scalar_prefetch=1,
            grid=grid,
            in_specs=in_specs + [pl.BlockSpec((bm, bn), lambda i, j, k, off: (half(i, 0, off), half(j, 1, off)))],
            out_specs=[piece, piece],
        ),
        out_shape=[jax.ShapeDtypeStruct((bm, bn), F32)] * 2,
        cost_estimate=cost,
        compiler_params=params,
    )(offs, a, b, got)


def out_kernel(off, a, b, full, send):
    block = dot(a[...], b[...], NN).astype(BF16)
    full[...] = block
    send[...] = block


def project_out(mixed, wo, core, tile=1024):
    rows, depth = mixed.shape
    width = wo.shape[1]
    blocks = rows // tile
    return pl.pallas_call(
        out_kernel,
        grid_spec=pltpu.PrefetchScalarGridSpec(
            num_scalar_prefetch=1,
            grid=(width // tile, blocks),
            in_specs=[pl.BlockSpec((tile, depth), lambda j, i, off: (i, 0)), pl.BlockSpec((depth, tile), lambda j, i, off: (0, j))],
            out_specs=[pl.BlockSpec((tile, tile), lambda j, i, off: (off[0] * blocks + i, j)), pl.BlockSpec((tile, tile), lambda j, i, off: (i, j))],
        ),
        out_shape=[jax.ShapeDtypeStruct((2 * rows, width), BF16), jax.ShapeDtypeStruct((rows, width), BF16)],
        cost_estimate=pl.CostEstimate(flops=2 * rows * depth * width, bytes_accessed=2 * rows * (depth + 2 * width), transcendentals=0),
        compiler_params=pltpu.CompilerParams(vmem_limit_bytes=LIMIT),
    )(core, mixed, wo)


def grad_tok_kernel(passing, off, gqkv, wcat, gain, tok, means, inv_stds, *refs):
    if passing:
        got, _, _, full, send, y_full = refs
        y_full[...] = got[...]
    else:
        full, send = refs
    mean, inv_std = means[:, :1], inv_stds[:, :1]
    g = dot(gqkv[...], wcat[...], NT) * gain[...]
    normed = (tok[...].astype(F32) - mean) * inv_std
    block = (inv_std * (g - jnp.mean(g, axis=-1, keepdims=True) - normed * jnp.mean(g * normed, axis=-1, keepdims=True))).astype(BF16)
    full[...] = block
    send[...] = block


def grad_tok(gqkv, wcat, gain, tok, means, inv_stds, core, part, earlier=None, tile=512):
    rows, total = gqkv.shape
    depth = wcat.shape[0]
    blocks = rows // tile
    steps = blocks // 2
    first = part * steps
    whole = lambda i, off: (0, 0)
    once = pl.Buffered(1)
    in_specs = [
        pl.BlockSpec((tile, total), lambda i, off: (first + i, 0)),
        pl.BlockSpec((depth, total), whole, pipeline_mode=once),
        pl.BlockSpec((1, depth), whole, pipeline_mode=once),
        pl.BlockSpec((tile, depth), lambda i, off: (off[0] * blocks + first + i, 0)),
        pl.BlockSpec((tile, 128), lambda i, off: (first + i, 0)),
        pl.BlockSpec((tile, 128), lambda i, off: (first + i, 0)),
    ]
    own = pl.BlockSpec((tile, depth), lambda i, off: (off[0] * blocks + first + i, 0))
    out_specs = [own, pl.BlockSpec((tile, depth), lambda i, off: (i, 0))]
    out_shape = [jax.ShapeDtypeStruct((2 * rows, depth), BF16), jax.ShapeDtypeStruct((rows // 2, depth), BF16)]
    args, aliases = [core, gqkv, wcat, gain, tok, means, inv_stds], {}
    if earlier is not None:
        dx, y, got = earlier
        args += [got, dx, y]
        wide = 2 * tile
        in_specs += [pl.BlockSpec((wide, depth), lambda i, off: (i, 0)), ANY, ANY]
        out_specs.append(pl.BlockSpec((wide, depth), lambda i, off: ((1 - off[0]) * steps + i, 0)))
        out_shape.append(jax.ShapeDtypeStruct(y.shape, BF16))
        aliases = {8: 0, 9: 2}
    return pl.pallas_call(
        functools.partial(grad_tok_kernel, earlier is not None),
        grid_spec=pltpu.PrefetchScalarGridSpec(num_scalar_prefetch=1, grid=(steps,), in_specs=in_specs, out_specs=out_specs),
        out_shape=out_shape,
        input_output_aliases=aliases,
        cost_estimate=pl.CostEstimate(flops=rows * depth * total, bytes_accessed=5 * rows * depth, transcendentals=0),
        compiler_params=pltpu.CompilerParams(vmem_limit_bytes=LIMIT),
    )(*args)


def fill_kernel(off, got, _, out):
    out[...] = got[...]


def fill(full, got, core, part, tile=1024):
    rows, width = got.shape
    blocks = rows // tile
    return pl.pallas_call(
        fill_kernel,
        grid_spec=pltpu.PrefetchScalarGridSpec(
            num_scalar_prefetch=1,
            grid=(blocks,),
            in_specs=[pl.BlockSpec((tile, width), lambda i, off: (i, 0)), ANY],
            out_specs=pl.BlockSpec((tile, width), lambda i, off: ((1 - off[0]) * 2 * blocks + part * blocks + i, 0)),
        ),
        out_shape=jax.ShapeDtypeStruct(full.shape, full.dtype),
        input_output_aliases={2: 0},
        cost_estimate=pl.CostEstimate(flops=rows * width, bytes_accessed=4 * rows * width, transcendentals=0),
        compiler_params=pltpu.CompilerParams(vmem_limit_bytes=LIMIT),
    )(core, got, full)


def after(value, *others):
    return lax.optimization_barrier((value,) + others)[0]


def solution(mesh):
    model_size = mesh.shape["model"]
    cores = [(i, i ^ 1) for i in range(model_size)]
    datas = [(0, 1), (1, 0)]
    sems = lambda n: pltpu.SemaphoreType.DMA((n,))

    def layer(tok, wq_blk, wkv_blk, wo_blk, ln_gain, positions, grad):
        count, depth = tok.shape
        half = count // 2
        width = wq_blk.shape[1] * model_size
        pair = wkv_blk.shape[1]
        piece = width // model_size
        m = lax.axis_index("model")
        d = lax.axis_index("data")
        x, c = m // 2, m % 2
        gain = ln_gain.reshape(1, depth)
        core = c.reshape(1).astype(jnp.int32)
        index = lambda *v: jnp.stack([jnp.asarray(t, jnp.int32) for t in v])

        def swap(a):
            return lax.ppermute(a, "model", cores)

        def cross(a):
            return lax.ppermute(a, "data", datas)


        wcat, wo, hidden, means, inv_stds, proj = pl.pallas_call(
            functools.partial(front_kernel, half),
            in_specs=[ANY, VMEM, VMEM, VMEM, VMEM],
            out_specs=[ANY] * 6,
            out_shape=[
                jax.ShapeDtypeStruct((depth, width + pair), BF16),
                jax.ShapeDtypeStruct((width, depth), BF16),
                jax.ShapeDtypeStruct((half, depth), BF16),
                jax.ShapeDtypeStruct((half, 128), F32),
                jax.ShapeDtypeStruct((half, 128), F32),
                jax.ShapeDtypeStruct((half, width + pair), BF16),
            ],
            scratch_shapes=[sems(9), sems(9), sems(9), sems(9), sems(2), sems(2), sems(3)],
            compiler_params=pltpu.CompilerParams(collective_id=0, has_side_effects=True, vmem_limit_bytes=LIMIT),
        )(tok, wq_blk, wkv_blk, wo_blk, gain)

        grad_mixed = matmul(grad, wo, NT, half, core * (half // 1024))
        mixed, gqkv = attend(proj, grad_mixed, positions)

        deep = 2048
        mine, other = 2 * x + c, 2 * x + 1 - c
        row_o = c * (half // deep)
        give_o = wgrad(mixed, grad, index(other, row_o, 0, 0), (piece, depth), (piece, depth // 2, deep))
        got_o = swap(give_o)
        give_q = wgrad(after(hidden, give_o), gqkv, index(0, 0, other, 0), (depth, piece), (depth // 2, piece, deep))
        got_q = swap(give_q)
        part_kv = wgrad(after(hidden, give_q), gqkv, index(0, 0, width // pair, 0), (depth, pair), (depth // 2, pair, deep))
        send_o, keep_o = wgrad(after(mixed, part_kv), grad, index(mine, row_o, 0, d), (piece, depth), (piece, depth // 2, deep), got_o, 1)
        data_o = cross(send_o)
        send_q, keep_q = wgrad(after(hidden, send_o), gqkv, index(0, 0, mine, d), (depth, piece), (depth // 2, piece, deep), got_q, 0)
        data_q = cross(send_q)

        def halves(a, i, axis):
            size = a.shape[axis] // 2
            return lax.dynamic_slice_in_dim(a, i * size, size, axis), lax.dynamic_slice_in_dim(a, (1 - i) * size, size, axis)

        kv_keep, kv_give = halves(part_kv, c, 1)
        kv_sum = kv_keep + swap(kv_give)
        kv_keep, kv_give = halves(kv_sum, d, 0)
        kv_data = cross(kv_give)

        y, y_send = project_out(after(mixed, send_q, kv_sum), wo, core)
        y_got = swap(y_send)
        kv_cols = (kv_keep + kv_data).astype(BF16)
        kv_other = swap(kv_cols)
        grad_w_out = (keep_o + data_o).astype(BF16)
        dx, dx_send = grad_tok(after(gqkv, y_send, grad_w_out, kv_cols), wcat, gain, tok, means, inv_stds, core, 0)
        dx_got_0 = swap(dx_send)
        grad_w_query = (keep_q + data_q).astype(BF16)
        grad_w_kv = jnp.where(c == 0, jnp.concatenate([kv_cols, kv_other], axis=1), jnp.concatenate([kv_other, kv_cols], axis=1))
        dx, dx_send, y = grad_tok(after(gqkv, dx_send, grad_w_query, grad_w_kv), wcat, gain, tok, means, inv_stds, core, 1, (dx, y, y_got))
        dx_got_1 = swap(dx_send)
        dx = fill(dx, dx_got_0, core, 0)
        dx = fill(dx, dx_got_1, core, 1)
        return y, dx, grad_w_query, grad_w_kv, grad_w_out

    return jax.shard_map(
        layer,
        mesh=mesh,
        in_specs=(P("data", None), P("data", "model"), P("data", None), P("model", "data"), P(), P(), P("data", None)),
        out_specs=(P("data", None), P("data", None), P("data", "model"), P("data", None), P("model", "data")),
        check_vma=False,
    )
```

```python
import functools

import jax
import jax.numpy as jnp
from jax import lax
from jax.experimental import pallas as pl
from jax.experimental.pallas import tpu as pltpu
from jax.sharding import PartitionSpec as P


NORM_EPS = 1e-6
LOG2E = 1.4426950408889634
BF16, F32 = jnp.bfloat16, jnp.float32
NN = (((1,), (0,)), ((), ()))
NT = (((1,), (1,)), ((), ()))
TN = (((0,), (0,)), ((), ()))
MESH = pl.DeviceIdType.MESH
ANY = pl.BlockSpec(memory_space=pl.ANY)
VMEM = pl.BlockSpec(memory_space=pltpu.VMEM)
LIMIT = 62 * 2**20


def dot(a, b, dims):
    return lax.dot_general(a, b, dims, preferred_element_type=F32)


def place():
    d, m = lax.axis_index("data"), lax.axis_index("model")
    x, c = m // 2, m % 2
    return d, m, x, c, (1 - d, m), (d, 2 * (1 - x) + c), (d, 2 * x + (1 - c))


def entry_barrier(peers):
    barrier = pltpu.get_barrier_semaphore()
    for peer in peers:
        pl.semaphore_signal(barrier, inc=1, device_id=peer, device_id_type=MESH)
    pl.semaphore_wait(barrier, len(peers))


def remote(src, dst, send, recv, peer):
    return pltpu.make_async_remote_copy(src_ref=src, dst_ref=dst, send_sem=send, recv_sem=recv, device_id=peer, device_id_type=MESH)


class Gather:
    def __init__(self, piece, full, region, send, recv, local):
        self.piece, self.full, self.region = piece, full, region
        self.send, self.recv, self.local = send, recv, local

    def copies(self):
        d, m, x, c, yn, xn, pn = place()
        ym, xm = (1 - d, m), (d, 2 * (1 - x) + c)
        full, reg, s, r = self.full, self.region, self.send, self.recv
        at = lambda dm, part=None: full.at[reg(dm[0], dm[1], part)]
        diag = (1 - d, 2 * (1 - x) + c)
        own = at((d, m))
        first = [remote(self.piece, own, s.at[0], r.at[0], yn), remote(self.piece, own, s.at[1], r.at[1], xn), remote(self.piece, own, s.at[2], r.at[2], pn)]
        second = [
            remote(at(ym, 0), at(ym, 0), s.at[3], r.at[3], xn),
            remote(at(xm, 1), at(xm, 1), s.at[4], r.at[4], yn),
            remote(at(ym), at(ym), s.at[5], r.at[5], pn),
            remote(at(xm), at(xm), s.at[6], r.at[6], pn),
        ]
        third = [remote(at(diag, 0), at(diag, 0), s.at[7], r.at[7], pn), remote(at(diag, 1), at(diag, 1), s.at[8], r.at[8], pn)]
        mine = pltpu.make_async_copy(self.piece, own, self.local)
        return first, second, third, mine

    def start(self):
        first, _, _, mine = self.copies()
        for copy in first:
            copy.start()
        mine.start()

    def middle(self):
        first, second, _, _ = self.copies()
        first[1].wait_recv()
        second[1].start()
        second[3].start()
        first[0].wait_recv()
        second[0].start()
        second[2].start()

    def own_half(self):
        first, second, _, mine = self.copies()
        mine.wait()
        first[2].wait_recv()
        second[2].wait_recv()

    def finish(self):
        first, second, third, _ = self.copies()
        second[0].wait_recv()
        third[0].start()
        second[1].wait_recv()
        third[1].start()
        second[3].wait_recv()
        third[0].wait_recv()
        third[1].wait_recv()
        for copy in first + second + third:
            copy.wait_send()


def q_region(rows, cols, d, m, part):
    if part is None:
        return pl.ds(d * rows, rows), pl.ds(pl.multiple_of(m * cols, cols), cols)
    return pl.ds(d * rows + part * (rows // 2), rows // 2), pl.ds(pl.multiple_of(m * cols, cols), cols)


def o_region(rows, cols, d, m, part):
    if part is None:
        return pl.ds(m * rows, rows), pl.ds(pl.multiple_of(d * cols, cols), cols)
    return pl.ds(m * rows + part * (rows // 2), rows // 2), pl.ds(pl.multiple_of(d * cols, cols), cols)


def front_kernel(half, tok, grad, wq, wkv, wo, gain, wcat, wo_full, hidden, means, inv_stds, proj, grad_mixed, wbuf, obuf, kbuf, q_send, q_recv, o_send, o_recv, kv_send, kv_recv, local):
    d, _, x, c, yn, xn, pn = place()
    rows, cols = wq.shape
    depth, width = wo_full.shape[1], wo_full.shape[0]
    krows, pair = wkv.shape[0] // 2, wkv.shape[1]
    part = width // 2
    entry_barrier((yn, xn, pn))
    k_here = lambda dd, cc: wcat.at[pl.ds(dd * 2 * krows + cc * krows, krows), pl.ds(width, pair)]
    k_out = remote(wkv.at[pl.ds(c * krows, krows), :], k_here(d, c), kv_send.at[0], kv_recv.at[0], yn)
    k_fwd = remote(k_here(1 - d, c), k_here(1 - d, c), kv_send.at[1], kv_recv.at[1], pn)
    k_own = pltpu.make_async_copy(wkv, wcat.at[pl.ds(d * 2 * krows, 2 * krows), pl.ds(width, pair)], local.at[2])
    gather_q = Gather(wq, wcat, functools.partial(q_region, rows, cols), q_send, q_recv, local.at[0])
    gather_o = Gather(wo, wo_full, functools.partial(o_region, wo.shape[0], wo.shape[1]), o_send, o_recv, local.at[1])
    gather_q.start()
    k_out.start()
    k_own.start()
    mine = lambda *_: pl.ds(pl.multiple_of(x * part, part), part)
    other = lambda *_: pl.ds(pl.multiple_of((1 - x) * part, part), part)
    load_q0 = pltpu.make_async_copy(wcat.at[:, mine()], wbuf.at[0], local.at[3])
    load_q1 = pltpu.make_async_copy(wcat.at[:, other()], wbuf.at[1], local.at[4])
    load_kv = pltpu.make_async_copy(wcat.at[:, pl.ds(width, pair)], kbuf, local.at[5])
    load_o0 = pltpu.make_async_copy(wo_full.at[mine(), :], obuf.at[0], local.at[6])
    load_o1 = pltpu.make_async_copy(wo_full.at[other(), :], obuf.at[1], local.at[7])

    def norm_block(tok_blk, hid_blk, mean_blk, inv_blk):
        rows_f = tok_blk[...].astype(F32)
        mean = jnp.mean(rows_f, axis=-1, keepdims=True)
        centred = rows_f - mean
        inv_std = lax.rsqrt(jnp.mean(centred * centred, axis=-1, keepdims=True) + NORM_EPS)
        hid_blk[...] = (centred * inv_std * gain[...]).astype(BF16)
        mean_blk[...] = jnp.broadcast_to(mean, mean_blk.shape)
        inv_blk[...] = jnp.broadcast_to(inv_std, inv_blk.shape)

    tile = 512
    pltpu.emit_pipeline(
        norm_block,
        grid=(half // tile,),
        in_specs=[pl.BlockSpec((tile, depth), lambda i: (i, 0))],
        out_specs=[pl.BlockSpec((tile, depth), lambda i: (i, 0))] + [pl.BlockSpec((tile, 128), lambda i: (i, 0))] * 2,
    )(tok.at[pl.ds(c * half, half), :], hidden, means, inv_stds)

    big = 1024

    def run(src, weight, dims, out):
        def block(a, o):
            o[...] = dot(a[...], weight[...], dims).astype(BF16)

        pltpu.emit_pipeline(
            block,
            grid=(half // big,),
            in_specs=[pl.BlockSpec((big, depth), lambda i: (i, 0))],
            out_specs=[pl.BlockSpec((big, out.shape[1]), lambda i: (i, 0))],
        )(src, out)

    gather_q.middle()
    gather_o.start()
    gather_q.own_half()
    load_q0.start()
    k_out.wait_recv()
    k_fwd.start()
    k_own.wait()
    load_q0.wait()
    run(hidden, wbuf.at[0], NN, proj.at[:, mine()])
    gather_q.finish()
    load_q1.start()
    k_fwd.wait_recv()
    load_kv.start()
    load_kv.wait()
    run(hidden, kbuf, NN, proj.at[:, pl.ds(width, pair)])
    load_q1.wait()
    run(hidden, wbuf.at[1], NN, proj.at[:, other()])
    gather_o.middle()
    gather_o.own_half()
    load_o0.start()
    load_o0.wait()
    own_grad = grad.at[pl.ds(c * half, half), :]
    run(own_grad, obuf.at[0], NT, grad_mixed.at[:, mine()])
    gather_o.finish()
    load_o1.start()
    load_o1.wait()
    run(own_grad, obuf.at[1], NT, grad_mixed.at[:, other()])
    k_out.wait_send()
    k_fwd.wait_send()


def attend_kernel(heads, head_dim, qkv_ref, do_ref, pos_c_ref, pos_r_ref, o_ref, dqkv_ref, seen, pt, dst):
    seq, width = do_ref.shape
    q_ref, dq_ref = qkv_ref, dqkv_ref

    @pl.when(pl.program_id(0) == 0)
    def _():
        seen[...] = jnp.where(pos_c_ref[...] <= pos_r_ref[...], 1.0, -1.0)

    k, v = qkv_ref[:, width : width + head_dim], qkv_ref[:, width + head_dim :]
    kt, vt = k.T, v.T
    scale = head_dim ** -0.5
    cols = lambda h: slice(h * head_dim, (h + 1) * head_dim)
    lanes = lambda h: slice(h * seq, (h + 1) * seq)
    scores, grads, total = {}, {}, [None, None]

    def scored(h):
        scores[h] = dot(k, q_ref[:, cols(h)], NT)
        grads[h] = dot(v, do_ref[:, cols(h)], NT)

    def softmax(h):
        s = jnp.where(seen[...] > 0, scores.pop(h) * (scale * LOG2E), -1e30)
        e = jnp.exp2(s - jnp.max(s, axis=0, keepdims=True))
        p = e * (1.0 / jnp.sum(e, axis=0, keepdims=True))
        pt[:, lanes(h)] = p.astype(BF16)
        dp = grads.pop(h)
        dst[:, lanes(h)] = (p * (dp - jnp.sum(p * dp, axis=0, keepdims=True))).astype(BF16)

    def mixed(h):
        o_ref[:, cols(h)] = dot(vt, pt[:, lanes(h)], NN).T.astype(BF16)
        dq_ref[:, cols(h)] = (dot(kt, dst[:, lanes(h)], NN).T * scale).astype(BF16)
        dv = dot(pt[:, lanes(h)], do_ref[:, cols(h)], NN)
        dk = dot(dst[:, lanes(h)], q_ref[:, cols(h)], NN)
        total[0] = dk if total[0] is None else total[0] + dk
        total[1] = dv if total[1] is None else total[1] + dv

    for t in range(heads + 2):
        if t < heads:
            scored(t)
        if 0 <= t - 2:
            mixed(t - 2)
        if 0 <= t - 1 < heads:
            softmax(t - 1)
    dqkv_ref[:, width : width + head_dim] = (total[0] * scale).astype(BF16)
    dqkv_ref[:, width + head_dim :] = total[1].astype(BF16)


def attend(proj, grad_mixed, positions):
    rows, width = grad_mixed.shape
    seq, total = positions.shape[0], proj.shape[1]
    head_dim = (total - width) // 2
    heads = width // head_dim
    wide = pl.BlockSpec((seq, width), lambda i: (i, 0))
    wider = pl.BlockSpec((seq, total), lambda i: (i, 0))
    return pl.pallas_call(
        functools.partial(attend_kernel, heads, head_dim),
        grid=(rows // seq,),
        in_specs=[wider, wide, pl.BlockSpec((seq, 1), lambda i: (0, 0)), pl.BlockSpec((1, seq), lambda i: (0, 0))],
        out_specs=[wide, wider],
        out_shape=[jax.ShapeDtypeStruct((rows, width), BF16), jax.ShapeDtypeStruct((rows, total), BF16)],
        scratch_shapes=[pltpu.VMEM((seq, seq), F32), pltpu.VMEM((seq, heads * seq), BF16), pltpu.VMEM((seq, heads * seq), BF16)],
        cost_estimate=pl.CostEstimate(flops=12 * rows * seq * width, bytes_accessed=8 * rows * width, transcendentals=rows * seq * heads),
        compiler_params=pltpu.CompilerParams(vmem_limit_bytes=LIMIT),
    )(proj, grad_mixed, positions.reshape(seq, 1), positions.reshape(1, seq))


def give_kernel(count, off, a, *refs):
    for b, out in zip(refs[:count], refs[count:]):
        out[...] = dot(a[...], b[...], TN)


def give(a, bs, offs, shape, widths, tile=512):
    rows = a.shape[0]
    height, width = shape
    wide = width // tile
    blocks = [tile] + list(widths[1:])
    b_specs = [pl.BlockSpec((rows, w), functools.partial(lambda n, i, j, off: (off[1], off[2 + n] + (j if n == 0 else 0)), n)) for n, w in enumerate(blocks)]
    o_specs = [pl.BlockSpec((tile, w), functools.partial(lambda n, i, j, off: (i, j if n == 0 else 0), n)) for n, w in enumerate(blocks)]
    return pl.pallas_call(
        functools.partial(give_kernel, len(bs)),
        grid_spec=pltpu.PrefetchScalarGridSpec(
            num_scalar_prefetch=1,
            grid=(height // tile, wide),
            in_specs=[pl.BlockSpec((rows, tile), lambda i, j, off: (0, off[0] + i))] + b_specs,
            out_specs=o_specs,
        ),
        out_shape=[jax.ShapeDtypeStruct((height, w), F32) for w in widths],
        cost_estimate=pl.CostEstimate(flops=2 * rows * height * sum(widths), bytes_accessed=2 * rows * (height + sum(widths)), transcendentals=0),
        compiler_params=pltpu.CompilerParams(vmem_limit_bytes=LIMIT),
    )(offs, a, *bs)


def keep_kernel(half, off, a, b, got, send, keep):
    step = pl.program_id(0)
    value = got[...] + dot(a[...], b[...], TN)

    @pl.when(step < half)
    def _():
        send[...] = value

    @pl.when(step >= half)
    def _():
        keep[...] = value


def keep(a, b, offs, shape, axis, got, tile=512):
    rows = a.shape[0]
    steps = shape[axis] // tile
    half = steps // 2
    turn = lambda t, off: jnp.where(t < half, (1 - off[3]) * half + t, off[3] * half + t - half)
    at = (lambda t, off: (turn(t, off), 0)) if axis == 0 else (lambda t, off: (0, turn(t, off)))
    line = (lambda t: (t, 0)) if axis == 0 else (lambda t: (0, t))
    out = (shape[0] // 2, shape[1]) if axis == 0 else (shape[0], shape[1] // 2)
    return pl.pallas_call(
        functools.partial(keep_kernel, half),
        grid_spec=pltpu.PrefetchScalarGridSpec(
            num_scalar_prefetch=1,
            grid=(steps,),
            in_specs=[
                pl.BlockSpec((rows, tile), lambda t, off: (0, off[0] + at(t, off)[0])),
                pl.BlockSpec((rows, tile), lambda t, off: (off[1], off[2] + at(t, off)[1])),
                pl.BlockSpec((tile, tile), at),
            ],
            out_specs=[
                pl.BlockSpec((tile, tile), lambda t, off: line(jnp.minimum(t, half - 1))),
                pl.BlockSpec((tile, tile), lambda t, off: line(jnp.maximum(t - half, 0))),
            ],
        ),
        out_shape=[jax.ShapeDtypeStruct(out, F32)] * 2,
        cost_estimate=pl.CostEstimate(flops=2 * rows * shape[0] * shape[1], bytes_accessed=2 * rows * sum(shape), transcendentals=0),
        compiler_params=pltpu.CompilerParams(vmem_limit_bytes=LIMIT),
    )(offs, a, b, got)


def out_kernel(off, a, b, full, send):
    block = dot(a[...], b[...], NN).astype(BF16)
    full[...] = block
    send[...] = block


def project_out(mixed, wo, core, tile=1024):
    rows, depth = mixed.shape
    width = wo.shape[1]
    blocks = rows // tile
    return pl.pallas_call(
        out_kernel,
        grid_spec=pltpu.PrefetchScalarGridSpec(
            num_scalar_prefetch=1,
            grid=(width // tile, blocks),
            in_specs=[pl.BlockSpec((tile, depth), lambda j, i, off: (i, 0)), pl.BlockSpec((depth, tile), lambda j, i, off: (0, j))],
            out_specs=[pl.BlockSpec((tile, tile), lambda j, i, off: (off[0] * blocks + i, j)), pl.BlockSpec((tile, tile), lambda j, i, off: (i, j))],
        ),
        out_shape=[jax.ShapeDtypeStruct((2 * rows, width), BF16), jax.ShapeDtypeStruct((rows, width), BF16)],
        cost_estimate=pl.CostEstimate(flops=2 * rows * depth * width, bytes_accessed=2 * rows * (depth + 2 * width), transcendentals=0),
        compiler_params=pltpu.CompilerParams(vmem_limit_bytes=LIMIT),
    )(core, mixed, wo)


def grad_tok_kernel(passing, off, gqkv, wcat, gain, tok, means, inv_stds, *refs):
    if passing:
        got, _, _, full, send, y_full = refs
        y_full[...] = got[...]
    else:
        full, send = refs
    mean, inv_std = means[:, :1], inv_stds[:, :1]
    g = dot(gqkv[...], wcat[...], NT) * gain[...]
    normed = (tok[...].astype(F32) - mean) * inv_std
    block = (inv_std * (g - jnp.mean(g, axis=-1, keepdims=True) - normed * jnp.mean(g * normed, axis=-1, keepdims=True))).astype(BF16)
    full[...] = block
    send[...] = block


def grad_tok(gqkv, wcat, gain, tok, means, inv_stds, core, part, earlier=None, tile=512):
    rows, total = gqkv.shape
    depth = wcat.shape[0]
    blocks = rows // tile
    steps = blocks // 2
    first = part * steps
    whole = lambda i, off: (0, 0)
    once = pl.Buffered(1)
    in_specs = [
        pl.BlockSpec((tile, total), lambda i, off: (first + i, 0)),
        pl.BlockSpec((depth, total), whole, pipeline_mode=once),
        pl.BlockSpec((1, depth), whole, pipeline_mode=once),
        pl.BlockSpec((tile, depth), lambda i, off: (off[0] * blocks + first + i, 0)),
        pl.BlockSpec((tile, 128), lambda i, off: (first + i, 0)),
        pl.BlockSpec((tile, 128), lambda i, off: (first + i, 0)),
    ]
    own = pl.BlockSpec((tile, depth), lambda i, off: (off[0] * blocks + first + i, 0))
    out_specs = [own, pl.BlockSpec((tile, depth), lambda i, off: (i, 0))]
    out_shape = [jax.ShapeDtypeStruct((2 * rows, depth), BF16), jax.ShapeDtypeStruct((rows // 2, depth), BF16)]
    args, aliases = [core, gqkv, wcat, gain, tok, means, inv_stds], {}
    if earlier is not None:
        dx, y, got = earlier
        args += [got, dx, y]
        wide = 2 * tile
        in_specs += [pl.BlockSpec((wide, depth), lambda i, off: (i, 0)), ANY, ANY]
        out_specs.append(pl.BlockSpec((wide, depth), lambda i, off: ((1 - off[0]) * steps + i, 0)))
        out_shape.append(jax.ShapeDtypeStruct(y.shape, BF16))
        aliases = {8: 0, 9: 2}
    return pl.pallas_call(
        functools.partial(grad_tok_kernel, earlier is not None),
        grid_spec=pltpu.PrefetchScalarGridSpec(num_scalar_prefetch=1, grid=(steps,), in_specs=in_specs, out_specs=out_specs),
        out_shape=out_shape,
        input_output_aliases=aliases,
        cost_estimate=pl.CostEstimate(flops=rows * depth * total, bytes_accessed=5 * rows * depth, transcendentals=0),
        compiler_params=pltpu.CompilerParams(vmem_limit_bytes=LIMIT),
    )(*args)


def fill_kernel(off, got, _, out):
    out[...] = got[...]


def fill(full, got, core, part, tile=1024):
    rows, width = got.shape
    blocks = rows // tile
    return pl.pallas_call(
        fill_kernel,
        grid_spec=pltpu.PrefetchScalarGridSpec(
            num_scalar_prefetch=1,
            grid=(blocks,),
            in_specs=[pl.BlockSpec((tile, width), lambda i, off: (i, 0)), ANY],
            out_specs=pl.BlockSpec((tile, width), lambda i, off: ((1 - off[0]) * 2 * blocks + part * blocks + i, 0)),
        ),
        out_shape=jax.ShapeDtypeStruct(full.shape, full.dtype),
        input_output_aliases={2: 0},
        cost_estimate=pl.CostEstimate(flops=rows * width, bytes_accessed=4 * rows * width, transcendentals=0),
        compiler_params=pltpu.CompilerParams(vmem_limit_bytes=LIMIT),
    )(core, got, full)


def after(value, *others):
    return lax.optimization_barrier((value,) + others)[0]


def solution(mesh):
    model_size = mesh.shape["model"]
    cores = [(i, i ^ 1) for i in range(model_size)]
    datas = [(0, 1), (1, 0)]
    sems = lambda n: pltpu.SemaphoreType.DMA((n,))

    def layer(tok, wq_blk, wkv_blk, wo_blk, ln_gain, positions, grad):
        count, depth = tok.shape
        half = count // 2
        width = wq_blk.shape[1] * model_size
        pair = wkv_blk.shape[1]
        piece = width // model_size
        m = lax.axis_index("model")
        d = lax.axis_index("data")
        x, c = m // 2, m % 2
        gain = ln_gain.reshape(1, depth)
        core = c.reshape(1).astype(jnp.int32)
        index = lambda *v: jnp.stack([jnp.asarray(t, jnp.int32) for t in v])

        def swap(a):
            return lax.ppermute(a, "model", cores)

        def cross(a):
            return lax.ppermute(a, "data", datas)


        wcat, wo, hidden, means, inv_stds, proj, grad_mixed = pl.pallas_call(
            functools.partial(front_kernel, half),
            in_specs=[ANY, ANY, VMEM, VMEM, VMEM, VMEM],
            out_specs=[ANY] * 7,
            out_shape=[
                jax.ShapeDtypeStruct((depth, width + pair), BF16),
                jax.ShapeDtypeStruct((width, depth), BF16),
                jax.ShapeDtypeStruct((half, depth), BF16),
                jax.ShapeDtypeStruct((half, 128), F32),
                jax.ShapeDtypeStruct((half, 128), F32),
                jax.ShapeDtypeStruct((half, width + pair), BF16),
                jax.ShapeDtypeStruct((half, width), BF16),
            ],
            scratch_shapes=[pltpu.VMEM((2, depth, width // 2), BF16), pltpu.VMEM((2, width // 2, depth), BF16), pltpu.VMEM((depth, pair), BF16)]
            + [sems(9), sems(9), sems(9), sems(9), sems(2), sems(2), sems(8)],
            compiler_params=pltpu.CompilerParams(collective_id=0, has_side_effects=True, vmem_limit_bytes=LIMIT),
        )(tok, grad, wq_blk, wkv_blk, wo_blk, gain)

        mixed, gqkv = attend(proj, grad_mixed, positions)

        mine, other = 2 * x + c, 2 * x + 1 - c
        (give_o,) = give(mixed, [grad], index(other, c, 0), (piece, depth), [depth])
        got_o = swap(give_o)
        give_q, part_kv = give(after(hidden, give_o), [gqkv, gqkv], index(0, 0, other, width // pair), (depth, piece), [piece, pair])
        got_q = swap(give_q)
        send_o, keep_o = keep(after(mixed, give_q), grad, index(mine, c, 0, d), (piece, depth), 1, got_o)
        data_o = cross(send_o)
        send_q, keep_q = keep(after(hidden, send_o), gqkv, index(0, 0, mine, d), (depth, piece), 0, got_q)
        data_q = cross(send_q)

        def halves(a, i, axis):
            size = a.shape[axis] // 2
            return lax.dynamic_slice_in_dim(a, i * size, size, axis), lax.dynamic_slice_in_dim(a, (1 - i) * size, size, axis)

        kv_keep, kv_give = halves(after(part_kv, send_o), c, 1)
        kv_sum = kv_keep + swap(kv_give)
        kv_keep, kv_give = halves(kv_sum, d, 0)
        kv_data = cross(kv_give)

        y, y_send = project_out(after(mixed, send_q, kv_sum), wo, core)
        y_got = swap(y_send)
        kv_cols = (kv_keep + kv_data).astype(BF16)
        kv_other = swap(kv_cols)
        grad_w_out = (keep_o + data_o).astype(BF16)
        dx, dx_send = grad_tok(after(gqkv, y_send, grad_w_out, kv_cols), wcat, gain, tok, means, inv_stds, core, 0)
        dx_got_0 = swap(dx_send)
        grad_w_query = (keep_q + data_q).astype(BF16)
        grad_w_kv = jnp.where(c == 0, jnp.concatenate([kv_cols, kv_other], axis=1), jnp.concatenate([kv_other, kv_cols], axis=1))
        dx, dx_send, y = grad_tok(after(gqkv, dx_send, grad_w_query), wcat, gain, tok, means, inv_stds, core, 1, (dx, y, y_got))
        dx_got_1 = swap(dx_send)
        dx = fill(dx, dx_got_0, core, 0)
        dx = fill(dx, dx_got_1, core, 1)
        return y, dx, grad_w_query, grad_w_kv, grad_w_out

    return jax.shard_map(
        layer,
        mesh=mesh,
        in_specs=(P("data", None), P("data", "model"), P("data", None), P("model", "data"), P(), P(), P("data", None)),
        out_specs=(P("data", None), P("data", None), P("data", "model"), P("data", None), P("model", "data")),
        check_vma=False,
    )
```

```python
import functools

import jax
import jax.numpy as jnp
from jax import lax
from jax.experimental import pallas as pl
from jax.experimental.pallas import tpu as pltpu
from jax.sharding import PartitionSpec as P


NORM_EPS = 1e-6
LOG2E = 1.4426950408889634
BF16, F32 = jnp.bfloat16, jnp.float32
NN = (((1,), (0,)), ((), ()))
NT = (((1,), (1,)), ((), ()))
TN = (((0,), (0,)), ((), ()))
MESH = pl.DeviceIdType.MESH
ANY = pl.BlockSpec(memory_space=pl.ANY)
VMEM = pl.BlockSpec(memory_space=pltpu.VMEM)
LIMIT = 62 * 2**20


def dot(a, b, dims):
    return lax.dot_general(a, b, dims, preferred_element_type=F32)


def place():
    d, m = lax.axis_index("data"), lax.axis_index("model")
    x, c = m // 2, m % 2
    return d, m, x, c, (1 - d, m), (d, 2 * (1 - x) + c), (d, 2 * x + (1 - c))


def entry_barrier(peers):
    barrier = pltpu.get_barrier_semaphore()
    for peer in peers:
        pl.semaphore_signal(barrier, inc=1, device_id=peer, device_id_type=MESH)
    pl.semaphore_wait(barrier, len(peers))


def remote(src, dst, send, recv, peer):
    return pltpu.make_async_remote_copy(src_ref=src, dst_ref=dst, send_sem=send, recv_sem=recv, device_id=peer, device_id_type=MESH)


class Gather:
    def __init__(self, piece, full, region, send, recv, local):
        self.piece, self.full, self.region = piece, full, region
        self.send, self.recv, self.local = send, recv, local

    def copies(self):
        d, m, x, c, yn, xn, pn = place()
        ym, xm = (1 - d, m), (d, 2 * (1 - x) + c)
        full, reg, s, r = self.full, self.region, self.send, self.recv
        at = lambda dm, part=None: full.at[reg(dm[0], dm[1], part)]
        diag = (1 - d, 2 * (1 - x) + c)
        own = at((d, m))
        first = [remote(self.piece, own, s.at[0], r.at[0], yn), remote(self.piece, own, s.at[1], r.at[1], xn), remote(self.piece, own, s.at[2], r.at[2], pn)]
        second = [
            remote(at(ym, 0), at(ym, 0), s.at[3], r.at[3], xn),
            remote(at(xm, 1), at(xm, 1), s.at[4], r.at[4], yn),
            remote(at(ym), at(ym), s.at[5], r.at[5], pn),
            remote(at(xm), at(xm), s.at[6], r.at[6], pn),
        ]
        third = [remote(at(diag, 0), at(diag, 0), s.at[7], r.at[7], pn), remote(at(diag, 1), at(diag, 1), s.at[8], r.at[8], pn)]
        mine = pltpu.make_async_copy(self.piece, own, self.local)
        return first, second, third, mine

    def start(self):
        first, _, _, mine = self.copies()
        for copy in first:
            copy.start()
        mine.start()

    def middle(self):
        first, second, _, _ = self.copies()
        first[1].wait_recv()
        second[1].start()
        second[3].start()
        first[0].wait_recv()
        second[0].start()
        second[2].start()

    def own_half(self):
        first, second, _, mine = self.copies()
        mine.wait()
        first[2].wait_recv()
        second[2].wait_recv()

    def finish(self):
        first, second, third, _ = self.copies()
        second[0].wait_recv()
        third[0].start()
        second[1].wait_recv()
        third[1].start()
        second[3].wait_recv()
        third[0].wait_recv()
        third[1].wait_recv()
        for copy in first + second + third:
            copy.wait_send()


def q_region(rows, cols, d, m, part):
    if part is None:
        return pl.ds(d * rows, rows), pl.ds(pl.multiple_of(m * cols, cols), cols)
    return pl.ds(d * rows + part * (rows // 2), rows // 2), pl.ds(pl.multiple_of(m * cols, cols), cols)


def o_region(rows, cols, d, m, part):
    if part is None:
        return pl.ds(m * rows, rows), pl.ds(pl.multiple_of(d * cols, cols), cols)
    return pl.ds(m * rows + part * (rows // 2), rows // 2), pl.ds(pl.multiple_of(d * cols, cols), cols)


def front_kernel(half, tok, grad, wq, wkv, wo, gain, wcat, wo_full, hidden, means, inv_stds, proj, grad_mixed, wbuf, obuf, kbuf, q_send, q_recv, o_send, o_recv, kv_send, kv_recv, local):
    d, _, x, c, yn, xn, pn = place()
    rows, cols = wq.shape
    depth, width = wo_full.shape[1], wo_full.shape[0]
    krows, pair = wkv.shape[0] // 2, wkv.shape[1]
    part = width // 2
    entry_barrier((yn, xn, pn))
    k_here = lambda dd, cc: wcat.at[pl.ds(dd * 2 * krows + cc * krows, krows), pl.ds(width, pair)]
    k_out = remote(wkv.at[pl.ds(c * krows, krows), :], k_here(d, c), kv_send.at[0], kv_recv.at[0], yn)
    k_fwd = remote(k_here(1 - d, c), k_here(1 - d, c), kv_send.at[1], kv_recv.at[1], pn)
    k_own = pltpu.make_async_copy(wkv, wcat.at[pl.ds(d * 2 * krows, 2 * krows), pl.ds(width, pair)], local.at[2])
    gather_q = Gather(wq, wcat, functools.partial(q_region, rows, cols), q_send, q_recv, local.at[0])
    gather_o = Gather(wo, wo_full, functools.partial(o_region, wo.shape[0], wo.shape[1]), o_send, o_recv, local.at[1])
    k_out.start()
    gather_q.start()
    k_own.start()
    mine = lambda *_: pl.ds(pl.multiple_of(x * part, part), part)
    other = lambda *_: pl.ds(pl.multiple_of((1 - x) * part, part), part)
    load_q0 = pltpu.make_async_copy(wcat.at[:, mine()], wbuf.at[0], local.at[3])
    load_q1 = pltpu.make_async_copy(wcat.at[:, other()], wbuf.at[1], local.at[4])
    load_kv = pltpu.make_async_copy(wcat.at[:, pl.ds(width, pair)], kbuf, local.at[5])
    load_o0 = pltpu.make_async_copy(wo_full.at[mine(), :], obuf.at[0], local.at[6])
    load_o1 = pltpu.make_async_copy(wo_full.at[other(), :], obuf.at[1], local.at[7])

    def norm_block(tok_blk, hid_blk, mean_blk, inv_blk):
        rows_f = tok_blk[...].astype(F32)
        mean = jnp.mean(rows_f, axis=-1, keepdims=True)
        centred = rows_f - mean
        inv_std = lax.rsqrt(jnp.mean(centred * centred, axis=-1, keepdims=True) + NORM_EPS)
        hid_blk[...] = (centred * inv_std * gain[...]).astype(BF16)
        mean_blk[...] = jnp.broadcast_to(mean, mean_blk.shape)
        inv_blk[...] = jnp.broadcast_to(inv_std, inv_blk.shape)

    tile = 512
    pltpu.emit_pipeline(
        norm_block,
        grid=(half // tile,),
        in_specs=[pl.BlockSpec((tile, depth), lambda i: (i, 0))],
        out_specs=[pl.BlockSpec((tile, depth), lambda i: (i, 0))] + [pl.BlockSpec((tile, 128), lambda i: (i, 0))] * 2,
    )(tok.at[pl.ds(c * half, half), :], hidden, means, inv_stds)

    big = 1024

    def run(src, weight, dims, out):
        def block(a, o):
            o[...] = dot(a[...], weight[...], dims).astype(BF16)

        pltpu.emit_pipeline(
            block,
            grid=(half // big,),
            in_specs=[pl.BlockSpec((big, depth), lambda i: (i, 0))],
            out_specs=[pl.BlockSpec((big, out.shape[1]), lambda i: (i, 0))],
        )(src, out)

    k_out.wait_recv()
    k_fwd.start()
    k_own.wait()
    k_fwd.wait_recv()
    load_kv.start()
    load_kv.wait()
    run(hidden, kbuf, NN, proj.at[:, pl.ds(width, pair)])
    gather_q.middle()
    gather_o.start()
    gather_q.own_half()
    load_q0.start()
    load_q0.wait()
    run(hidden, wbuf.at[0], NN, proj.at[:, mine()])
    gather_q.finish()
    load_q1.start()
    load_q1.wait()
    run(hidden, wbuf.at[1], NN, proj.at[:, other()])
    gather_o.middle()
    gather_o.own_half()
    load_o0.start()
    load_o0.wait()
    own_grad = grad.at[pl.ds(c * half, half), :]
    run(own_grad, obuf.at[0], NT, grad_mixed.at[:, mine()])
    gather_o.finish()
    load_o1.start()
    load_o1.wait()
    run(own_grad, obuf.at[1], NT, grad_mixed.at[:, other()])
    k_out.wait_send()
    k_fwd.wait_send()


def attend_kernel(heads, head_dim, qkv_ref, do_ref, pos_c_ref, pos_r_ref, o_ref, dqkv_ref, seen, pt, dst):
    seq, width = do_ref.shape
    q_ref, dq_ref = qkv_ref, dqkv_ref

    @pl.when(pl.program_id(0) == 0)
    def _():
        seen[...] = jnp.where(pos_c_ref[...] <= pos_r_ref[...], 1.0, -1.0)

    k, v = qkv_ref[:, width : width + head_dim], qkv_ref[:, width + head_dim :]
    kt, vt = k.T, v.T
    scale = head_dim ** -0.5
    cols = lambda h: slice(h * head_dim, (h + 1) * head_dim)
    lanes = lambda h: slice(h * seq, (h + 1) * seq)
    scores, grads, total = {}, {}, [None, None]

    def scored(h):
        scores[h] = dot(k, q_ref[:, cols(h)], NT)
        grads[h] = dot(v, do_ref[:, cols(h)], NT)

    def softmax(h):
        s = jnp.where(seen[...] > 0, scores.pop(h) * (scale * LOG2E), -1e30)
        e = jnp.exp2(s - jnp.max(s, axis=0, keepdims=True))
        p = e * (1.0 / jnp.sum(e, axis=0, keepdims=True))
        pt[:, lanes(h)] = p.astype(BF16)
        dp = grads.pop(h)
        dst[:, lanes(h)] = (p * (dp - jnp.sum(p * dp, axis=0, keepdims=True))).astype(BF16)

    def mixed(h):
        o_ref[:, cols(h)] = dot(vt, pt[:, lanes(h)], NN).T.astype(BF16)
        dq_ref[:, cols(h)] = (dot(kt, dst[:, lanes(h)], NN).T * scale).astype(BF16)
        dv = dot(pt[:, lanes(h)], do_ref[:, cols(h)], NN)
        dk = dot(dst[:, lanes(h)], q_ref[:, cols(h)], NN)
        total[0] = dk if total[0] is None else total[0] + dk
        total[1] = dv if total[1] is None else total[1] + dv

    for t in range(heads + 2):
        if t < heads:
            scored(t)
        if 0 <= t - 2:
            mixed(t - 2)
        if 0 <= t - 1 < heads:
            softmax(t - 1)
    dqkv_ref[:, width : width + head_dim] = (total[0] * scale).astype(BF16)
    dqkv_ref[:, width + head_dim :] = total[1].astype(BF16)


def attend(proj, grad_mixed, positions):
    rows, width = grad_mixed.shape
    seq, total = positions.shape[0], proj.shape[1]
    head_dim = (total - width) // 2
    heads = width // head_dim
    wide = pl.BlockSpec((seq, width), lambda i: (i, 0))
    wider = pl.BlockSpec((seq, total), lambda i: (i, 0))
    return pl.pallas_call(
        functools.partial(attend_kernel, heads, head_dim),
        grid=(rows // seq,),
        in_specs=[wider, wide, pl.BlockSpec((seq, 1), lambda i: (0, 0)), pl.BlockSpec((1, seq), lambda i: (0, 0))],
        out_specs=[wide, wider],
        out_shape=[jax.ShapeDtypeStruct((rows, width), BF16), jax.ShapeDtypeStruct((rows, total), BF16)],
        scratch_shapes=[pltpu.VMEM((seq, seq), F32), pltpu.VMEM((seq, heads * seq), BF16), pltpu.VMEM((seq, heads * seq), BF16)],
        cost_estimate=pl.CostEstimate(flops=12 * rows * seq * width, bytes_accessed=8 * rows * width, transcendentals=rows * seq * heads),
        compiler_params=pltpu.CompilerParams(vmem_limit_bytes=LIMIT),
    )(proj, grad_mixed, positions.reshape(seq, 1), positions.reshape(1, seq))


def give_kernel(count, off, a, *refs):
    for b, out in zip(refs[:count], refs[count:]):
        out[...] = dot(a[...], b[...], TN)


def give(a, bs, offs, shape, widths, tile=512):
    rows = a.shape[0]
    height, width = shape
    wide = width // tile
    blocks = [tile] + list(widths[1:])
    b_specs = [pl.BlockSpec((rows, w), functools.partial(lambda n, i, j, off: (off[1], off[2 + n] + (j if n == 0 else 0)), n)) for n, w in enumerate(blocks)]
    o_specs = [pl.BlockSpec((tile, w), functools.partial(lambda n, i, j, off: (i, j if n == 0 else 0), n)) for n, w in enumerate(blocks)]
    return pl.pallas_call(
        functools.partial(give_kernel, len(bs)),
        grid_spec=pltpu.PrefetchScalarGridSpec(
            num_scalar_prefetch=1,
            grid=(height // tile, wide),
            in_specs=[pl.BlockSpec((rows, tile), lambda i, j, off: (0, off[0] + i))] + b_specs,
            out_specs=o_specs,
        ),
        out_shape=[jax.ShapeDtypeStruct((height, w), F32) for w in widths],
        cost_estimate=pl.CostEstimate(flops=2 * rows * height * sum(widths), bytes_accessed=2 * rows * (height + sum(widths)), transcendentals=0),
        compiler_params=pltpu.CompilerParams(vmem_limit_bytes=LIMIT),
    )(offs, a, *bs)


def keep_kernel(half, off, a, b, got, send, keep):
    step = pl.program_id(0)
    value = got[...] + dot(a[...], b[...], TN)

    @pl.when(step < half)
    def _():
        send[...] = value

    @pl.when(step >= half)
    def _():
        keep[...] = value


def keep(a, b, offs, shape, axis, got, tile=512):
    rows = a.shape[0]
    steps = shape[axis] // tile
    half = steps // 2
    turn = lambda t, off: jnp.where(t < half, (1 - off[3]) * half + t, off[3] * half + t - half)
    at = (lambda t, off: (turn(t, off), 0)) if axis == 0 else (lambda t, off: (0, turn(t, off)))
    line = (lambda t: (t, 0)) if axis == 0 else (lambda t: (0, t))
    out = (shape[0] // 2, shape[1]) if axis == 0 else (shape[0], shape[1] // 2)
    return pl.pallas_call(
        functools.partial(keep_kernel, half),
        grid_spec=pltpu.PrefetchScalarGridSpec(
            num_scalar_prefetch=1,
            grid=(steps,),
            in_specs=[
                pl.BlockSpec((rows, tile), lambda t, off: (0, off[0] + at(t, off)[0])),
                pl.BlockSpec((rows, tile), lambda t, off: (off[1], off[2] + at(t, off)[1])),
                pl.BlockSpec((tile, tile), at),
            ],
            out_specs=[
                pl.BlockSpec((tile, tile), lambda t, off: line(jnp.minimum(t, half - 1))),
                pl.BlockSpec((tile, tile), lambda t, off: line(jnp.maximum(t - half, 0))),
            ],
        ),
        out_shape=[jax.ShapeDtypeStruct(out, F32)] * 2,
        cost_estimate=pl.CostEstimate(flops=2 * rows * shape[0] * shape[1], bytes_accessed=2 * rows * sum(shape), transcendentals=0),
        compiler_params=pltpu.CompilerParams(vmem_limit_bytes=LIMIT),
    )(offs, a, b, got)


def out_kernel(off, a, b, full, send):
    block = dot(a[...], b[...], NN).astype(BF16)
    full[...] = block
    send[...] = block


def project_out(mixed, wo, core, tile=1024):
    rows, depth = mixed.shape
    width = wo.shape[1]
    blocks = rows // tile
    return pl.pallas_call(
        out_kernel,
        grid_spec=pltpu.PrefetchScalarGridSpec(
            num_scalar_prefetch=1,
            grid=(width // tile, blocks),
            in_specs=[pl.BlockSpec((tile, depth), lambda j, i, off: (i, 0)), pl.BlockSpec((depth, tile), lambda j, i, off: (0, j))],
            out_specs=[pl.BlockSpec((tile, tile), lambda j, i, off: (off[0] * blocks + i, j)), pl.BlockSpec((tile, tile), lambda j, i, off: (i, j))],
        ),
        out_shape=[jax.ShapeDtypeStruct((2 * rows, width), BF16), jax.ShapeDtypeStruct((rows, width), BF16)],
        cost_estimate=pl.CostEstimate(flops=2 * rows * depth * width, bytes_accessed=2 * rows * (depth + 2 * width), transcendentals=0),
        compiler_params=pltpu.CompilerParams(vmem_limit_bytes=LIMIT),
    )(core, mixed, wo)


def grad_tok_kernel(passing, off, gqkv, wcat, gain, tok, means, inv_stds, *refs):
    if passing:
        got, _, _, full, send, y_full = refs
        y_full[...] = got[...]
    else:
        full, send = refs
    mean, inv_std = means[:, :1], inv_stds[:, :1]
    g = dot(gqkv[...], wcat[...], NT) * gain[...]
    normed = (tok[...].astype(F32) - mean) * inv_std
    block = (inv_std * (g - jnp.mean(g, axis=-1, keepdims=True) - normed * jnp.mean(g * normed, axis=-1, keepdims=True))).astype(BF16)
    full[...] = block
    send[...] = block


def grad_tok(gqkv, wcat, gain, tok, means, inv_stds, core, part, earlier=None, tile=512):
    rows, total = gqkv.shape
    depth = wcat.shape[0]
    blocks = rows // tile
    steps = blocks // 2
    first = part * steps
    whole = lambda i, off: (0, 0)
    once = pl.Buffered(1)
    in_specs = [
        pl.BlockSpec((tile, total), lambda i, off: (first + i, 0)),
        pl.BlockSpec((depth, total), whole, pipeline_mode=once),
        pl.BlockSpec((1, depth), whole, pipeline_mode=once),
        pl.BlockSpec((tile, depth), lambda i, off: (off[0] * blocks + first + i, 0)),
        pl.BlockSpec((tile, 128), lambda i, off: (first + i, 0)),
        pl.BlockSpec((tile, 128), lambda i, off: (first + i, 0)),
    ]
    own = pl.BlockSpec((tile, depth), lambda i, off: (off[0] * blocks + first + i, 0))
    out_specs = [own, pl.BlockSpec((tile, depth), lambda i, off: (i, 0))]
    out_shape = [jax.ShapeDtypeStruct((2 * rows, depth), BF16), jax.ShapeDtypeStruct((rows // 2, depth), BF16)]
    args, aliases = [core, gqkv, wcat, gain, tok, means, inv_stds], {}
    if earlier is not None:
        dx, y, got = earlier
        args += [got, dx, y]
        wide = 2 * tile
        in_specs += [pl.BlockSpec((wide, depth), lambda i, off: (i, 0)), ANY, ANY]
        out_specs.append(pl.BlockSpec((wide, depth), lambda i, off: ((1 - off[0]) * steps + i, 0)))
        out_shape.append(jax.ShapeDtypeStruct(y.shape, BF16))
        aliases = {8: 0, 9: 2}
    return pl.pallas_call(
        functools.partial(grad_tok_kernel, earlier is not None),
        grid_spec=pltpu.PrefetchScalarGridSpec(num_scalar_prefetch=1, grid=(steps,), in_specs=in_specs, out_specs=out_specs),
        out_shape=out_shape,
        input_output_aliases=aliases,
        cost_estimate=pl.CostEstimate(flops=rows * depth * total, bytes_accessed=5 * rows * depth, transcendentals=0),
        compiler_params=pltpu.CompilerParams(vmem_limit_bytes=LIMIT),
    )(*args)


def fill_kernel(off, got, _, out):
    out[...] = got[...]


def fill(full, got, core, part, tile=1024):
    rows, width = got.shape
    blocks = rows // tile
    return pl.pallas_call(
        fill_kernel,
        grid_spec=pltpu.PrefetchScalarGridSpec(
            num_scalar_prefetch=1,
            grid=(blocks,),
            in_specs=[pl.BlockSpec((tile, width), lambda i, off: (i, 0)), ANY],
            out_specs=pl.BlockSpec((tile, width), lambda i, off: ((1 - off[0]) * 2 * blocks + part * blocks + i, 0)),
        ),
        out_shape=jax.ShapeDtypeStruct(full.shape, full.dtype),
        input_output_aliases={2: 0},
        cost_estimate=pl.CostEstimate(flops=rows * width, bytes_accessed=4 * rows * width, transcendentals=0),
        compiler_params=pltpu.CompilerParams(vmem_limit_bytes=LIMIT),
    )(core, got, full)


def after(value, *others):
    return lax.optimization_barrier((value,) + others)[0]


def solution(mesh):
    model_size = mesh.shape["model"]
    cores = [(i, i ^ 1) for i in range(model_size)]
    datas = [(0, 1), (1, 0)]
    sems = lambda n: pltpu.SemaphoreType.DMA((n,))

    def layer(tok, wq_blk, wkv_blk, wo_blk, ln_gain, positions, grad):
        count, depth = tok.shape
        half = count // 2
        width = wq_blk.shape[1] * model_size
        pair = wkv_blk.shape[1]
        piece = width // model_size
        m = lax.axis_index("model")
        d = lax.axis_index("data")
        x, c = m // 2, m % 2
        gain = ln_gain.reshape(1, depth)
        core = c.reshape(1).astype(jnp.int32)
        index = lambda *v: jnp.stack([jnp.asarray(t, jnp.int32) for t in v])

        def swap(a):
            return lax.ppermute(a, "model", cores)

        def cross(a):
            return lax.ppermute(a, "data", datas)


        wcat, wo, hidden, means, inv_stds, proj, grad_mixed = pl.pallas_call(
            functools.partial(front_kernel, half),
            in_specs=[ANY, ANY, VMEM, VMEM, VMEM, VMEM],
            out_specs=[ANY] * 7,
            out_shape=[
                jax.ShapeDtypeStruct((depth, width + pair), BF16),
                jax.ShapeDtypeStruct((width, depth), BF16),
                jax.ShapeDtypeStruct((half, depth), BF16),
                jax.ShapeDtypeStruct((half, 128), F32),
                jax.ShapeDtypeStruct((half, 128), F32),
                jax.ShapeDtypeStruct((half, width + pair), BF16),
                jax.ShapeDtypeStruct((half, width), BF16),
            ],
            scratch_shapes=[pltpu.VMEM((2, depth, width // 2), BF16), pltpu.VMEM((2, width // 2, depth), BF16), pltpu.VMEM((depth, pair), BF16)]
            + [sems(9), sems(9), sems(9), sems(9), sems(2), sems(2), sems(8)],
            compiler_params=pltpu.CompilerParams(collective_id=0, has_side_effects=True, vmem_limit_bytes=LIMIT),
        )(tok, grad, wq_blk, wkv_blk, wo_blk, gain)

        mixed, gqkv = attend(proj, grad_mixed, positions)

        def halves(a, i, axis):
            size = a.shape[axis] // 2
            return lax.dynamic_slice_in_dim(a, i * size, size, axis), lax.dynamic_slice_in_dim(a, (1 - i) * size, size, axis)

        mine, other = 2 * x + c, 2 * x + 1 - c
        (give_o,) = give(mixed, [grad], index(other, c, 0), (piece, depth), [depth])
        got_o = swap(give_o)
        give_q, part_kv = give(after(hidden, give_o), [gqkv, gqkv], index(0, 0, other, width // pair), (depth, piece), [piece, pair])
        got_q = swap(give_q)
        kv_keep, kv_give = halves(part_kv, c, 1)
        kv_got = swap(kv_give)
        send_o, keep_o = keep(after(mixed, give_q), grad, index(mine, c, 0, d), (piece, depth), 1, got_o)
        data_o = cross(send_o)
        kv_keep, kv_give = halves(kv_keep + kv_got, d, 0)
        kv_data = cross(kv_give)
        send_q, keep_q = keep(after(hidden, send_o, kv_give), gqkv, index(0, 0, mine, d), (depth, piece), 0, got_q)
        data_q = cross(send_q)

        y, y_send = project_out(after(mixed, send_q), wo, core)
        y_got = swap(y_send)
        grad_w_out = (keep_o + data_o).astype(BF16)
        dx, dx_send = grad_tok(after(gqkv, y_send, grad_w_out), wcat, gain, tok, means, inv_stds, core, 0)
        dx_got_0 = swap(dx_send)
        kv_cols = (kv_keep + kv_data).astype(BF16)
        kv_other = swap(kv_cols)
        grad_w_query = (keep_q + data_q).astype(BF16)
        grad_w_kv = jnp.where(c == 0, jnp.concatenate([kv_cols, kv_other], axis=1), jnp.concatenate([kv_other, kv_cols], axis=1))
        dx, dx_send, y = grad_tok(after(gqkv, dx_send, grad_w_query, kv_cols), wcat, gain, tok, means, inv_stds, core, 1, (dx, y, y_got))
        dx_got_1 = swap(dx_send)
        dx = fill(dx, dx_got_0, core, 0)
        dx = fill(dx, dx_got_1, core, 1)
        return y, dx, grad_w_query, grad_w_kv, grad_w_out

    return jax.shard_map(
        layer,
        mesh=mesh,
        in_specs=(P("data", None), P("data", "model"), P("data", None), P("model", "data"), P(), P(), P("data", None)),
        out_specs=(P("data", None), P("data", None), P("data", "model"), P("data", None), P("model", "data")),
        check_vma=False,
    )
```

```python
import functools

import jax
import jax.numpy as jnp
from jax import lax
from jax.experimental import pallas as pl
from jax.experimental.pallas import tpu as pltpu
from jax.sharding import PartitionSpec as P


NORM_EPS = 1e-6
LOG2E = 1.4426950408889634
BF16, F32 = jnp.bfloat16, jnp.float32
NN = (((1,), (0,)), ((), ()))
NT = (((1,), (1,)), ((), ()))
TN = (((0,), (0,)), ((), ()))
MESH = pl.DeviceIdType.MESH
ANY = pl.BlockSpec(memory_space=pl.ANY)
VMEM = pl.BlockSpec(memory_space=pltpu.VMEM)
LIMIT = 62 * 2**20


def dot(a, b, dims):
    return lax.dot_general(a, b, dims, preferred_element_type=F32)


def place():
    d, m = lax.axis_index("data"), lax.axis_index("model")
    x, c = m // 2, m % 2
    return d, m, x, c, (1 - d, m), (d, 2 * (1 - x) + c), (d, 2 * x + (1 - c))


def entry_barrier(peers):
    barrier = pltpu.get_barrier_semaphore()
    for peer in peers:
        pl.semaphore_signal(barrier, inc=1, device_id=peer, device_id_type=MESH)
    pl.semaphore_wait(barrier, len(peers))


def remote(src, dst, send, recv, peer):
    return pltpu.make_async_remote_copy(src_ref=src, dst_ref=dst, send_sem=send, recv_sem=recv, device_id=peer, device_id_type=MESH)


class Gather:
    def __init__(self, piece, full, region, send, recv, local):
        self.piece, self.full, self.region = piece, full, region
        self.send, self.recv, self.local = send, recv, local

    def copies(self):
        d, m, x, c, yn, xn, pn = place()
        ym, xm = (1 - d, m), (d, 2 * (1 - x) + c)
        full, reg, s, r = self.full, self.region, self.send, self.recv
        at = lambda dm, part=None: full.at[reg(dm[0], dm[1], part)]
        diag = (1 - d, 2 * (1 - x) + c)
        own = at((d, m))
        first = [remote(self.piece, own, s.at[0], r.at[0], yn), remote(self.piece, own, s.at[1], r.at[1], xn), remote(self.piece, own, s.at[2], r.at[2], pn)]
        second = [
            remote(at(ym, 0), at(ym, 0), s.at[3], r.at[3], xn),
            remote(at(xm, 1), at(xm, 1), s.at[4], r.at[4], yn),
            remote(at(ym), at(ym), s.at[5], r.at[5], pn),
            remote(at(xm), at(xm), s.at[6], r.at[6], pn),
        ]
        third = [remote(at(diag, 0), at(diag, 0), s.at[7], r.at[7], pn), remote(at(diag, 1), at(diag, 1), s.at[8], r.at[8], pn)]
        mine = pltpu.make_async_copy(self.piece, own, self.local)
        return first, second, third, mine

    def start(self):
        first, _, _, mine = self.copies()
        for copy in first:
            copy.start()
        mine.start()

    def middle(self):
        first, second, _, _ = self.copies()
        first[1].wait_recv()
        second[1].start()
        second[3].start()
        first[0].wait_recv()
        second[0].start()
        second[2].start()

    def own_half(self):
        first, second, _, mine = self.copies()
        mine.wait()
        first[2].wait_recv()
        second[2].wait_recv()

    def finish(self):
        first, second, third, _ = self.copies()
        second[0].wait_recv()
        third[0].start()
        second[1].wait_recv()
        third[1].start()
        second[3].wait_recv()
        third[0].wait_recv()
        third[1].wait_recv()
        for copy in first + second + third:
            copy.wait_send()


def q_region(rows, cols, d, m, part):
    if part is None:
        return pl.ds(d * rows, rows), pl.ds(pl.multiple_of(m * cols, cols), cols)
    return pl.ds(d * rows + part * (rows // 2), rows // 2), pl.ds(pl.multiple_of(m * cols, cols), cols)


def o_region(rows, cols, d, m, part):
    if part is None:
        return pl.ds(m * rows, rows), pl.ds(pl.multiple_of(d * cols, cols), cols)
    return pl.ds(m * rows + part * (rows // 2), rows // 2), pl.ds(pl.multiple_of(d * cols, cols), cols)


def front_kernel(half, tok, grad, wq, wkv, wo, gain, wcat, wo_full, hidden, means, inv_stds, proj, grad_mixed, wbuf, obuf, kbuf, q_send, q_recv, o_send, o_recv, kv_send, kv_recv, local):
    d, _, x, c, yn, xn, pn = place()
    rows, cols = wq.shape
    depth, width = wo_full.shape[1], wo_full.shape[0]
    krows, pair = wkv.shape[0] // 2, wkv.shape[1]
    part = width // 2
    entry_barrier((yn, xn, pn))
    k_here = lambda dd, cc: wcat.at[pl.ds(dd * 2 * krows + cc * krows, krows), pl.ds(width, pair)]
    k_out = remote(wkv.at[pl.ds(c * krows, krows), :], k_here(d, c), kv_send.at[0], kv_recv.at[0], yn)
    k_fwd = remote(k_here(1 - d, c), k_here(1 - d, c), kv_send.at[1], kv_recv.at[1], pn)
    k_own = pltpu.make_async_copy(wkv, wcat.at[pl.ds(d * 2 * krows, 2 * krows), pl.ds(width, pair)], local.at[2])
    gather_q = Gather(wq, wcat, functools.partial(q_region, rows, cols), q_send, q_recv, local.at[0])
    gather_o = Gather(wo, wo_full, functools.partial(o_region, wo.shape[0], wo.shape[1]), o_send, o_recv, local.at[1])
    k_out.start()
    gather_q.start()
    k_own.start()
    mine = lambda *_: pl.ds(pl.multiple_of(x * part, part), part)
    other = lambda *_: pl.ds(pl.multiple_of((1 - x) * part, part), part)
    load_q0 = pltpu.make_async_copy(wcat.at[:, mine()], wbuf.at[0], local.at[3])
    load_q1 = pltpu.make_async_copy(wcat.at[:, other()], wbuf.at[1], local.at[4])
    load_kv = pltpu.make_async_copy(wcat.at[:, pl.ds(width, pair)], kbuf, local.at[5])
    load_o0 = pltpu.make_async_copy(wo_full.at[mine(), :], obuf.at[0], local.at[6])
    load_o1 = pltpu.make_async_copy(wo_full.at[other(), :], obuf.at[1], local.at[7])

    def norm_block(tok_blk, hid_blk, mean_blk, inv_blk):
        rows_f = tok_blk[...].astype(F32)
        mean = jnp.mean(rows_f, axis=-1, keepdims=True)
        centred = rows_f - mean
        inv_std = lax.rsqrt(jnp.mean(centred * centred, axis=-1, keepdims=True) + NORM_EPS)
        hid_blk[...] = (centred * inv_std * gain[...]).astype(BF16)
        mean_blk[...] = jnp.broadcast_to(mean, mean_blk.shape)
        inv_blk[...] = jnp.broadcast_to(inv_std, inv_blk.shape)

    tile = 512
    pltpu.emit_pipeline(
        norm_block,
        grid=(half // tile,),
        in_specs=[pl.BlockSpec((tile, depth), lambda i: (i, 0))],
        out_specs=[pl.BlockSpec((tile, depth), lambda i: (i, 0))] + [pl.BlockSpec((tile, 128), lambda i: (i, 0))] * 2,
    )(tok.at[pl.ds(c * half, half), :], hidden, means, inv_stds)

    big = 1024

    def run(src, weight, dims, out):
        def block(a, o):
            o[...] = dot(a[...], weight[...], dims).astype(BF16)

        pltpu.emit_pipeline(
            block,
            grid=(half // big,),
            in_specs=[pl.BlockSpec((big, depth), lambda i: (i, 0))],
            out_specs=[pl.BlockSpec((big, out.shape[1]), lambda i: (i, 0))],
        )(src, out)

    k_out.wait_recv()
    k_fwd.start()
    k_own.wait()
    k_fwd.wait_recv()
    load_kv.start()
    load_kv.wait()
    run(hidden, kbuf, NN, proj.at[:, pl.ds(width, pair)])
    gather_q.middle()
    gather_o.start()
    gather_q.own_half()
    load_q0.start()
    load_q0.wait()
    run(hidden, wbuf.at[0], NN, proj.at[:, mine()])
    gather_q.finish()
    load_q1.start()
    load_q1.wait()
    run(hidden, wbuf.at[1], NN, proj.at[:, other()])
    gather_o.middle()
    gather_o.own_half()
    load_o0.start()
    load_o0.wait()
    own_grad = grad.at[pl.ds(c * half, half), :]
    run(own_grad, obuf.at[0], NT, grad_mixed.at[:, mine()])
    gather_o.finish()
    load_o1.start()
    load_o1.wait()
    run(own_grad, obuf.at[1], NT, grad_mixed.at[:, other()])
    k_out.wait_send()
    k_fwd.wait_send()


def attend_kernel(heads, head_dim, qkv_ref, do_ref, pos_ref, o_ref, dqkv_ref, seen, pt, dst):
    seq, width = do_ref.shape
    q_ref, dq_ref = qkv_ref, dqkv_ref

    @pl.when(pl.program_id(0) == 0)
    def _():
        query_pos = jnp.broadcast_to(pos_ref[...].astype(F32), (seq, seq))
        seen[...] = jnp.where(query_pos.T <= query_pos, 1.0, -1.0)

    k, v = qkv_ref[:, width : width + head_dim], qkv_ref[:, width + head_dim :]
    kt, vt = k.T, v.T
    scale = head_dim ** -0.5
    cols = lambda h: slice(h * head_dim, (h + 1) * head_dim)
    lanes = lambda h: slice(h * seq, (h + 1) * seq)
    scores, grads, total = {}, {}, [None, None]

    def scored(h):
        scores[h] = dot(k, q_ref[:, cols(h)], NT)
        grads[h] = dot(v, do_ref[:, cols(h)], NT)

    def softmax(h):
        s = jnp.where(seen[...] > 0, scores.pop(h) * (scale * LOG2E), -1e30)
        e = jnp.exp2(s - jnp.max(s, axis=0, keepdims=True))
        p = e * (1.0 / jnp.sum(e, axis=0, keepdims=True))
        pt[:, lanes(h)] = p.astype(BF16)
        dp = grads.pop(h)
        dst[:, lanes(h)] = (p * (dp - jnp.sum(p * dp, axis=0, keepdims=True))).astype(BF16)

    def mixed(h):
        o_ref[:, cols(h)] = dot(vt, pt[:, lanes(h)], NN).T.astype(BF16)
        dq_ref[:, cols(h)] = (dot(kt, dst[:, lanes(h)], NN).T * scale).astype(BF16)
        dv = dot(pt[:, lanes(h)], do_ref[:, cols(h)], NN)
        dk = dot(dst[:, lanes(h)], q_ref[:, cols(h)], NN)
        total[0] = dk if total[0] is None else total[0] + dk
        total[1] = dv if total[1] is None else total[1] + dv

    for t in range(heads + 2):
        if t < heads:
            scored(t)
        if 0 <= t - 2:
            mixed(t - 2)
        if 0 <= t - 1 < heads:
            softmax(t - 1)
    dqkv_ref[:, width : width + head_dim] = (total[0] * scale).astype(BF16)
    dqkv_ref[:, width + head_dim :] = total[1].astype(BF16)


def attend(proj, grad_mixed, positions):
    rows, width = grad_mixed.shape
    seq, total = positions.shape[0], proj.shape[1]
    head_dim = (total - width) // 2
    heads = width // head_dim
    wide = pl.BlockSpec((seq, width), lambda i: (i, 0))
    wider = pl.BlockSpec((seq, total), lambda i: (i, 0))
    return pl.pallas_call(
        functools.partial(attend_kernel, heads, head_dim),
        grid=(rows // seq,),
        in_specs=[wider, wide, pl.BlockSpec((1, seq), lambda i: (0, 0))],
        out_specs=[wide, wider],
        out_shape=[jax.ShapeDtypeStruct((rows, width), BF16), jax.ShapeDtypeStruct((rows, total), BF16)],
        scratch_shapes=[pltpu.VMEM((seq, seq), F32), pltpu.VMEM((seq, heads * seq), BF16), pltpu.VMEM((seq, heads * seq), BF16)],
        cost_estimate=pl.CostEstimate(flops=12 * rows * seq * width, bytes_accessed=8 * rows * width, transcendentals=rows * seq * heads),
        compiler_params=pltpu.CompilerParams(vmem_limit_bytes=LIMIT),
    )(proj, grad_mixed, positions.reshape(1, seq))


def give_kernel(count, off, a, *refs):
    for b, out in zip(refs[:count], refs[count:]):
        out[...] = dot(a[...], b[...], TN)


def give(a, bs, offs, shape, widths, tile=512):
    rows = a.shape[0]
    height, width = shape
    wide = width // tile
    blocks = [tile] + list(widths[1:])
    b_specs = [pl.BlockSpec((rows, w), functools.partial(lambda n, i, j, off: (off[1], off[2 + n] + (j if n == 0 else 0)), n)) for n, w in enumerate(blocks)]
    o_specs = [pl.BlockSpec((tile, w), functools.partial(lambda n, i, j, off: (i, j if n == 0 else 0), n)) for n, w in enumerate(blocks)]
    return pl.pallas_call(
        functools.partial(give_kernel, len(bs)),
        grid_spec=pltpu.PrefetchScalarGridSpec(
            num_scalar_prefetch=1,
            grid=(height // tile, wide),
            in_specs=[pl.BlockSpec((rows, tile), lambda i, j, off: (0, off[0] + i))] + b_specs,
            out_specs=o_specs,
        ),
        out_shape=[jax.ShapeDtypeStruct((height, w), F32) for w in widths],
        cost_estimate=pl.CostEstimate(flops=2 * rows * height * sum(widths), bytes_accessed=2 * rows * (height + sum(widths)), transcendentals=0),
        compiler_params=pltpu.CompilerParams(vmem_limit_bytes=LIMIT),
    )(offs, a, *bs)


def keep_kernel(half, off, a, b, got, send, keep):
    step = pl.program_id(0)
    value = got[...] + dot(a[...], b[...], TN)

    @pl.when(step < half)
    def _():
        send[...] = value

    @pl.when(step >= half)
    def _():
        keep[...] = value


def keep(a, b, offs, shape, axis, got, tile=512):
    rows = a.shape[0]
    steps = shape[axis] // tile
    half = steps // 2
    turn = lambda t, off: jnp.where(t < half, (1 - off[3]) * half + t, off[3] * half + t - half)
    at = (lambda t, off: (turn(t, off), 0)) if axis == 0 else (lambda t, off: (0, turn(t, off)))
    line = (lambda t: (t, 0)) if axis == 0 else (lambda t: (0, t))
    out = (shape[0] // 2, shape[1]) if axis == 0 else (shape[0], shape[1] // 2)
    return pl.pallas_call(
        functools.partial(keep_kernel, half),
        grid_spec=pltpu.PrefetchScalarGridSpec(
            num_scalar_prefetch=1,
            grid=(steps,),
            in_specs=[
                pl.BlockSpec((rows, tile), lambda t, off: (0, off[0] + at(t, off)[0])),
                pl.BlockSpec((rows, tile), lambda t, off: (off[1], off[2] + at(t, off)[1])),
                pl.BlockSpec((tile, tile), at),
            ],
            out_specs=[
                pl.BlockSpec((tile, tile), lambda t, off: line(jnp.minimum(t, half - 1))),
                pl.BlockSpec((tile, tile), lambda t, off: line(jnp.maximum(t - half, 0))),
            ],
        ),
        out_shape=[jax.ShapeDtypeStruct(out, F32)] * 2,
        cost_estimate=pl.CostEstimate(flops=2 * rows * shape[0] * shape[1], bytes_accessed=2 * rows * sum(shape), transcendentals=0),
        compiler_params=pltpu.CompilerParams(vmem_limit_bytes=LIMIT),
    )(offs, a, b, got)


def out_kernel(off, a, b, full, send):
    block = dot(a[...], b[...], NN).astype(BF16)
    full[...] = block
    send[...] = block


def project_out(mixed, wo, core, tile=1024):
    rows, depth = mixed.shape
    width = wo.shape[1]
    blocks = rows // tile
    return pl.pallas_call(
        out_kernel,
        grid_spec=pltpu.PrefetchScalarGridSpec(
            num_scalar_prefetch=1,
            grid=(width // tile, blocks),
            in_specs=[pl.BlockSpec((tile, depth), lambda j, i, off: (i, 0)), pl.BlockSpec((depth, tile), lambda j, i, off: (0, j))],
            out_specs=[pl.BlockSpec((tile, tile), lambda j, i, off: (off[0] * blocks + i, j)), pl.BlockSpec((tile, tile), lambda j, i, off: (i, j))],
        ),
        out_shape=[jax.ShapeDtypeStruct((2 * rows, width), BF16), jax.ShapeDtypeStruct((rows, width), BF16)],
        cost_estimate=pl.CostEstimate(flops=2 * rows * depth * width, bytes_accessed=2 * rows * (depth + 2 * width), transcendentals=0),
        compiler_params=pltpu.CompilerParams(vmem_limit_bytes=LIMIT),
    )(core, mixed, wo)


def grad_tok_kernel(passing, off, gqkv, wcat, gain, tok, means, inv_stds, *refs):
    if passing:
        got, _, _, full, send, y_full = refs
        y_full[...] = got[...]
    else:
        full, send = refs
    mean, inv_std = means[:, :1], inv_stds[:, :1]
    g = dot(gqkv[...], wcat[...], NT) * gain[...]
    normed = (tok[...].astype(F32) - mean) * inv_std
    block = (inv_std * (g - jnp.mean(g, axis=-1, keepdims=True) - normed * jnp.mean(g * normed, axis=-1, keepdims=True))).astype(BF16)
    full[...] = block
    send[...] = block


def grad_tok(gqkv, wcat, gain, tok, means, inv_stds, core, part, earlier=None, tile=512):
    rows, total = gqkv.shape
    depth = wcat.shape[0]
    blocks = rows // tile
    steps = blocks // 2
    first = part * steps
    whole = lambda i, off: (0, 0)
    once = pl.Buffered(1)
    in_specs = [
        pl.BlockSpec((tile, total), lambda i, off: (first + i, 0)),
        pl.BlockSpec((depth, total), whole, pipeline_mode=once),
        pl.BlockSpec((1, depth), whole, pipeline_mode=once),
        pl.BlockSpec((tile, depth), lambda i, off: (off[0] * blocks + first + i, 0)),
        pl.BlockSpec((tile, 128), lambda i, off: (first + i, 0)),
        pl.BlockSpec((tile, 128), lambda i, off: (first + i, 0)),
    ]
    own = pl.BlockSpec((tile, depth), lambda i, off: (off[0] * blocks + first + i, 0))
    out_specs = [own, pl.BlockSpec((tile, depth), lambda i, off: (i, 0))]
    out_shape = [jax.ShapeDtypeStruct((2 * rows, depth), BF16), jax.ShapeDtypeStruct((rows // 2, depth), BF16)]
    args, aliases = [core, gqkv, wcat, gain, tok, means, inv_stds], {}
    if earlier is not None:
        dx, y, got = earlier
        args += [got, dx, y]
        wide = 2 * tile
        in_specs += [pl.BlockSpec((wide, depth), lambda i, off: (i, 0)), ANY, ANY]
        out_specs.append(pl.BlockSpec((wide, depth), lambda i, off: ((1 - off[0]) * steps + i, 0)))
        out_shape.append(jax.ShapeDtypeStruct(y.shape, BF16))
        aliases = {8: 0, 9: 2}
    return pl.pallas_call(
        functools.partial(grad_tok_kernel, earlier is not None),
        grid_spec=pltpu.PrefetchScalarGridSpec(num_scalar_prefetch=1, grid=(steps,), in_specs=in_specs, out_specs=out_specs),
        out_shape=out_shape,
        input_output_aliases=aliases,
        cost_estimate=pl.CostEstimate(flops=rows * depth * total, bytes_accessed=5 * rows * depth, transcendentals=0),
        compiler_params=pltpu.CompilerParams(vmem_limit_bytes=LIMIT),
    )(*args)


def fill_kernel(off, got, _, out):
    out[...] = got[...]


def fill(full, got, core, part, tile=1024):
    rows, width = got.shape
    blocks = rows // tile
    return pl.pallas_call(
        fill_kernel,
        grid_spec=pltpu.PrefetchScalarGridSpec(
            num_scalar_prefetch=1,
            grid=(blocks,),
            in_specs=[pl.BlockSpec((tile, width), lambda i, off: (i, 0)), ANY],
            out_specs=pl.BlockSpec((tile, width), lambda i, off: ((1 - off[0]) * 2 * blocks + part * blocks + i, 0)),
        ),
        out_shape=jax.ShapeDtypeStruct(full.shape, full.dtype),
        input_output_aliases={2: 0},
        cost_estimate=pl.CostEstimate(flops=rows * width, bytes_accessed=4 * rows * width, transcendentals=0),
        compiler_params=pltpu.CompilerParams(vmem_limit_bytes=LIMIT),
    )(core, got, full)


def after(value, *others):
    return lax.optimization_barrier((value,) + others)[0]


def solution(mesh):
    model_size = mesh.shape["model"]
    cores = [(i, i ^ 1) for i in range(model_size)]
    datas = [(0, 1), (1, 0)]
    sems = lambda n: pltpu.SemaphoreType.DMA((n,))

    def layer(tok, wq_blk, wkv_blk, wo_blk, ln_gain, positions, grad):
        count, depth = tok.shape
        half = count // 2
        width = wq_blk.shape[1] * model_size
        pair = wkv_blk.shape[1]
        piece = width // model_size
        m = lax.axis_index("model")
        d = lax.axis_index("data")
        x, c = m // 2, m % 2
        gain = ln_gain.reshape(1, depth)
        core = c.reshape(1).astype(jnp.int32)
        index = lambda *v: jnp.stack([jnp.asarray(t, jnp.int32) for t in v])

        def swap(a):
            return lax.ppermute(a, "model", cores)

        def cross(a):
            return lax.ppermute(a, "data", datas)


        wcat, wo, hidden, means, inv_stds, proj, grad_mixed = pl.pallas_call(
            functools.partial(front_kernel, half),
            in_specs=[ANY, ANY, VMEM, VMEM, VMEM, VMEM],
            out_specs=[ANY] * 7,
            out_shape=[
                jax.ShapeDtypeStruct((depth, width + pair), BF16),
                jax.ShapeDtypeStruct((width, depth), BF16),
                jax.ShapeDtypeStruct((half, depth), BF16),
                jax.ShapeDtypeStruct((half, 128), F32),
                jax.ShapeDtypeStruct((half, 128), F32),
                jax.ShapeDtypeStruct((half, width + pair), BF16),
                jax.ShapeDtypeStruct((half, width), BF16),
            ],
            scratch_shapes=[pltpu.VMEM((2, depth, width // 2), BF16), pltpu.VMEM((2, width // 2, depth), BF16), pltpu.VMEM((depth, pair), BF16)]
            + [sems(9), sems(9), sems(9), sems(9), sems(2), sems(2), sems(8)],
            compiler_params=pltpu.CompilerParams(collective_id=0, has_side_effects=True, vmem_limit_bytes=LIMIT),
        )(tok, grad, wq_blk, wkv_blk, wo_blk, gain)

        mixed, gqkv = attend(proj, grad_mixed, positions)

        def halves(a, i, axis):
            size = a.shape[axis] // 2
            return lax.dynamic_slice_in_dim(a, i * size, size, axis), lax.dynamic_slice_in_dim(a, (1 - i) * size, size, axis)

        mine, other = 2 * x + c, 2 * x + 1 - c
        (give_o,) = give(mixed, [grad], index(other, c, 0), (piece, depth), [depth])
        got_o = swap(give_o)
        give_q, part_kv = give(after(hidden, give_o), [gqkv, gqkv], index(0, 0, other, width // pair), (depth, piece), [piece, pair])
        got_q = swap(give_q)
        kv_keep, kv_give = halves(part_kv, c, 1)
        kv_got = swap(kv_give)
        send_o, keep_o = keep(after(mixed, give_q), grad, index(mine, c, 0, d), (piece, depth), 1, got_o)
        data_o = cross(send_o)
        kv_keep, kv_give = halves(kv_keep + kv_got, d, 0)
        kv_data = cross(kv_give)
        send_q, keep_q = keep(after(hidden, send_o, kv_give), gqkv, index(0, 0, mine, d), (depth, piece), 0, got_q)
        data_q = cross(send_q)

        y, y_send = project_out(after(mixed, send_q), wo, core)
        y_got = swap(y_send)
        dx, dx_send = grad_tok(after(gqkv, y_send), wcat, gain, tok, means, inv_stds, core, 0)
        dx_got_0 = swap(dx_send)
        kv_cols = (kv_keep + kv_data).astype(BF16)
        kv_other = swap(kv_cols)
        dx, dx_send, y = grad_tok(after(gqkv, dx_send, kv_cols), wcat, gain, tok, means, inv_stds, core, 1, (dx, y, y_got))
        dx_got_1 = swap(dx_send)
        dx = fill(dx, dx_got_0, core, 0)
        data_o, data_q, kv_other = lax.optimization_barrier((data_o, data_q, kv_other, dx_send))[:3]
        grad_w_out = (keep_o + data_o).astype(BF16)
        grad_w_query = (keep_q + data_q).astype(BF16)
        grad_w_kv = jnp.where(c == 0, jnp.concatenate([kv_cols, kv_other], axis=1), jnp.concatenate([kv_other, kv_cols], axis=1))
        dx = fill(dx, dx_got_1, core, 1)
        return y, dx, grad_w_query, grad_w_kv, grad_w_out

    return jax.shard_map(
        layer,
        mesh=mesh,
        in_specs=(P("data", None), P("data", "model"), P("data", None), P("model", "data"), P(), P(), P("data", None)),
        out_specs=(P("data", None), P("data", None), P("data", "model"), P("data", None), P("model", "data")),
        check_vma=False,
    )
```

```python
import functools

import jax
import jax.numpy as jnp
from jax import lax
from jax.experimental import pallas as pl
from jax.experimental.pallas import tpu as pltpu
from jax.sharding import PartitionSpec as P


NORM_EPS = 1e-6
LOG2E = 1.4426950408889634
BF16, F32 = jnp.bfloat16, jnp.float32
NN = (((1,), (0,)), ((), ()))
NT = (((1,), (1,)), ((), ()))
TN = (((0,), (0,)), ((), ()))
MESH = pl.DeviceIdType.MESH
ANY = pl.BlockSpec(memory_space=pl.ANY)
VMEM = pl.BlockSpec(memory_space=pltpu.VMEM)
LIMIT = 62 * 2**20


def dot(a, b, dims):
    return lax.dot_general(a, b, dims, preferred_element_type=F32)


def place():
    d, m = lax.axis_index("data"), lax.axis_index("model")
    x, c = m // 2, m % 2
    return d, m, x, c, (1 - d, m), (d, 2 * (1 - x) + c), (d, 2 * x + (1 - c))


def entry_barrier(peers):
    barrier = pltpu.get_barrier_semaphore()
    for peer in peers:
        pl.semaphore_signal(barrier, inc=1, device_id=peer, device_id_type=MESH)
    pl.semaphore_wait(barrier, len(peers))


def remote(src, dst, send, recv, peer):
    return pltpu.make_async_remote_copy(src_ref=src, dst_ref=dst, send_sem=send, recv_sem=recv, device_id=peer, device_id_type=MESH)


class Gather:
    def __init__(self, piece, full, region, send, recv, local):
        self.piece, self.full, self.region = piece, full, region
        self.send, self.recv, self.local = send, recv, local

    def copies(self):
        d, m, x, c, yn, xn, pn = place()
        ym, xm = (1 - d, m), (d, 2 * (1 - x) + c)
        full, reg, s, r = self.full, self.region, self.send, self.recv
        at = lambda dm, part=None: full.at[reg(dm[0], dm[1], part)]
        diag = (1 - d, 2 * (1 - x) + c)
        own = at((d, m))
        first = [remote(self.piece, own, s.at[0], r.at[0], yn), remote(self.piece, own, s.at[1], r.at[1], xn), remote(self.piece, own, s.at[2], r.at[2], pn)]
        second = [
            remote(at(ym, 0), at(ym, 0), s.at[3], r.at[3], xn),
            remote(at(xm, 1), at(xm, 1), s.at[4], r.at[4], yn),
            remote(at(ym), at(ym), s.at[5], r.at[5], pn),
            remote(at(xm), at(xm), s.at[6], r.at[6], pn),
        ]
        third = [remote(at(diag, 0), at(diag, 0), s.at[7], r.at[7], pn), remote(at(diag, 1), at(diag, 1), s.at[8], r.at[8], pn)]
        mine = pltpu.make_async_copy(self.piece, own, self.local)
        return first, second, third, mine

    def start(self):
        first, _, _, mine = self.copies()
        for copy in first:
            copy.start()
        mine.start()

    def middle(self):
        first, second, _, _ = self.copies()
        first[1].wait_recv()
        second[1].start()
        second[3].start()
        first[0].wait_recv()
        second[0].start()
        second[2].start()

    def own_half(self):
        first, second, _, mine = self.copies()
        mine.wait()
        first[2].wait_recv()
        second[2].wait_recv()

    def finish(self):
        first, second, third, _ = self.copies()
        second[0].wait_recv()
        third[0].start()
        second[1].wait_recv()
        third[1].start()
        second[3].wait_recv()
        third[0].wait_recv()
        third[1].wait_recv()
        for copy in first + second + third:
            copy.wait_send()


def q_region(rows, cols, d, m, part):
    if part is None:
        return pl.ds(d * rows, rows), pl.ds(pl.multiple_of(m * cols, cols), cols)
    return pl.ds(d * rows + part * (rows // 2), rows // 2), pl.ds(pl.multiple_of(m * cols, cols), cols)


def o_region(rows, cols, d, m, part):
    if part is None:
        return pl.ds(m * rows, rows), pl.ds(pl.multiple_of(d * cols, cols), cols)
    return pl.ds(m * rows + part * (rows // 2), rows // 2), pl.ds(pl.multiple_of(d * cols, cols), cols)


def front_kernel(half, tok, grad, wq, wkv, wo, gain, wcat, wo_full, hidden, means, inv_stds, proj, grad_mixed, wbuf, kbuf, q_send, q_recv, o_send, o_recv, kv_send, kv_recv, local):
    d, _, x, c, yn, xn, pn = place()
    rows, cols = wq.shape
    depth, width = wo_full.shape[1], wo_full.shape[0]
    krows, pair = wkv.shape[0] // 2, wkv.shape[1]
    part = width // 2
    entry_barrier((yn, xn, pn))
    k_here = lambda dd, cc: wcat.at[pl.ds(dd * 2 * krows + cc * krows, krows), pl.ds(width, pair)]
    k_out = remote(wkv.at[pl.ds(c * krows, krows), :], k_here(d, c), kv_send.at[0], kv_recv.at[0], yn)
    k_fwd = remote(k_here(1 - d, c), k_here(1 - d, c), kv_send.at[1], kv_recv.at[1], pn)
    k_own = pltpu.make_async_copy(wkv, wcat.at[pl.ds(d * 2 * krows, 2 * krows), pl.ds(width, pair)], local.at[2])
    gather_q = Gather(wq, wcat, functools.partial(q_region, rows, cols), q_send, q_recv, local.at[0])
    gather_o = Gather(wo, wo_full, functools.partial(o_region, wo.shape[0], wo.shape[1]), o_send, o_recv, local.at[1])
    k_out.start()
    gather_q.start()
    k_own.start()
    mine = lambda *_: pl.ds(pl.multiple_of(x * part, part), part)
    other = lambda *_: pl.ds(pl.multiple_of((1 - x) * part, part), part)
    load_q0 = pltpu.make_async_copy(wcat.at[:, mine()], wbuf.at[0], local.at[3])
    load_q1 = pltpu.make_async_copy(wcat.at[:, other()], wbuf.at[1], local.at[4])
    load_kv = pltpu.make_async_copy(wcat.at[:, pl.ds(width, pair)], kbuf, local.at[5])

    def norm_block(tok_blk, hid_blk, mean_blk, inv_blk):
        rows_f = tok_blk[...].astype(F32)
        mean = jnp.mean(rows_f, axis=-1, keepdims=True)
        centred = rows_f - mean
        inv_std = lax.rsqrt(jnp.mean(centred * centred, axis=-1, keepdims=True) + NORM_EPS)
        hid_blk[...] = (centred * inv_std * gain[...]).astype(BF16)
        mean_blk[...] = jnp.broadcast_to(mean, mean_blk.shape)
        inv_blk[...] = jnp.broadcast_to(inv_std, inv_blk.shape)

    tile = 512
    pltpu.emit_pipeline(
        norm_block,
        grid=(half // tile,),
        in_specs=[pl.BlockSpec((tile, depth), lambda i: (i, 0))],
        out_specs=[pl.BlockSpec((tile, depth), lambda i: (i, 0))] + [pl.BlockSpec((tile, 128), lambda i: (i, 0))] * 2,
    )(tok.at[pl.ds(c * half, half), :], hidden, means, inv_stds)

    big = 1024

    def run(src, weight, out, lo=0, n=half // big):
        def block(a, o):
            o[...] = dot(a[...], weight[...], NN).astype(BF16)

        pltpu.emit_pipeline(
            block,
            grid=(n,),
            in_specs=[pl.BlockSpec((big, depth), lambda i: (lo + i, 0))],
            out_specs=[pl.BlockSpec((big, out.shape[1]), lambda i: (lo + i, 0))],
        )(src, out)

    k_out.wait_recv()
    k_fwd.start()
    k_own.wait()
    k_fwd.wait_recv()
    load_kv.start()
    load_kv.wait()
    run(hidden, kbuf, proj.at[:, pl.ds(width, pair)])
    gather_q.middle()
    gather_o.start()
    gather_q.own_half()
    load_q0.start()
    load_q0.wait()
    run(hidden, wbuf.at[0], proj.at[:, mine()])
    gather_q.finish()
    load_q1.start()
    load_q1.wait()
    run(hidden, wbuf.at[1], proj.at[:, other()], 0, half // big // 2)
    gather_o.middle()
    run(hidden, wbuf.at[1], proj.at[:, other()], half // big // 2, half // big // 2)
    gather_o.own_half()
    gather_o.finish()

    def grad_block(a, b, o):
        o[...] = dot(a[...], b[...], NT).astype(BF16)

    pltpu.emit_pipeline(
        grad_block,
        grid=(width // part, half // big),
        in_specs=[pl.BlockSpec((big, depth), lambda j, i: (i, 0)), pl.BlockSpec((part, depth), lambda j, i: (j, 0))],
        out_specs=[pl.BlockSpec((big, part), lambda j, i: (i, j))],
    )(grad.at[pl.ds(c * half, half), :], wo_full, grad_mixed)
    k_out.wait_send()
    k_fwd.wait_send()


def attend_kernel(heads, head_dim, qkv_ref, do_ref, pos_ref, o_ref, dqkv_ref, seen, pt, dst):
    seq, width = do_ref.shape
    q_ref, dq_ref = qkv_ref, dqkv_ref

    @pl.when(pl.program_id(0) == 0)
    def _():
        query_pos = jnp.broadcast_to(pos_ref[...].astype(F32), (seq, seq))
        seen[...] = jnp.where(query_pos.T <= query_pos, 1.0, -1.0)

    k, v = qkv_ref[:, width : width + head_dim], qkv_ref[:, width + head_dim :]
    kt, vt = k.T, v.T
    scale = head_dim ** -0.5
    cols = lambda h: slice(h * head_dim, (h + 1) * head_dim)
    lanes = lambda h: slice(h * seq, (h + 1) * seq)
    scores, grads, total = {}, {}, [None, None]

    def scored(h):
        scores[h] = dot(k, q_ref[:, cols(h)], NT)
        grads[h] = dot(v, do_ref[:, cols(h)], NT)

    def softmax(h):
        s = jnp.where(seen[...] > 0, scores.pop(h) * (scale * LOG2E), -1e30)
        e = jnp.exp2(s - jnp.max(s, axis=0, keepdims=True))
        p = e * (1.0 / jnp.sum(e, axis=0, keepdims=True))
        pt[:, lanes(h)] = p.astype(BF16)
        dp = grads.pop(h)
        dst[:, lanes(h)] = (p * (dp - jnp.sum(p * dp, axis=0, keepdims=True))).astype(BF16)

    def mixed(h):
        o_ref[:, cols(h)] = dot(vt, pt[:, lanes(h)], NN).T.astype(BF16)
        dq_ref[:, cols(h)] = (dot(kt, dst[:, lanes(h)], NN).T * scale).astype(BF16)
        dv = dot(pt[:, lanes(h)], do_ref[:, cols(h)], NN)
        dk = dot(dst[:, lanes(h)], q_ref[:, cols(h)], NN)
        total[0] = dk if total[0] is None else total[0] + dk
        total[1] = dv if total[1] is None else total[1] + dv

    for t in range(heads + 2):
        if t < heads:
            scored(t)
        if 0 <= t - 2:
            mixed(t - 2)
        if 0 <= t - 1 < heads:
            softmax(t - 1)
    dqkv_ref[:, width : width + head_dim] = (total[0] * scale).astype(BF16)
    dqkv_ref[:, width + head_dim :] = total[1].astype(BF16)


def attend(proj, grad_mixed, positions):
    rows, width = grad_mixed.shape
    seq, total = positions.shape[0], proj.shape[1]
    head_dim = (total - width) // 2
    heads = width // head_dim
    wide = pl.BlockSpec((seq, width), lambda i: (i, 0))
    wider = pl.BlockSpec((seq, total), lambda i: (i, 0))
    return pl.pallas_call(
        functools.partial(attend_kernel, heads, head_dim),
        grid=(rows // seq,),
        in_specs=[wider, wide, pl.BlockSpec((1, seq), lambda i: (0, 0))],
        out_specs=[wide, wider],
        out_shape=[jax.ShapeDtypeStruct((rows, width), BF16), jax.ShapeDtypeStruct((rows, total), BF16)],
        scratch_shapes=[pltpu.VMEM((seq, seq), F32), pltpu.VMEM((seq, heads * seq), BF16), pltpu.VMEM((seq, heads * seq), BF16)],
        cost_estimate=pl.CostEstimate(flops=12 * rows * seq * width, bytes_accessed=8 * rows * width, transcendentals=rows * seq * heads),
        compiler_params=pltpu.CompilerParams(vmem_limit_bytes=LIMIT),
    )(proj, grad_mixed, positions.reshape(1, seq))


def give_kernel(count, off, a, *refs):
    for b, out in zip(refs[:count], refs[count:]):
        out[...] = dot(a[...], b[...], TN)


def give(a, bs, offs, shape, widths, tile=512):
    rows = a.shape[0]
    height, width = shape
    wide = width // tile
    blocks = [tile] + list(widths[1:])
    b_specs = [pl.BlockSpec((rows, w), functools.partial(lambda n, i, j, off: (off[1], off[2 + n] + (j if n == 0 else 0)), n)) for n, w in enumerate(blocks)]
    o_specs = [pl.BlockSpec((tile, w), functools.partial(lambda n, i, j, off: (i, j if n == 0 else 0), n)) for n, w in enumerate(blocks)]
    return pl.pallas_call(
        functools.partial(give_kernel, len(bs)),
        grid_spec=pltpu.PrefetchScalarGridSpec(
            num_scalar_prefetch=1,
            grid=(height // tile, wide),
            in_specs=[pl.BlockSpec((rows, tile), lambda i, j, off: (0, off[0] + i))] + b_specs,
            out_specs=o_specs,
        ),
        out_shape=[jax.ShapeDtypeStruct((height, w), F32) for w in widths],
        cost_estimate=pl.CostEstimate(flops=2 * rows * height * sum(widths), bytes_accessed=2 * rows * (height + sum(widths)), transcendentals=0),
        compiler_params=pltpu.CompilerParams(vmem_limit_bytes=LIMIT),
    )(offs, a, *bs)


def keep_kernel(half, off, a, b, got, send, keep):
    step = pl.program_id(0)
    value = got[...] + dot(a[...], b[...], TN)

    @pl.when(step < half)
    def _():
        send[...] = value

    @pl.when(step >= half)
    def _():
        keep[...] = value


def keep(a, b, offs, shape, axis, got, tile=512):
    rows = a.shape[0]
    steps = shape[axis] // tile
    half = steps // 2
    turn = lambda t, off: jnp.where(t < half, (1 - off[3]) * half + t, off[3] * half + t - half)
    at = (lambda t, off: (turn(t, off), 0)) if axis == 0 else (lambda t, off: (0, turn(t, off)))
    line = (lambda t: (t, 0)) if axis == 0 else (lambda t: (0, t))
    out = (shape[0] // 2, shape[1]) if axis == 0 else (shape[0], shape[1] // 2)
    return pl.pallas_call(
        functools.partial(keep_kernel, half),
        grid_spec=pltpu.PrefetchScalarGridSpec(
            num_scalar_prefetch=1,
            grid=(steps,),
            in_specs=[
                pl.BlockSpec((rows, tile), lambda t, off: (0, off[0] + at(t, off)[0])),
                pl.BlockSpec((rows, tile), lambda t, off: (off[1], off[2] + at(t, off)[1])),
                pl.BlockSpec((tile, tile), at),
            ],
            out_specs=[
                pl.BlockSpec((tile, tile), lambda t, off: line(jnp.minimum(t, half - 1))),
                pl.BlockSpec((tile, tile), lambda t, off: line(jnp.maximum(t - half, 0))),
            ],
        ),
        out_shape=[jax.ShapeDtypeStruct(out, F32)] * 2,
        cost_estimate=pl.CostEstimate(flops=2 * rows * shape[0] * shape[1], bytes_accessed=2 * rows * sum(shape), transcendentals=0),
        compiler_params=pltpu.CompilerParams(vmem_limit_bytes=LIMIT),
    )(offs, a, b, got)


def out_kernel(off, a, b, full, send):
    block = dot(a[...], b[...], NN).astype(BF16)
    full[...] = block
    send[...] = block


def project_out(mixed, wo, core, tile=1024):
    rows, depth = mixed.shape
    width = wo.shape[1]
    blocks = rows // tile
    return pl.pallas_call(
        out_kernel,
        grid_spec=pltpu.PrefetchScalarGridSpec(
            num_scalar_prefetch=1,
            grid=(width // tile, blocks),
            in_specs=[pl.BlockSpec((tile, depth), lambda j, i, off: (i, 0)), pl.BlockSpec((depth, tile), lambda j, i, off: (0, j))],
            out_specs=[pl.BlockSpec((tile, tile), lambda j, i, off: (off[0] * blocks + i, j)), pl.BlockSpec((tile, tile), lambda j, i, off: (i, j))],
        ),
        out_shape=[jax.ShapeDtypeStruct((2 * rows, width), BF16), jax.ShapeDtypeStruct((rows, width), BF16)],
        cost_estimate=pl.CostEstimate(flops=2 * rows * depth * width, bytes_accessed=2 * rows * (depth + 2 * width), transcendentals=0),
        compiler_params=pltpu.CompilerParams(vmem_limit_bytes=LIMIT),
    )(core, mixed, wo)


def grad_tok_kernel(passing, off, gqkv, wcat, gain, tok, means, inv_stds, *refs):
    if passing:
        got, _, _, full, send, y_full = refs
        y_full[...] = got[...]
    else:
        full, send = refs
    mean, inv_std = means[:, :1], inv_stds[:, :1]
    g = dot(gqkv[...], wcat[...], NT) * gain[...]
    normed = (tok[...].astype(F32) - mean) * inv_std
    block = (inv_std * (g - jnp.mean(g, axis=-1, keepdims=True) - normed * jnp.mean(g * normed, axis=-1, keepdims=True))).astype(BF16)
    full[...] = block
    send[...] = block


def grad_tok(gqkv, wcat, gain, tok, means, inv_stds, core, part, earlier=None, tile=512):
    rows, total = gqkv.shape
    depth = wcat.shape[0]
    blocks = rows // tile
    steps = blocks // 2
    first = part * steps
    whole = lambda i, off: (0, 0)
    once = pl.Buffered(1)
    in_specs = [
        pl.BlockSpec((tile, total), lambda i, off: (first + i, 0)),
        pl.BlockSpec((depth, total), whole, pipeline_mode=once),
        pl.BlockSpec((1, depth), whole, pipeline_mode=once),
        pl.BlockSpec((tile, depth), lambda i, off: (off[0] * blocks + first + i, 0)),
        pl.BlockSpec((tile, 128), lambda i, off: (first + i, 0)),
        pl.BlockSpec((tile, 128), lambda i, off: (first + i, 0)),
    ]
    own = pl.BlockSpec((tile, depth), lambda i, off: (off[0] * blocks + first + i, 0))
    out_specs = [own, pl.BlockSpec((tile, depth), lambda i, off: (i, 0))]
    out_shape = [jax.ShapeDtypeStruct((2 * rows, depth), BF16), jax.ShapeDtypeStruct((rows // 2, depth), BF16)]
    args, aliases = [core, gqkv, wcat, gain, tok, means, inv_stds], {}
    if earlier is not None:
        dx, y, got = earlier
        args += [got, dx, y]
        wide = 2 * tile
        in_specs += [pl.BlockSpec((wide, depth), lambda i, off: (i, 0)), ANY, ANY]
        out_specs.append(pl.BlockSpec((wide, depth), lambda i, off: ((1 - off[0]) * steps + i, 0)))
        out_shape.append(jax.ShapeDtypeStruct(y.shape, BF16))
        aliases = {8: 0, 9: 2}
    return pl.pallas_call(
        functools.partial(grad_tok_kernel, earlier is not None),
        grid_spec=pltpu.PrefetchScalarGridSpec(num_scalar_prefetch=1, grid=(steps,), in_specs=in_specs, out_specs=out_specs),
        out_shape=out_shape,
        input_output_aliases=aliases,
        cost_estimate=pl.CostEstimate(flops=rows * depth * total, bytes_accessed=5 * rows * depth, transcendentals=0),
        compiler_params=pltpu.CompilerParams(vmem_limit_bytes=LIMIT),
    )(*args)


def fill_kernel(off, got, _, out):
    out[...] = got[...]


def fill(full, got, core, part, tile=1024):
    rows, width = got.shape
    blocks = rows // tile
    return pl.pallas_call(
        fill_kernel,
        grid_spec=pltpu.PrefetchScalarGridSpec(
            num_scalar_prefetch=1,
            grid=(blocks,),
            in_specs=[pl.BlockSpec((tile, width), lambda i, off: (i, 0)), ANY],
            out_specs=pl.BlockSpec((tile, width), lambda i, off: ((1 - off[0]) * 2 * blocks + part * blocks + i, 0)),
        ),
        out_shape=jax.ShapeDtypeStruct(full.shape, full.dtype),
        input_output_aliases={2: 0},
        cost_estimate=pl.CostEstimate(flops=rows * width, bytes_accessed=4 * rows * width, transcendentals=0),
        compiler_params=pltpu.CompilerParams(vmem_limit_bytes=LIMIT),
    )(core, got, full)


def after(value, *others):
    return lax.optimization_barrier((value,) + others)[0]


def solution(mesh):
    model_size = mesh.shape["model"]
    cores = [(i, i ^ 1) for i in range(model_size)]
    datas = [(0, 1), (1, 0)]
    sems = lambda n: pltpu.SemaphoreType.DMA((n,))

    def layer(tok, wq_blk, wkv_blk, wo_blk, ln_gain, positions, grad):
        count, depth = tok.shape
        half = count // 2
        width = wq_blk.shape[1] * model_size
        pair = wkv_blk.shape[1]
        piece = width // model_size
        m = lax.axis_index("model")
        d = lax.axis_index("data")
        x, c = m // 2, m % 2
        gain = ln_gain.reshape(1, depth)
        core = c.reshape(1).astype(jnp.int32)
        index = lambda *v: jnp.stack([jnp.asarray(t, jnp.int32) for t in v])

        def swap(a):
            return lax.ppermute(a, "model", cores)

        def cross(a):
            return lax.ppermute(a, "data", datas)


        wcat, wo, hidden, means, inv_stds, proj, grad_mixed = pl.pallas_call(
            functools.partial(front_kernel, half),
            in_specs=[ANY, ANY, VMEM, VMEM, VMEM, VMEM],
            out_specs=[ANY] * 7,
            out_shape=[
                jax.ShapeDtypeStruct((depth, width + pair), BF16),
                jax.ShapeDtypeStruct((width, depth), BF16),
                jax.ShapeDtypeStruct((half, depth), BF16),
                jax.ShapeDtypeStruct((half, 128), F32),
                jax.ShapeDtypeStruct((half, 128), F32),
                jax.ShapeDtypeStruct((half, width + pair), BF16),
                jax.ShapeDtypeStruct((half, width), BF16),
            ],
            scratch_shapes=[pltpu.VMEM((2, depth, width // 2), BF16), pltpu.VMEM((depth, pair), BF16)]
            + [sems(9), sems(9), sems(9), sems(9), sems(2), sems(2), sems(6)],
            compiler_params=pltpu.CompilerParams(collective_id=0, has_side_effects=True, vmem_limit_bytes=LIMIT),
        )(tok, grad, wq_blk, wkv_blk, wo_blk, gain)

        mixed, gqkv = attend(proj, grad_mixed, positions)

        def halves(a, i, axis):
            size = a.shape[axis] // 2
            return lax.dynamic_slice_in_dim(a, i * size, size, axis), lax.dynamic_slice_in_dim(a, (1 - i) * size, size, axis)

        mine, other = 2 * x + c, 2 * x + 1 - c
        (give_o,) = give(mixed, [grad], index(other, c, 0), (piece, depth), [depth])
        got_o = swap(give_o)
        give_q, part_kv = give(after(hidden, give_o), [gqkv, gqkv], index(0, 0, other, width // pair), (depth, piece), [piece, pair])
        got_q = swap(give_q)
        kv_keep, kv_give = halves(part_kv, c, 1)
        kv_got = swap(kv_give)
        send_o, keep_o = keep(after(mixed, give_q), grad, index(mine, c, 0, d), (piece, depth), 1, got_o)
        data_o = cross(send_o)
        kv_keep, kv_give = halves(kv_keep + kv_got, d, 0)
        kv_data = cross(kv_give)
        send_q, keep_q = keep(after(hidden, send_o, kv_give), gqkv, index(0, 0, mine, d), (depth, piece), 0, got_q)
        data_q = cross(send_q)

        y, y_send = project_out(after(mixed, send_q), wo, core)
        y_got = swap(y_send)
        dx, dx_send = grad_tok(after(gqkv, y_send), wcat, gain, tok, means, inv_stds, core, 0)
        dx_got_0 = swap(dx_send)
        kv_cols = (kv_keep + kv_data).astype(BF16)
        kv_other = swap(kv_cols)
        dx, dx_send, y = grad_tok(after(gqkv, dx_send, kv_cols), wcat, gain, tok, means, inv_stds, core, 1, (dx, y, y_got))
        dx_got_1 = swap(dx_send)
        dx = fill(dx, dx_got_0, core, 0)
        data_o, data_q, kv_other = lax.optimization_barrier((data_o, data_q, kv_other, dx_send))[:3]
        grad_w_out = (keep_o + data_o).astype(BF16)
        grad_w_query = (keep_q + data_q).astype(BF16)
        grad_w_kv = jnp.where(c == 0, jnp.concatenate([kv_cols, kv_other], axis=1), jnp.concatenate([kv_other, kv_cols], axis=1))
        dx = fill(dx, dx_got_1, core, 1)
        return y, dx, grad_w_query, grad_w_kv, grad_w_out

    return jax.shard_map(
        layer,
        mesh=mesh,
        in_specs=(P("data", None), P("data", "model"), P("data", None), P("model", "data"), P(), P(), P("data", None)),
        out_specs=(P("data", None), P("data", None), P("data", "model"), P("data", None), P("model", "data")),
        check_vma=False,
    )
```

```python
import functools

import jax
import jax.numpy as jnp
from jax import lax
from jax.experimental import pallas as pl
from jax.experimental.pallas import tpu as pltpu
from jax.sharding import PartitionSpec as P


NORM_EPS = 1e-6
LOG2E = 1.4426950408889634
BF16, F32 = jnp.bfloat16, jnp.float32
NN = (((1,), (0,)), ((), ()))
NT = (((1,), (1,)), ((), ()))
TN = (((0,), (0,)), ((), ()))
MESH = pl.DeviceIdType.MESH
ANY = pl.BlockSpec(memory_space=pl.ANY)
VMEM = pl.BlockSpec(memory_space=pltpu.VMEM)
LIMIT = 62 * 2**20


def dot(a, b, dims):
    return lax.dot_general(a, b, dims, preferred_element_type=F32)


def place():
    d, m = lax.axis_index("data"), lax.axis_index("model")
    x, c = m // 2, m % 2
    return d, m, x, c, (1 - d, m), (d, 2 * (1 - x) + c), (d, 2 * x + (1 - c))


def entry_barrier(peers):
    barrier = pltpu.get_barrier_semaphore()
    for peer in peers:
        pl.semaphore_signal(barrier, inc=1, device_id=peer, device_id_type=MESH)
    pl.semaphore_wait(barrier, len(peers))


def remote(src, dst, send, recv, peer):
    return pltpu.make_async_remote_copy(src_ref=src, dst_ref=dst, send_sem=send, recv_sem=recv, device_id=peer, device_id_type=MESH)


class Gather:
    def __init__(self, piece, full, region, send, recv, local):
        self.piece, self.full, self.region = piece, full, region
        self.send, self.recv, self.local = send, recv, local

    def copies(self):
        d, m, x, c, yn, xn, pn = place()
        ym, xm = (1 - d, m), (d, 2 * (1 - x) + c)
        full, reg, s, r = self.full, self.region, self.send, self.recv
        at = lambda dm, part=None: full.at[reg(dm[0], dm[1], part)]
        diag = (1 - d, 2 * (1 - x) + c)
        own = at((d, m))
        first = [remote(self.piece, own, s.at[0], r.at[0], yn), remote(self.piece, own, s.at[1], r.at[1], xn), remote(self.piece, own, s.at[2], r.at[2], pn)]
        second = [
            remote(at(ym, 0), at(ym, 0), s.at[3], r.at[3], xn),
            remote(at(xm, 1), at(xm, 1), s.at[4], r.at[4], yn),
            remote(at(ym), at(ym), s.at[5], r.at[5], pn),
            remote(at(xm), at(xm), s.at[6], r.at[6], pn),
        ]
        third = [remote(at(diag, 0), at(diag, 0), s.at[7], r.at[7], pn), remote(at(diag, 1), at(diag, 1), s.at[8], r.at[8], pn)]
        mine = pltpu.make_async_copy(self.piece, own, self.local)
        return first, second, third, mine

    def start(self):
        first, _, _, mine = self.copies()
        for copy in first:
            copy.start()
        mine.start()

    def middle(self):
        first, second, _, _ = self.copies()
        first[1].wait_recv()
        second[1].start()
        second[3].start()
        first[0].wait_recv()
        second[0].start()
        second[2].start()

    def own_half(self):
        first, second, _, mine = self.copies()
        mine.wait()
        first[2].wait_recv()
        second[2].wait_recv()

    def finish(self):
        first, second, third, _ = self.copies()
        second[0].wait_recv()
        third[0].start()
        second[1].wait_recv()
        third[1].start()
        second[3].wait_recv()
        third[0].wait_recv()
        third[1].wait_recv()
        for copy in first + second + third:
            copy.wait_send()


def q_region(rows, cols, d, m, part):
    if part is None:
        return pl.ds(d * rows, rows), pl.ds(pl.multiple_of(m * cols, cols), cols)
    return pl.ds(d * rows + part * (rows // 2), rows // 2), pl.ds(pl.multiple_of(m * cols, cols), cols)


def o_region(rows, cols, d, m, part):
    if part is None:
        return pl.ds(m * rows, rows), pl.ds(pl.multiple_of(d * cols, cols), cols)
    return pl.ds(m * rows + part * (rows // 2), rows // 2), pl.ds(pl.multiple_of(d * cols, cols), cols)


def front_kernel(half, tok, grad, wq, wkv, wo, gain, wcat, wo_full, hidden, means, inv_stds, proj, grad_mixed, wbuf, kbuf, q_send, q_recv, o_send, o_recv, kv_send, kv_recv, local):
    d, _, x, c, yn, xn, pn = place()
    rows, cols = wq.shape
    depth, width = wo_full.shape[1], wo_full.shape[0]
    krows, pair = wkv.shape[0] // 2, wkv.shape[1]
    part = width // 2
    entry_barrier((yn, xn, pn))
    k_here = lambda dd, cc: wcat.at[pl.ds(dd * 2 * krows + cc * krows, krows), pl.ds(width, pair)]
    k_out = remote(wkv.at[pl.ds(c * krows, krows), :], k_here(d, c), kv_send.at[0], kv_recv.at[0], yn)
    k_fwd = remote(k_here(1 - d, c), k_here(1 - d, c), kv_send.at[1], kv_recv.at[1], pn)
    k_own = pltpu.make_async_copy(wkv, wcat.at[pl.ds(d * 2 * krows, 2 * krows), pl.ds(width, pair)], local.at[2])
    gather_q = Gather(wq, wcat, functools.partial(q_region, rows, cols), q_send, q_recv, local.at[0])
    gather_o = Gather(wo, wo_full, functools.partial(o_region, wo.shape[0], wo.shape[1]), o_send, o_recv, local.at[1])
    k_out.start()
    gather_q.start()
    k_own.start()
    mine = lambda *_: pl.ds(pl.multiple_of(x * part, part), part)
    other = lambda *_: pl.ds(pl.multiple_of((1 - x) * part, part), part)
    load_q0 = pltpu.make_async_copy(wcat.at[:, mine()], wbuf.at[0], local.at[3])
    load_q1 = pltpu.make_async_copy(wcat.at[:, other()], wbuf.at[1], local.at[4])
    load_kv = pltpu.make_async_copy(wcat.at[:, pl.ds(width, pair)], kbuf, local.at[5])

    def norm_block(tok_blk, hid_blk, mean_blk, inv_blk):
        rows_f = tok_blk[...].astype(F32)
        mean = jnp.mean(rows_f, axis=-1, keepdims=True)
        centred = rows_f - mean
        inv_std = lax.rsqrt(jnp.mean(centred * centred, axis=-1, keepdims=True) + NORM_EPS)
        hid_blk[...] = (centred * inv_std * gain[...]).astype(BF16)
        mean_blk[...] = jnp.broadcast_to(mean, mean_blk.shape)
        inv_blk[...] = jnp.broadcast_to(inv_std, inv_blk.shape)

    tile = 512
    pltpu.emit_pipeline(
        norm_block,
        grid=(half // tile,),
        in_specs=[pl.BlockSpec((tile, depth), lambda i: (i, 0))],
        out_specs=[pl.BlockSpec((tile, depth), lambda i: (i, 0))] + [pl.BlockSpec((tile, 128), lambda i: (i, 0))] * 2,
    )(tok.at[pl.ds(c * half, half), :], hidden, means, inv_stds)

    big = 1024

    def run(src, weight, out, lo=0, n=half // big):
        def block(a, o):
            o[...] = dot(a[...], weight[...], NN).astype(BF16)

        pltpu.emit_pipeline(
            block,
            grid=(n,),
            in_specs=[pl.BlockSpec((big, depth), lambda i: (lo + i, 0))],
            out_specs=[pl.BlockSpec((big, out.shape[1]), lambda i: (lo + i, 0))],
        )(src, out)

    k_out.wait_recv()
    k_fwd.start()
    k_own.wait()
    k_fwd.wait_recv()
    load_kv.start()
    load_kv.wait()
    run(hidden, kbuf, proj.at[:, pl.ds(width, pair)])
    gather_q.middle()
    gather_o.start()
    gather_q.own_half()
    load_q0.start()
    load_q0.wait()
    run(hidden, wbuf.at[0], proj.at[:, mine()])
    gather_q.finish()
    load_q1.start()
    load_q1.wait()
    run(hidden, wbuf.at[1], proj.at[:, other()], 0, half // big // 2)
    gather_o.middle()
    run(hidden, wbuf.at[1], proj.at[:, other()], half // big // 2, half // big // 2)
    gather_o.own_half()
    gather_o.finish()

    def grad_block(a, b, o):
        o[...] = dot(a[...], b[...], NT).astype(BF16)

    pltpu.emit_pipeline(
        grad_block,
        grid=(width // part, half // big),
        in_specs=[pl.BlockSpec((big, depth), lambda j, i: (i, 0)), pl.BlockSpec((part, depth), lambda j, i: (j, 0))],
        out_specs=[pl.BlockSpec((big, part), lambda j, i: (i, j))],
    )(grad.at[pl.ds(c * half, half), :], wo_full, grad_mixed)
    k_out.wait_send()
    k_fwd.wait_send()


def attend_kernel(heads, head_dim, qkv_ref, do_ref, pos_ref, o_ref, dqkv_ref, seen, pt, dst):
    seq, width = do_ref.shape
    q_ref, dq_ref = qkv_ref, dqkv_ref

    @pl.when(pl.program_id(0) == 0)
    def _():
        query_pos = jnp.broadcast_to(pos_ref[...].astype(F32), (seq, seq))
        seen[...] = jnp.where(query_pos.T <= query_pos, 1.0, -1.0)

    k, v = qkv_ref[:, width : width + head_dim], qkv_ref[:, width + head_dim :]
    kt, vt = k.T, v.T
    scale = head_dim ** -0.5
    cols = lambda h: slice(h * head_dim, (h + 1) * head_dim)
    lanes = lambda h: slice(h * seq, (h + 1) * seq)
    scores, grads, total = {}, {}, [None, None]

    def scored(h):
        scores[h] = dot(k, q_ref[:, cols(h)], NT)
        grads[h] = dot(v, do_ref[:, cols(h)], NT)

    def softmax(h):
        s = jnp.where(seen[...] > 0, scores.pop(h) * (scale * LOG2E), -1e30)
        e = jnp.exp2(s - jnp.max(s, axis=0, keepdims=True))
        p = e * (1.0 / jnp.sum(e, axis=0, keepdims=True))
        pt[:, lanes(h)] = p.astype(BF16)
        dp = grads.pop(h)
        dst[:, lanes(h)] = (p * (dp - jnp.sum(p * dp, axis=0, keepdims=True))).astype(BF16)

    def mixed(h):
        o_ref[:, cols(h)] = dot(vt, pt[:, lanes(h)], NN).T.astype(BF16)
        dq_ref[:, cols(h)] = (dot(kt, dst[:, lanes(h)], NN).T * scale).astype(BF16)
        dv = dot(pt[:, lanes(h)], do_ref[:, cols(h)], NN)
        dk = dot(dst[:, lanes(h)], q_ref[:, cols(h)], NN)
        total[0] = dk if total[0] is None else total[0] + dk
        total[1] = dv if total[1] is None else total[1] + dv

    for t in range(heads + 2):
        if t < heads:
            scored(t)
        if 0 <= t - 2:
            mixed(t - 2)
        if 0 <= t - 1 < heads:
            softmax(t - 1)
    dqkv_ref[:, width : width + head_dim] = (total[0] * scale).astype(BF16)
    dqkv_ref[:, width + head_dim :] = total[1].astype(BF16)


def attend(proj, grad_mixed, positions):
    rows, width = grad_mixed.shape
    seq, total = positions.shape[0], proj.shape[1]
    head_dim = (total - width) // 2
    heads = width // head_dim
    wide = pl.BlockSpec((seq, width), lambda i: (i, 0))
    wider = pl.BlockSpec((seq, total), lambda i: (i, 0))
    return pl.pallas_call(
        functools.partial(attend_kernel, heads, head_dim),
        grid=(rows // seq,),
        in_specs=[wider, wide, pl.BlockSpec((1, seq), lambda i: (0, 0))],
        out_specs=[wide, wider],
        out_shape=[jax.ShapeDtypeStruct((rows, width), BF16), jax.ShapeDtypeStruct((rows, total), BF16)],
        scratch_shapes=[pltpu.VMEM((seq, seq), F32), pltpu.VMEM((seq, heads * seq), BF16), pltpu.VMEM((seq, heads * seq), BF16)],
        cost_estimate=pl.CostEstimate(flops=12 * rows * seq * width, bytes_accessed=8 * rows * width, transcendentals=rows * seq * heads),
        compiler_params=pltpu.CompilerParams(vmem_limit_bytes=LIMIT),
    )(proj, grad_mixed, positions.reshape(1, seq))


def give_kernel(count, off, a, *refs):
    for b, out in zip(refs[:count], refs[count:]):
        out[...] = dot(a[...], b[...], TN)


def give(a, bs, offs, shape, widths, tile=512):
    rows = a.shape[0]
    height, width = shape
    wide = width // tile
    blocks = [tile] + list(widths[1:])
    b_specs = [pl.BlockSpec((rows, w), functools.partial(lambda n, i, j, off: (off[1], off[2 + n] + (j if n == 0 else 0)), n)) for n, w in enumerate(blocks)]
    o_specs = [pl.BlockSpec((tile, w), functools.partial(lambda n, i, j, off: (i, j if n == 0 else 0), n)) for n, w in enumerate(blocks)]
    return pl.pallas_call(
        functools.partial(give_kernel, len(bs)),
        grid_spec=pltpu.PrefetchScalarGridSpec(
            num_scalar_prefetch=1,
            grid=(height // tile, wide),
            in_specs=[pl.BlockSpec((rows, tile), lambda i, j, off: (0, off[0] + i))] + b_specs,
            out_specs=o_specs,
        ),
        out_shape=[jax.ShapeDtypeStruct((height, w), F32) for w in widths],
        cost_estimate=pl.CostEstimate(flops=2 * rows * height * sum(widths), bytes_accessed=2 * rows * (height + sum(widths)), transcendentals=0),
        compiler_params=pltpu.CompilerParams(vmem_limit_bytes=LIMIT),
    )(offs, a, *bs)


def keep_kernel(half, off, a, b, got, send, keep):
    step = pl.program_id(0)
    value = got[...] + dot(a[...], b[...], TN)

    @pl.when(step < half)
    def _():
        send[...] = value

    @pl.when(step >= half)
    def _():
        keep[...] = value


def keep(a, b, offs, shape, axis, got, tile=512):
    rows = a.shape[0]
    steps = shape[axis] // tile
    half = steps // 2
    turn = lambda t, off: jnp.where(t < half, (1 - off[3]) * half + t, off[3] * half + t - half)
    at = (lambda t, off: (turn(t, off), 0)) if axis == 0 else (lambda t, off: (0, turn(t, off)))
    line = (lambda t: (t, 0)) if axis == 0 else (lambda t: (0, t))
    out = (shape[0] // 2, shape[1]) if axis == 0 else (shape[0], shape[1] // 2)
    return pl.pallas_call(
        functools.partial(keep_kernel, half),
        grid_spec=pltpu.PrefetchScalarGridSpec(
            num_scalar_prefetch=1,
            grid=(steps,),
            in_specs=[
                pl.BlockSpec((rows, tile), lambda t, off: (0, off[0] + at(t, off)[0])),
                pl.BlockSpec((rows, tile), lambda t, off: (off[1], off[2] + at(t, off)[1])),
                pl.BlockSpec((tile, tile), at),
            ],
            out_specs=[
                pl.BlockSpec((tile, tile), lambda t, off: line(jnp.minimum(t, half - 1))),
                pl.BlockSpec((tile, tile), lambda t, off: line(jnp.maximum(t - half, 0))),
            ],
        ),
        out_shape=[jax.ShapeDtypeStruct(out, F32)] * 2,
        cost_estimate=pl.CostEstimate(flops=2 * rows * shape[0] * shape[1], bytes_accessed=2 * rows * sum(shape), transcendentals=0),
        compiler_params=pltpu.CompilerParams(vmem_limit_bytes=LIMIT),
    )(offs, a, b, got)


def out_kernel(passing, off, a, b, *refs):
    if passing:
        got, _, _, full, send, dx_full = refs
        dx_full[...] = got[...]
    else:
        full, send = refs
    block = dot(a[...], b[...], NN).astype(BF16)
    full[...] = block
    send[...] = block


def project_out(mixed, wo, core, part, earlier=None, tile=1024):
    rows, depth = mixed.shape
    width = wo.shape[1]
    blocks = rows // tile
    steps = blocks // 2
    first = part * steps
    in_specs = [pl.BlockSpec((tile, depth), lambda j, i, off: (first + i, 0)), pl.BlockSpec((depth, tile), lambda j, i, off: (0, j))]
    out_specs = [pl.BlockSpec((tile, tile), lambda j, i, off: (off[0] * blocks + first + i, j)), pl.BlockSpec((tile, tile), lambda j, i, off: (i, j))]
    out_shape = [jax.ShapeDtypeStruct((2 * rows, width), BF16), jax.ShapeDtypeStruct((rows // 2, width), BF16)]
    args, aliases = [core, mixed, wo], {}
    if earlier is not None:
        y, dx, got = earlier
        args += [got, y, dx]
        turns = steps * (width // tile)
        wide = rows // turns
        in_specs += [pl.BlockSpec((wide, width), lambda j, i, off: (j * steps + i, 0)), ANY, ANY]
        out_specs.append(pl.BlockSpec((wide, width), lambda j, i, off: ((1 - off[0]) * turns + j * steps + i, 0)))
        out_shape.append(jax.ShapeDtypeStruct(dx.shape, BF16))
        aliases = {4: 0, 5: 2}
    return pl.pallas_call(
        functools.partial(out_kernel, earlier is not None),
        grid_spec=pltpu.PrefetchScalarGridSpec(num_scalar_prefetch=1, grid=(width // tile, steps), in_specs=in_specs, out_specs=out_specs),
        out_shape=out_shape,
        input_output_aliases=aliases,
        cost_estimate=pl.CostEstimate(flops=rows * depth * width, bytes_accessed=5 * rows * depth, transcendentals=0),
        compiler_params=pltpu.CompilerParams(vmem_limit_bytes=LIMIT),
    )(*args)


def grad_tok_kernel(passing, off, gqkv, wcat, gain, tok, means, inv_stds, *refs):
    if passing:
        got, _, _, full, send, y_full = refs
        y_full[...] = got[...]
    else:
        full, send = refs
    mean, inv_std = means[:, :1], inv_stds[:, :1]
    g = dot(gqkv[...], wcat[...], NT) * gain[...]
    normed = (tok[...].astype(F32) - mean) * inv_std
    block = (inv_std * (g - jnp.mean(g, axis=-1, keepdims=True) - normed * jnp.mean(g * normed, axis=-1, keepdims=True))).astype(BF16)
    full[...] = block
    send[...] = block


def grad_tok(gqkv, wcat, gain, tok, means, inv_stds, core, earlier=None, tile=512):
    rows, total = gqkv.shape
    depth = wcat.shape[0]
    blocks = rows // tile
    steps, first = blocks, 0
    whole = lambda i, off: (0, 0)
    once = pl.Buffered(1)
    in_specs = [
        pl.BlockSpec((tile, total), lambda i, off: (first + i, 0)),
        pl.BlockSpec((depth, total), whole, pipeline_mode=once),
        pl.BlockSpec((1, depth), whole, pipeline_mode=once),
        pl.BlockSpec((tile, depth), lambda i, off: (off[0] * blocks + first + i, 0)),
        pl.BlockSpec((tile, 128), lambda i, off: (first + i, 0)),
        pl.BlockSpec((tile, 128), lambda i, off: (first + i, 0)),
    ]
    own = pl.BlockSpec((tile, depth), lambda i, off: (off[0] * blocks + first + i, 0))
    out_specs = [own, pl.BlockSpec((tile, depth), lambda i, off: (i, 0))]
    out_shape = [jax.ShapeDtypeStruct((2 * rows, depth), BF16), jax.ShapeDtypeStruct((rows, depth), BF16)]
    args, aliases = [core, gqkv, wcat, gain, tok, means, inv_stds], {}
    if earlier is not None:
        dx, y, got = earlier
        args += [got, dx, y]
        wide = 2 * tile
        in_specs += [pl.BlockSpec((wide, depth), lambda i, off: (i, 0)), ANY, ANY]
        out_specs.append(pl.BlockSpec((wide, depth), lambda i, off: ((1 - off[0]) * steps + i, 0)))
        out_shape.append(jax.ShapeDtypeStruct(y.shape, BF16))
        aliases = {8: 0, 9: 2}
    return pl.pallas_call(
        functools.partial(grad_tok_kernel, earlier is not None),
        grid_spec=pltpu.PrefetchScalarGridSpec(num_scalar_prefetch=1, grid=(steps,), in_specs=in_specs, out_specs=out_specs),
        out_shape=out_shape,
        input_output_aliases=aliases,
        cost_estimate=pl.CostEstimate(flops=rows * depth * total, bytes_accessed=5 * rows * depth, transcendentals=0),
        compiler_params=pltpu.CompilerParams(vmem_limit_bytes=LIMIT),
    )(*args)


def fill_kernel(off, got, _, out):
    out[...] = got[...]


def fill(full, got, core, part, tile=1024):
    rows, width = got.shape
    blocks = rows // tile
    return pl.pallas_call(
        fill_kernel,
        grid_spec=pltpu.PrefetchScalarGridSpec(
            num_scalar_prefetch=1,
            grid=(blocks,),
            in_specs=[pl.BlockSpec((tile, width), lambda i, off: (i, 0)), ANY],
            out_specs=pl.BlockSpec((tile, width), lambda i, off: ((1 - off[0]) * 2 * blocks + part * blocks + i, 0)),
        ),
        out_shape=jax.ShapeDtypeStruct(full.shape, full.dtype),
        input_output_aliases={2: 0},
        cost_estimate=pl.CostEstimate(flops=rows * width, bytes_accessed=4 * rows * width, transcendentals=0),
        compiler_params=pltpu.CompilerParams(vmem_limit_bytes=LIMIT),
    )(core, got, full)


def after(value, *others):
    return lax.optimization_barrier((value,) + others)[0]


def solution(mesh):
    model_size = mesh.shape["model"]
    cores = [(i, i ^ 1) for i in range(model_size)]
    datas = [(0, 1), (1, 0)]
    sems = lambda n: pltpu.SemaphoreType.DMA((n,))

    def layer(tok, wq_blk, wkv_blk, wo_blk, ln_gain, positions, grad):
        count, depth = tok.shape
        half = count // 2
        width = wq_blk.shape[1] * model_size
        pair = wkv_blk.shape[1]
        piece = width // model_size
        m = lax.axis_index("model")
        d = lax.axis_index("data")
        x, c = m // 2, m % 2
        gain = ln_gain.reshape(1, depth)
        core = c.reshape(1).astype(jnp.int32)
        index = lambda *v: jnp.stack([jnp.asarray(t, jnp.int32) for t in v])

        def swap(a):
            return lax.ppermute(a, "model", cores)

        def cross(a):
            return lax.ppermute(a, "data", datas)


        wcat, wo, hidden, means, inv_stds, proj, grad_mixed = pl.pallas_call(
            functools.partial(front_kernel, half),
            in_specs=[ANY, ANY, VMEM, VMEM, VMEM, VMEM],
            out_specs=[ANY] * 7,
            out_shape=[
                jax.ShapeDtypeStruct((depth, width + pair), BF16),
                jax.ShapeDtypeStruct((width, depth), BF16),
                jax.ShapeDtypeStruct((half, depth), BF16),
                jax.ShapeDtypeStruct((half, 128), F32),
                jax.ShapeDtypeStruct((half, 128), F32),
                jax.ShapeDtypeStruct((half, width + pair), BF16),
                jax.ShapeDtypeStruct((half, width), BF16),
            ],
            scratch_shapes=[pltpu.VMEM((2, depth, width // 2), BF16), pltpu.VMEM((depth, pair), BF16)]
            + [sems(9), sems(9), sems(9), sems(9), sems(2), sems(2), sems(6)],
            compiler_params=pltpu.CompilerParams(collective_id=0, has_side_effects=True, vmem_limit_bytes=LIMIT),
        )(tok, grad, wq_blk, wkv_blk, wo_blk, gain)

        mixed, gqkv = attend(proj, grad_mixed, positions)

        def halves(a, i, axis):
            size = a.shape[axis] // 2
            return lax.dynamic_slice_in_dim(a, i * size, size, axis), lax.dynamic_slice_in_dim(a, (1 - i) * size, size, axis)

        mine, other = 2 * x + c, 2 * x + 1 - c
        (give_o,) = give(mixed, [grad], index(other, c, 0), (piece, depth), [depth])
        got_o = swap(give_o)
        give_q, part_kv = give(after(hidden, give_o), [gqkv, gqkv], index(0, 0, other, width // pair), (depth, piece), [piece, pair])
        got_q = swap(give_q)
        kv_keep, kv_give = halves(part_kv, c, 1)
        kv_got = swap(kv_give)
        send_o, keep_o = keep(after(mixed, give_q), grad, index(mine, c, 0, d), (piece, depth), 1, got_o)
        data_o = cross(send_o)
        kv_keep, kv_give = halves(kv_keep + kv_got, d, 0)
        kv_data = cross(kv_give)
        send_q, keep_q = keep(after(hidden, send_o, kv_give), gqkv, index(0, 0, mine, d), (depth, piece), 0, got_q)
        data_q = cross(send_q)

        dx, dx_send = grad_tok(after(gqkv, send_q), wcat, gain, tok, means, inv_stds, core)
        dx_got = swap(dx_send)
        y, y_send = project_out(after(mixed, dx_send), wo, core, 0)
        y_got_0 = swap(y_send)
        kv_cols = (kv_keep + kv_data).astype(BF16)
        kv_other = swap(kv_cols)
        y, y_send, dx = project_out(after(mixed, y_send, kv_cols), wo, core, 1, (y, dx, dx_got))
        y_got_1 = swap(y_send)
        y = fill(y, y_got_0, core, 0)
        data_o, data_q, kv_other = lax.optimization_barrier((data_o, data_q, kv_other, y_send))[:3]
        grad_w_out = (keep_o + data_o).astype(BF16)
        grad_w_query = (keep_q + data_q).astype(BF16)
        grad_w_kv = jnp.where(c == 0, jnp.concatenate([kv_cols, kv_other], axis=1), jnp.concatenate([kv_other, kv_cols], axis=1))
        y = fill(y, y_got_1, core, 1)
        return y, dx, grad_w_query, grad_w_kv, grad_w_out

    return jax.shard_map(
        layer,
        mesh=mesh,
        in_specs=(P("data", None), P("data", "model"), P("data", None), P("model", "data"), P(), P(), P("data", None)),
        out_specs=(P("data", None), P("data", None), P("data", "model"), P("data", None), P("model", "data")),
        check_vma=False,
    )
```
